32 devices in a mesh: seq: 8 (over y, x, core), kvh: 4 (over z).
Axes of the slice: x: 2, y: 2, z: 4, core: 2. Of those that a mesh axis runs over, the one named last changes fastest.
Arguments:
- hidden: bfloat16 [6144, 4096], P('seq'), may hold values from -32 to 32
- w_query: bfloat16 [4096, 4096], P(None, 'kvh'), may hold values from -0.09375 to 0.09375
- w_key: bfloat16 [4096, 1024], P(None, 'kvh'), may hold values from -0.09375 to 0.09375
- w_value: bfloat16 [4096, 1024], P(None, 'kvh'), may hold values from -0.09375 to 0.09375
- cached_key: bfloat16 [6144, 1024], P('seq', 'kvh'), may hold values from -6 to 6
- cached_value: bfloat16 [6144, 1024], P('seq', 'kvh'), may hold values from -6 to 6
- doc_lengths: int32 [4], replicated, may hold values from 1 to 3072, 6144 in all
- selected: int32 [960], replicated, may hold values from 0 to 767, as said below
Outputs:
- attended: bfloat16 [960, 4096], P('seq', 'kvh')
- score: float32 [6144], P('seq')
The draws below stay inside these ranges and needn't reach their ends.
Inputs may be any that keep to these rules, and one draw needn't show every extreme that they name: `selected`: each block of 120 entries holds distinct local row numbers in increasing order.
All inputs are finite; a program needn't handle non-finite values.
Results may differ from the reference program's by a relative error of at most 0.02.
Values may be sent and summed in bfloat16 or wider, within the bound.
A program may use at most 192 MiB of HBM per device.

```python
import math
import jax
import jax.numpy as jnp
import numpy as np
from jax import lax

D = 4096
HEADS = 32
KV_HEADS = 8
HEAD_DIM = 128
TOK_DEV = 768
DOCS = 4
SEL_DEV = 120
TOKENS = 6144
SELECTED = 960
DOC_MOST = 3072


def draw_selected(key, part):
    blocks = TOKENS // TOK_DEV
    block_keys = jax.random.split(key, blocks)

    def one_block(block_key):
        shuffled = jax.random.permutation(block_key, TOK_DEV)
        return jnp.sort(shuffled[:SEL_DEV]).astype(jnp.int32)
    return jax.vmap(one_block)(block_keys).reshape(-1).astype(jnp.int32)


def draw_hidden(key, part):
    base = jnp.clip(jax.random.normal(key, (TOKENS, D), jnp.float32), -4.0, 4.0)
    region_scale = jnp.exp(jax.random.uniform(jax.random.fold_in(key, 11), (16,), jnp.float32, jnp.log(0.5), jnp.log(2.5)))
    region = jnp.arange(TOKENS, dtype=jnp.int32) * 16 // TOKENS
    base = base * region_scale[region][:, None]
    return base.astype(jnp.bfloat16)


def level_of(stream_key, shape, cuts, low, largest):
    level, own = 1.0, jax.random.fold_in(stream_key, 6)
    for position, parts in cuts:
        heights = jnp.exp(jax.random.uniform(jax.random.fold_in(own, position), (parts,), jnp.float32, low / len(cuts), largest / len(cuts)))
        level = level * jnp.repeat(heights, shape[position] // parts).reshape([-1 if axis == position else 1 for axis in range(len(shape))])
    return level


def profile(number_of, total, bound, skew):
    weights = [(1 << 20) // math.isqrt(standing ** skew) + 1 for standing in range(2, number_of + 1)]
    spare, given = total - bound - (number_of - 1), [1] * (number_of - 1)
    while spare > 0:
        candidates = [i for i in range(number_of - 1) if given[i] < bound]
        pool, budget = sum([weights[i] for i in candidates]), spare
        for i in candidates:
            addition = min(bound - given[i], max(1, budget * weights[i] // pool), spare)
            given[i] = given[i] + addition
            spare = spare - addition
    return np.array([bound] + given)


def ragged_sizes(own_key, amount, total, limit, slope):
    if amount == 2:
        one = jax.random.randint(own_key, (), max(1, total - limit), min(limit, total - 1) + 1)
        return jnp.stack([one, total - one])
    lengths = jnp.asarray(profile(amount, total, limit, slope), jnp.int32)
    pairs = (amount - 1) // 2
    giver, receiver = lengths[1:1 + 2 * pairs:2], lengths[2:2 + 2 * pairs:2]
    margin = jnp.minimum(giver - 1, limit - receiver)
    shifted = jax.random.randint(jax.random.fold_in(own_key, 1), (pairs,), 0, 1 << 20) % (margin + 1)
    lengths = lengths.at[1:1 + 2 * pairs:2].set(giver - shifted).at[2:2 + 2 * pairs:2].set(receiver + shifted)
    return lengths[jax.random.permutation(jax.random.fold_in(own_key, 2), amount)]


def scatter_about(stream_key, extent, width, bound, shards=(), kind=jnp.bfloat16):
    values = jax.random.normal(stream_key, extent, jnp.float32) * width
    if len(shards) > 0:
        values = level_of(stream_key, extent, shards, -0.22, 0.18) * values
    return jnp.clip(values, min=-bound, max=bound).astype(kind)


def setup_inputs(seed: int = 0) -> dict:
    keys = jax.random.split(jax.random.key(seed), 9)
    return {
        "hidden": draw_hidden(jax.random.fold_in(keys[8], 71), 0),
        "w_query": scatter_about(keys[1], (D, HEADS * HEAD_DIM), D ** -0.5, 0.09375, ((1, 4),)),
        "w_key": scatter_about(keys[2], (D, KV_HEADS * HEAD_DIM), D ** -0.5, 0.09375, ((1, 4),)),
        "w_value": scatter_about(keys[3], (D, KV_HEADS * HEAD_DIM), D ** -0.5, 0.09375, ((1, 4),)),
        "cached_key": scatter_about(keys[4], (TOKENS, KV_HEADS * HEAD_DIM), 1.0, 6.0, ((0, 8), (1, 4))),
        "cached_value": scatter_about(keys[5], (TOKENS, KV_HEADS * HEAD_DIM), 1.0, 6.0, ((0, 8), (1, 4))),
        "doc_lengths": ragged_sizes(keys[6], DOCS, TOKENS, DOC_MOST, 2).astype(jnp.int32),
        "selected": draw_selected(jax.random.fold_in(keys[8], 71), 0),
    }


def doc_numbers(positions, doc_lengths):
    boundary = jnp.cumsum(doc_lengths).astype(jnp.int32)
    return jnp.sum((positions[:, None] >= boundary[None, :]).astype(jnp.int32), axis=1).astype(jnp.int32)


def reference(hidden, w_query, w_key, w_value, cached_key, cached_value, doc_lengths, selected):
    group_size = HEADS // KV_HEADS
    scaling = HEAD_DIM ** -0.5
    key_fresh = jnp.dot(hidden, w_key, preferred_element_type=jnp.float32)
    value_fresh = jnp.dot(hidden, w_value, preferred_element_type=jnp.float32)
    key_shift = key_fresh - cached_key.astype(jnp.float32)
    value_shift = value_fresh - cached_value.astype(jnp.float32)
    deviation = jnp.sum(key_shift * key_shift, axis=1) + jnp.sum(value_shift * value_shift, axis=1)
    positions = jnp.arange(TOKENS, dtype=jnp.int32)
    doc_of = doc_numbers(positions, doc_lengths)
    doc_table = (doc_of[:, None] == jnp.arange(DOCS, dtype=jnp.int32)[None, :]).astype(jnp.float32)
    doc_total = jnp.dot(deviation, doc_table, precision=lax.Precision.HIGHEST)
    doc_mean = doc_total / doc_lengths.astype(jnp.float32)
    score = deviation / (jnp.dot(doc_table, doc_mean, precision=lax.Precision.HIGHEST) + 1.0)
    picked = (jnp.arange(SELECTED, dtype=jnp.int32) // SEL_DEV) * TOK_DEV + selected.astype(jnp.int32)
    chosen = jnp.zeros((TOKENS,), jnp.int32).at[picked].set(1) > 0
    key_used = jnp.where(chosen[:, None], key_fresh.astype(jnp.bfloat16), cached_key)
    value_used = jnp.where(chosen[:, None], value_fresh.astype(jnp.bfloat16), cached_value)
    queries = jnp.dot(hidden[picked], w_query, preferred_element_type=jnp.float32).astype(jnp.bfloat16)
    allowed = positions[None, :] <= picked[:, None]
    query_heads = queries.astype(jnp.float32).reshape(SELECTED, HEADS, HEAD_DIM)

    def one_head(head_number):
        query_head = lax.dynamic_index_in_dim(query_heads, head_number, 1, keepdims=False)
        shared = (head_number // group_size).astype(jnp.int32)
        key_head = lax.dynamic_slice_in_dim(key_used, shared * HEAD_DIM, HEAD_DIM, 1).astype(jnp.float32)
        value_head = lax.dynamic_slice_in_dim(value_used, shared * HEAD_DIM, HEAD_DIM, 1).astype(jnp.float32)
        scores = jnp.dot(query_head, key_head.T, precision=lax.Precision.HIGHEST) * scaling
        scores = jnp.where(allowed, scores, -1e30)
        row_max = jnp.max(scores, axis=1, keepdims=True)
        weights = jnp.where(allowed, jnp.exp(scores - row_max), 0.0)
        row_sum = jnp.sum(weights, axis=1, keepdims=True)
        rounded = lax.optimization_barrier(weights.astype(jnp.bfloat16))
        mixed = jnp.dot(rounded.astype(jnp.float32), value_head, precision=lax.Precision.HIGHEST)
        return mixed / row_sum

    heads_out = lax.map(one_head, jnp.arange(HEADS, dtype=jnp.int32))
    attended = jnp.transpose(heads_out, (1, 0, 2)).reshape(SELECTED, HEADS * HEAD_DIM).astype(jnp.bfloat16)
    return attended, score
```

```python
import functools
import math

import jax
import jax.numpy as jnp
from jax import lax
from jax.experimental import pallas as pl
from jax.experimental.pallas import tpu as pltpu
from jax.sharding import PartitionSpec as P

HEADS = 32
KV_HEADS = 8
HEAD_DIM = 128
GROUP = HEADS // KV_HEADS
EXP_SCALE = HEAD_DIM ** (-0.5) * math.log2(math.e)
MESH = pl.DeviceIdType.MESH
NT = (((1,), (1,)), ((), ()))
LANES = 128
EXTRA = 16
HID_CHUNKS = 4


def round_up(a, b):
    return -(-a // b) * b


def kernel(
    n, kz, docs, sel_rows,
    hid_hbm, wq_hbm, wk_hbm, wv_hbm, ck_hbm, cv_hbm, lens_ref, sel_ref,
    out_ref, score_ref,
    hid, wq, wk, wv, ck, cv, hq, kbuf, vbuf, qbuf, pout, pout_stat, pin, pin_stat,
    m_ref, acc_ref, bias_ref, chosen_ref, dev_ref, devbuf, docbuf,
    load_sem, q_send, q_recv, p_send, p_recv, kv_send, kv_recv, z_send, z_recv, doc_send, doc_recv,
):
    tok, width = hid.shape
    heads = wk.shape[1] // HEAD_DIM
    pad = hq.shape[0]
    qrows = GROUP * pad
    qcols = GROUP * HEAD_DIM
    chips = n // 2
    me = lax.axis_index("seq")
    zme = lax.axis_index("kvh")
    core = me % 2
    chip = me // 2
    partner = me + 1 - 2 * core
    step = width // HID_CHUNKS

    def load(src, dst, sem):
        copy = pltpu.make_async_copy(src, dst, load_sem.at[sem])
        copy.start()
        return copy

    hid_loads, wq_loads = [], []
    for c in range(HID_CHUNKS):
        part = pl.ds(c * step, step)
        hid_loads.append(load(hid_hbm.at[:, part], hid.at[:, part], c))
        wq_loads.append(
            load(
                wq_hbm.at[part, pl.ds(0, qcols)], wq.at[part, pl.ds(0, qcols)], HID_CHUNKS + c
            )
        )
    base = 2 * HID_CHUNKS
    ck_load = load(ck_hbm, ck, base)
    rest_loads = [
        load(
            wq_hbm.at[:, pl.ds(h * qcols, qcols)], wq.at[:, pl.ds(h * qcols, qcols)], base + 3 + h
        )
        for h in range(1, heads)
    ]
    wk_load = load(wk_hbm, wk, base + 1)
    cv_load = load(cv_hbm, cv, base + 2)
    wv_load = load(wv_hbm, wv, base + 3)

    barrier = pltpu.get_barrier_semaphore()
    for d in range(1, n):
        pl.semaphore_signal(barrier, inc=1, device_id={"seq": (me + d) % n}, device_id_type=MESH)
    for d in range(1, kz):
        pl.semaphore_signal(barrier, inc=1, device_id={"kvh": (zme + d) % kz}, device_id_type=MESH)

    slot = lax.broadcasted_iota(jnp.int32, (8, pad), 1)

    def place(r, row):
        return jnp.where(slot == r, sel_ref[me * sel_rows + r], row)

    row_pos = lax.fori_loop(0, sel_rows, place, jnp.full((8, pad), -1, jnp.int32), unroll=8)[0:1]
    row_col = jnp.broadcast_to(row_pos.astype(jnp.float32), (LANES, pad)).T
    lane = lax.broadcasted_iota(jnp.int32, (pad, LANES), 1).astype(jnp.float32)
    pick = jnp.concatenate(
        [
            jnp.where(row_col == lane + float(k * LANES), 1.0, 0.0).astype(jnp.bfloat16)
            for k in range(tok // LANES)
        ],
        axis=1,
    )
    key_row = lax.broadcasted_iota(jnp.int32, (tok, pad), 0)
    pick_t = jnp.where(key_row == row_pos, 1.0, 0.0).astype(jnp.bfloat16)
    chosen_ref[...] = jnp.dot(
        pick_t, jnp.ones((pad, LANES), jnp.bfloat16), preferred_element_type=jnp.float32
    )
    bias_ref[...] = jnp.where(key_row <= row_pos, 0.0, -1e30)
    for h in range(heads):
        vbuf[core, h, HEAD_DIM:, :] = jnp.ones((EXTRA, tok), jnp.bfloat16)

    def q_copy(src, h, dest):
        view = qbuf.at[src, h]
        return pltpu.make_async_remote_copy(
            src_ref=view, dst_ref=view, send_sem=q_send.at[dest // 2, h],
            recv_sem=q_recv.at[src, h], device_id={"seq": dest}, device_id_type=MESH,
        )

    def send_queries(h, queries):
        scaled = (queries * EXP_SCALE).astype(jnp.bfloat16)
        for g in range(GROUP):
            qbuf[chip, h, g * pad:(g + 1) * pad, :] = scaled[:, g * HEAD_DIM:(g + 1) * HEAD_DIM]

        def send(s, carry):
            q_copy(chip, h, (chip - 1 - s) * 2 + core).start()
            return carry

        lax.fori_loop(0, chip, send, 0)

    queries = jnp.zeros((pad, qcols), jnp.float32)
    for c in range(HID_CHUNKS):
        part = slice(c * step, (c + 1) * step)
        hid_loads[c].wait()
        picked = jnp.dot(pick, hid[:, part], preferred_element_type=jnp.float32)
        picked = picked.astype(jnp.bfloat16)
        hq[:, part] = picked
        wq_loads[c].wait()
        queries = queries + jnp.dot(picked, wq[part, 0:qcols], preferred_element_type=jnp.float32)
    pl.semaphore_wait(barrier, n - 1 + kz - 1)
    send_queries(0, queries)
    for h in range(1, heads):
        rest_loads[h - 1].wait()
        send_queries(
            h,
            jnp.dot(
                hq[...], wq[:, h * qcols:(h + 1) * qcols], preferred_element_type=jnp.float32
            ),
        )

    def kv_copy(arr, which):
        view = (kbuf, vbuf)[arr].at[which]
        return pltpu.make_async_remote_copy(
            src_ref=view, dst_ref=view, send_sem=kv_send.at[arr], recv_sem=kv_recv.at[arr],
            device_id={"seq": partner}, device_id_type=MESH,
        )

    pieces = 2 if tok % (2 * LANES) == 0 else 1
    half = tok // pieces

    def fold(shift):
        square = shift * shift
        folded = square[:, 0:HEAD_DIM]
        for h in range(1, heads):
            folded = folded + square[:, h * HEAD_DIM:(h + 1) * HEAD_DIM]
        return jnp.sum(folded.T, axis=0, keepdims=True)

    ck_load.wait()
    wk_load.wait()
    key_dev = []
    for p in range(pieces):
        rows = slice(p * half, (p + 1) * half)
        fresh = jnp.dot(hid[rows, :], wk[...], preferred_element_type=jnp.float32)
        cached = ck[rows, :].astype(jnp.float32)
        key_dev.append(fold(fresh - cached))
        mask = jnp.concatenate([chosen_ref[rows, :]] * heads, axis=1) > 0.5
        used = jnp.where(mask, fresh, cached).astype(jnp.bfloat16)
        for h in range(heads):
            kbuf[core, h, rows, :] = used[:, h * HEAD_DIM:(h + 1) * HEAD_DIM]
    kv_copy(0, core).start()
    cv_load.wait()
    wv_load.wait()
    for p in range(pieces):
        rows = slice(p * half, (p + 1) * half)
        fresh = jnp.dot(hid[rows, :], wv[...], preferred_element_type=jnp.float32)
        cached = cv[rows, :].astype(jnp.float32)
        total = key_dev[p] + fold(fresh - cached)
        dev_ref[:, rows] = jnp.broadcast_to(total, (8, half))
        mask = jnp.concatenate([chosen_ref[rows, :]] * heads, axis=1) > 0.5
        used = jnp.where(mask, fresh, cached).T.astype(jnp.bfloat16)
        for h in range(heads):
            vbuf[core, h, 0:HEAD_DIM, rows] = used[h * HEAD_DIM:(h + 1) * HEAD_DIM, :]
    kv_copy(1, core).start()
    devbuf[zme] = dev_ref[...]
    sends = []
    for d in range(1, kz):
        sends.append(
            pltpu.make_async_remote_copy(
                src_ref=devbuf.at[zme], dst_ref=devbuf.at[zme], send_sem=z_send.at[d - 1],
                recv_sem=z_recv.at[zme], device_id={"kvh": (zme + d) % kz}, device_id_type=MESH,
            )
        )
        sends[-1].start()

    cols = 2 * LANES if qrows % (2 * LANES) == 0 else LANES
    col_parts = [slice(j, j + cols) for j in range(0, qrows, cols)]

    def run(items):
        def scores_of(item):
            src, h, block, part, masked, _ = item
            s = lax.dot_general(
                kbuf[block, h], qbuf[src, h, part, :], NT, preferred_element_type=jnp.float32
            )
            if masked:
                first = part.start % pad
                if cols <= pad:
                    bias = bias_ref[:, first:first + cols]
                else:
                    bias = jnp.concatenate([bias_ref[...]] * (cols // pad), axis=1)
                s = s + bias
            return s

        scores = scores_of(items[0])
        for i, (src, h, block, part, masked, sink) in enumerate(items):
            following = scores_of(items[i + 1]) if i + 1 < len(items) else None
            best = jnp.max(scores, axis=0, keepdims=True)
            weights = jnp.exp2(scores - best).astype(jnp.bfloat16)
            mixed = jnp.dot(vbuf[block, h], weights, preferred_element_type=jnp.float32)
            sink(best, mixed)
            scores = following

    def merge(a, b):
        best = jnp.maximum(a[0], b[0])
        return best, a[1] * jnp.exp2(a[0] - best) + b[1] * jnp.exp2(b[0] - best)

    def first_sink(h, part):
        def sink(best, mixed):
            m_ref[h, 0:1, part] = best
            acc_ref[h, :, part] = mixed
        return sink

    def more_sink(h, part):
        def sink(best, mixed):
            best, mixed = merge((m_ref[h, 0:1, part], acc_ref[h, :, part]), (best, mixed))
            m_ref[h, 0:1, part] = best
            acc_ref[h, :, part] = mixed
        return sink

    run([(chip, h, core, part, True, first_sink(h, part)) for h in range(heads) for part in col_parts])
    kv_copy(0, 1 - core).wait_recv()
    kv_copy(1, 1 - core).wait_recv()

    @pl.when(core == 1)
    def _():
        run(
            [
                (chip, h, 0, part, False, more_sink(h, part))
                for h in range(heads)
                for part in col_parts
            ]
        )

    for d in range(1, kz):
        src = (zme + d) % kz
        pltpu.make_async_remote_copy(
            src_ref=devbuf.at[src], dst_ref=devbuf.at[src], send_sem=z_send.at[0],
            recv_sem=z_recv.at[src], device_id={"kvh": src}, device_id_type=MESH,
        ).wait_recv()
    deviation = devbuf[0]
    for z in range(1, kz):
        deviation = deviation + devbuf[z]
    deviation = deviation[0:1]
    position = lax.broadcasted_iota(jnp.int32, (1, tok), 1) + me * tok
    inside = []
    end = jnp.int32(0)
    for d in range(docs):
        begin, end = end, end + lens_ref[d]
        inside.append((position >= begin) & (position < end))
    slot_row = lax.broadcasted_iota(jnp.int32, docbuf.shape[1:], 0)
    shares = jnp.zeros(docbuf.shape[1:], jnp.float32)
    for d in range(docs):
        share = jnp.sum(jnp.where(inside[d], deviation, 0.0), axis=1, keepdims=True)
        shares = jnp.where(slot_row == d, share, shares)
    docbuf[me] = shares
    for d in range(1, n):
        sends.append(
            pltpu.make_async_remote_copy(
                src_ref=docbuf.at[me], dst_ref=docbuf.at[me], send_sem=doc_send.at[d - 1],
                recv_sem=doc_recv.at[me], device_id={"seq": (me + d) % n}, device_id_type=MESH,
            )
        )
        sends[-1].start()

    def p_copies(src_chip, h, dest_chip):
        dest = {"seq": dest_chip * 2 + core}
        return [
            pltpu.make_async_remote_copy(
                src_ref=pout.at[dest_chip, h], dst_ref=pin.at[src_chip, h],
                send_sem=p_send.at[dest_chip, h, 0], recv_sem=p_recv.at[src_chip, h, 0],
                device_id=dest, device_id_type=MESH,
            ),
            pltpu.make_async_remote_copy(
                src_ref=pout_stat.at[dest_chip, h], dst_ref=pin_stat.at[src_chip, h],
                send_sem=p_send.at[dest_chip, h, 1], recv_sem=p_recv.at[src_chip, h, 1],
                device_id=dest, device_id_type=MESH,
            ),
        ]

    above = chips - 1 - chip
    stat_row = lax.broadcasted_iota(jnp.int32, (8, cols), 0)

    def serve(i, carry):
        h = i // above
        src = chip + 1 + i % above
        q_copy(src, h, me).wait_recv()
        held = {}

        def keep(part):
            def sink(best, mixed):
                held[part.start] = (best, mixed)
            return sink

        def finish(part):
            def sink(best, mixed):
                best, mixed = merge(held[part.start], (best, mixed))
                pout[src, h, :, part] = mixed[0:HEAD_DIM].astype(jnp.bfloat16)
                pout_stat[src, h, :, part] = jnp.where(
                    stat_row == 0, best, mixed[HEAD_DIM:HEAD_DIM + 8]
                )
            return sink

        items = []
        for part in col_parts:
            items.append((src, h, 0, part, False, keep(part)))
            items.append((src, h, 1, part, False, finish(part)))
        run(items)
        for copy in p_copies(chip, h, src):
            copy.start()
        return carry

    lax.fori_loop(0, heads * above, serve, 0)

    for d in range(1, n):
        src = (me + d) % n
        pltpu.make_async_remote_copy(
            src_ref=docbuf.at[src], dst_ref=docbuf.at[src], send_sem=doc_send.at[0],
            recv_sem=doc_recv.at[src], device_id={"seq": src}, device_id_type=MESH,
        ).wait_recv()
    totals = docbuf[0]
    for s in range(1, n):
        totals = totals + docbuf[s]
    mean = jnp.zeros((1, tok), jnp.float32)
    for d in range(docs):
        here = totals[d:d + 1, 0:1] / lens_ref[d].astype(jnp.float32)
        mean = jnp.where(inside[d], here, mean)
    score_ref[...] = deviation / (mean + 1.0)

    def gather(i, carry):
        src = chip - 1 - i // heads
        h = i % heads
        for copy in p_copies(src, h, chip):
            copy.wait_recv()
        best = m_ref[h, 0:1, :]
        other = pin_stat[src, h, 0:1, :]
        top = jnp.maximum(best, other)
        fade, rise = jnp.exp2(best - top), jnp.exp2(other - top)
        m_ref[h, 0:1, :] = top
        acc_ref[h, 0:HEAD_DIM, :] = (
            acc_ref[h, 0:HEAD_DIM, :] * fade + pin[src, h].astype(jnp.float32) * rise
        )
        acc_ref[h, HEAD_DIM:HEAD_DIM + 1, :] = (
            acc_ref[h, HEAD_DIM:HEAD_DIM + 1, :] * fade + pin_stat[src, h, 1:2, :] * rise
        )
        return carry

    lax.fori_loop(0, chip * heads, gather, 0)

    for h in range(heads):
        done = acc_ref[h, 0:HEAD_DIM, :] / acc_ref[h, HEAD_DIM:HEAD_DIM + 1, :]
        for g in range(GROUP):
            head = h * GROUP + g
            block = done[:, g * pad:(g + 1) * pad].T.astype(jnp.bfloat16)
            out_ref[:, head * HEAD_DIM:(head + 1) * HEAD_DIM] = block[0:sel_rows]

    for send in sends:
        send.wait_send()
    for arr in (0, 1):
        kv_copy(arr, core).wait_send()

    def drain_q(i, carry):
        q_copy(chip, i % heads, (i // heads) * 2 + core).wait_send()
        return carry

    lax.fori_loop(0, chip * heads, drain_q, 0)

    def drain_p(i, carry):
        for copy in p_copies(chip, i % heads, chip + 1 + i // heads):
            copy.wait_send()
        return carry

    lax.fori_loop(0, above * heads, drain_p, 0)


def shards(n, kz, hidden, w_query, w_key, w_value, cached_key, cached_value, doc_lengths, selected):
    tok, width = hidden.shape
    cols = w_key.shape[1]
    qcols = w_query.shape[1]
    sel_rows = selected.shape[0] // n
    docs = doc_lengths.shape[0]
    pad = round_up(sel_rows, LANES)
    heads = cols // HEAD_DIM
    qrows = GROUP * pad
    chips = n // 2
    bf, f32 = jnp.bfloat16, jnp.float32
    dma = pltpu.SemaphoreType.DMA
    any_space = pl.BlockSpec(memory_space=pl.ANY)
    vmem = pl.BlockSpec(memory_space=pltpu.VMEM)
    smem = pl.BlockSpec(memory_space=pltpu.SMEM)
    attended, score = pl.pallas_call(
        functools.partial(kernel, n, kz, docs, sel_rows),
        out_shape=(
            jax.ShapeDtypeStruct((sel_rows, qcols), bf),
            jax.ShapeDtypeStruct((1, tok), f32),
        ),
        in_specs=[any_space] * 6 + [smem] * 2,
        out_specs=(vmem, vmem),
        scratch_shapes=[
            pltpu.VMEM((tok, width), bf),
            pltpu.VMEM((width, qcols), bf),
            pltpu.VMEM((width, cols), bf),
            pltpu.VMEM((width, cols), bf),
            pltpu.VMEM((tok, cols), bf),
            pltpu.VMEM((tok, cols), bf),
            pltpu.VMEM((pad, width), bf),
            pltpu.VMEM((2, heads, tok, HEAD_DIM), bf),
            pltpu.VMEM((2, heads, HEAD_DIM + EXTRA, tok), bf),
            pltpu.VMEM((chips, heads, qrows, HEAD_DIM), bf),
            pltpu.VMEM((chips, heads, HEAD_DIM, qrows), bf),
            pltpu.VMEM((chips, heads, 8, qrows), f32),
            pltpu.VMEM((chips, heads, HEAD_DIM, qrows), bf),
            pltpu.VMEM((chips, heads, 8, qrows), f32),
            pltpu.VMEM((heads, 8, qrows), f32),
            pltpu.VMEM((heads, HEAD_DIM + EXTRA, qrows), f32),
            pltpu.VMEM((tok, pad), f32),
            pltpu.VMEM((tok, LANES), f32),
            pltpu.VMEM((8, tok), f32),
            pltpu.VMEM((kz, 8, tok), f32),
            pltpu.VMEM((n, round_up(docs, 8), 128), f32),
            dma((2 * HID_CHUNKS + 3 + heads,)),
            dma((chips, heads)),
            dma((chips, heads)),
            dma((chips, heads, 2)),
            dma((chips, heads, 2)),
            dma((2,)),
            dma((2,)),
            dma((max(1, kz - 1),)),
            dma((kz,)),
            dma((n - 1,)),
            dma((n,)),
        ],
        compiler_params=pltpu.CompilerParams(
            collective_id=0, has_side_effects=True, vmem_limit_bytes=62 * 1024 * 1024
        ),
        name="blend",
    )(hidden, w_query, w_key, w_value, cached_key, cached_value, doc_lengths, selected)
    return attended, score.reshape(tok)


def solution(mesh):
    return jax.shard_map(
        functools.partial(shards, mesh.shape["seq"], mesh.shape["kvh"]),
        mesh=mesh,
        in_specs=(
            P("seq", None),
            P(None, "kvh"),
            P(None, "kvh"),
            P(None, "kvh"),
            P("seq", "kvh"),
            P("seq", "kvh"),
            P(),
            P(),
        ),
        out_specs=(P("seq", "kvh"), P("seq")),
        check_vma=False,
    )
```

```python
import functools
import math

import jax
import jax.numpy as jnp
from jax import lax
from jax.experimental import pallas as pl
from jax.experimental.pallas import tpu as pltpu
from jax.sharding import PartitionSpec as P

HEADS = 32
KV_HEADS = 8
HEAD_DIM = 128
GROUP = HEADS // KV_HEADS
EXP_SCALE = HEAD_DIM ** (-0.5) * math.log2(math.e)
MESH = pl.DeviceIdType.MESH
NT = (((1,), (1,)), ((), ()))
LANES = 128
EXTRA = 16
HID_CHUNKS = 4


def round_up(a, b):
    return -(-a // b) * b


def split_chips(chips):
    small = max(a for a in range(1, math.isqrt(chips) + 1) if chips % a == 0)
    return small, chips // small


def kernel(
    n, kz, docs, sel_rows,
    hid_hbm, wq_hbm, wk_hbm, wv_hbm, ck_hbm, cv_hbm, lens_hbm, sel_hbm,
    out_ref, score_ref,
    hid, wq, wk, wv, ck, cv, hq, kall, vall, ksend, vsend, qbuf, pout, pout_stat, pin, pin_stat,
    m_ref, acc_ref, bias_ref, chosen_ref, last_ref, devbuf, docbuf, lens_ref, sel_ref,
    load_sem, q_send, q_recv, p_send, p_recv, mv_send, mv_recv, fw_send, fw_recv,
    z_send, z_recv, doc_send, doc_recv,
):
    tok, width = hid.shape
    heads = wk.shape[1] // HEAD_DIM
    pad = hq.shape[0]
    qrows = GROUP * pad
    qcols = GROUP * HEAD_DIM
    plain = tok - sel_rows
    cut = plain // LANES * LANES
    spans = ((0, cut), (cut, tok - cut), (0, tok))
    rows_a, rows_b = split_chips(n // 2)
    me = lax.axis_index("seq")
    zme = lax.axis_index("kvh")
    core = me % 2
    chip = me // 2
    ia, ib = chip // rows_b, chip % rows_b
    partner = me + 1 - 2 * core
    step = width // HID_CHUNKS
    barrier = pltpu.get_barrier_semaphore()
    for d in range(1, n):
        pl.semaphore_signal(barrier, inc=1, device_id={"seq": (me + d) % n}, device_id_type=MESH)
    for d in range(1, kz):
        pl.semaphore_signal(barrier, inc=1, device_id={"kvh": (zme + d) % kz}, device_id_type=MESH)

    loads = []

    def load(src, dst):
        copy = pltpu.make_async_copy(src, dst, load_sem.at[len(loads)])
        copy.start()
        loads.append(copy)
        return copy

    sel_load = load(sel_hbm, sel_ref)
    lens_load = load(lens_hbm, lens_ref)
    ck_load = load(ck_hbm, ck)
    cv_load = load(cv_hbm, cv)
    hid_loads, wq_loads = [], []
    for c in range(HID_CHUNKS):
        part = pl.ds(c * step, step)
        hid_loads.append(load(hid_hbm.at[:, part], hid.at[:, part]))
        wq_loads.append(load(wq_hbm.at[part, pl.ds(0, qcols)], wq.at[part, pl.ds(0, qcols)]))
    rest_loads = [
        load(wq_hbm.at[:, pl.ds(h * qcols, qcols)], wq.at[:, pl.ds(h * qcols, qcols)])
        for h in range(1, heads)
    ]
    wk_load = load(wk_hbm, wk)
    wv_load = load(wv_hbm, wv)

    def axes(h):
        if h % 2 == 0:
            return ib, rows_b, ia, rows_a
        return ia, rows_a, ib, rows_b

    def chip_at(h, q, k):
        return k * rows_b + q if h % 2 == 0 else q * rows_b + k

    def sends_kv(h, to):
        qc, nq, kc, nk = axes(h)
        if h % 2 == 0:
            return to > kc
        return (to != kc) & ((qc < nq - 1) | (to > kc))

    def takes_kv(h, source):
        qc, nq, kc, nk = axes(h)
        if h % 2 == 0:
            return source < kc
        return (source != kc) & ((qc < nq - 1) | (source < kc))

    def sends_q(h, to):
        qc, nq, kc, nk = axes(h)
        if h % 2 == 0:
            return (to != qc) & ((to < qc) | (kc > 0))
        return to < qc

    def takes_q(h, source):
        qc, nq, kc, nk = axes(h)
        if h % 2 == 0:
            return (source != qc) & ((source > qc) | (kc > 0))
        return source > qc

    def each(count, want, body):
        def go(i, carry):
            pl.when(want(i))(functools.partial(body, i))
            return carry
        lax.fori_loop(0, count, go, 0)

    def block(arr, h, slot, which, span):
        first, rows = spans[span]
        if arr == 0:
            return kall.at[h, slot, which, pl.ds(first, rows)]
        return vall.at[h, slot, which, pl.ds(0, HEAD_DIM), pl.ds(first, rows)]

    def move(arr, h, span, to):
        qc, nq, kc, nk = axes(h)
        first, rows = spans[span]
        src = ksend.at[h, pl.ds(first, rows)] if arr == 0 else vsend.at[h, :, pl.ds(first, rows)]
        return pltpu.make_async_remote_copy(
            src_ref=src, dst_ref=block(arr, h, kc, core, span),
            send_sem=mv_send.at[h, to, span, arr], recv_sem=mv_recv.at[h, kc, span, arr],
            device_id={"seq": chip_at(h, qc, to) * 2 + core}, device_id_type=MESH,
        )

    def moved(arr, h, span, source):
        view = block(arr, h, source, core, span)
        return pltpu.make_async_remote_copy(
            src_ref=view, dst_ref=view, send_sem=mv_send.at[h, source, span, arr],
            recv_sem=mv_recv.at[h, source, span, arr],
            device_id={"seq": partner}, device_id_type=MESH,
        )

    def forward(arr, h, slot, which, span):
        view = block(arr, h, slot, which, span)
        return pltpu.make_async_remote_copy(
            src_ref=view, dst_ref=view, send_sem=fw_send.at[h, slot, span % 2, arr],
            recv_sem=fw_recv.at[h, slot, span % 2, arr],
            device_id={"seq": partner}, device_id_type=MESH,
        )

    def send_blocks(span):
        for h in range(heads):
            def go(to, h=h):
                for arr in (0, 1):
                    move(arr, h, span, to).start()
            each(axes(h)[3], functools.partial(sends_kv, h), go)

    def forward_blocks(span):
        for h in range(heads):
            def go(source, h=h):
                for arr in (0, 1):
                    moved(arr, h, span, source).wait_recv()
                    forward(arr, h, source, core, span).start()
            each(axes(h)[3], functools.partial(takes_kv, h), go)

    for h in range(heads):
        for i in range(kall.shape[1]):
            for c in range(2):
                vall[h, i, c, HEAD_DIM:, :] = jnp.ones((EXTRA, tok), jnp.bfloat16)
        for j in range(m_ref.shape[1]):
            m_ref[h, j] = jnp.full(m_ref.shape[2:], -1e30, jnp.float32)
            acc_ref[h, j] = jnp.zeros(acc_ref.shape[2:], jnp.float32)

    slot = lax.broadcasted_iota(jnp.int32, (8, pad), 1)
    sel_load.wait()

    def place(r, row):
        return jnp.where(slot == r, sel_ref[me * sel_rows + r], row)

    row_pos = lax.fori_loop(0, sel_rows, place, jnp.full((8, pad), -1, jnp.int32), unroll=8)[0:1]
    row_col = jnp.broadcast_to(row_pos.astype(jnp.float32), (LANES, pad)).T
    lane = lax.broadcasted_iota(jnp.int32, (pad, LANES), 1).astype(jnp.float32)
    pick = jnp.concatenate(
        [
            jnp.where(row_col == lane + float(k * LANES), 1.0, 0.0).astype(jnp.bfloat16)
            for k in range(tok // LANES)
        ],
        axis=1,
    )
    key_row = lax.broadcasted_iota(jnp.int32, (tok, pad), 0)
    pick_t = jnp.where(key_row == row_pos, 1.0, 0.0).astype(jnp.bfloat16)
    chosen_ref[...] = jnp.dot(
        pick_t, jnp.ones((pad, LANES), jnp.bfloat16), preferred_element_type=jnp.float32
    )
    bias_ref[...] = jnp.where(key_row <= row_pos, 0.0, -1e30)

    chosen = jnp.dot(jnp.ones((16, pad), jnp.bfloat16), pick, preferred_element_type=jnp.float32)
    upper = (
        lax.broadcasted_iota(jnp.int32, (LANES, LANES), 0)
        <= lax.broadcasted_iota(jnp.int32, (LANES, LANES), 1)
    ).astype(jnp.float32).astype(jnp.bfloat16)
    counts, before = [], jnp.zeros((1, 1), jnp.float32)
    for k in range(tok // LANES):
        tile = chosen[:, k * LANES:(k + 1) * LANES].astype(jnp.bfloat16)
        inner = jnp.dot(tile, upper, preferred_element_type=jnp.float32)[0:1]
        counts.append(inner + before)
        before = before + inner[:, LANES - 1:LANES]
    count = jnp.concatenate(counts, axis=1).astype(jnp.int32)
    token = lax.broadcasted_iota(jnp.int32, (1, tok), 1)
    target = jnp.where(chosen[0:1] > 0.5, plain + count - 1, token - count)

    def order(first, rows):
        row = lax.broadcasted_iota(jnp.int32, (rows, tok), 0) + first
        return jnp.where(row == target, 1.0, 0.0).astype(jnp.bfloat16)

    last_ref[...] = order(cut, tok - cut)
    early = order(0, cut)
    ck_load.wait()
    cv_load.wait()
    keys = jnp.dot(early, ck[...], preferred_element_type=jnp.float32).astype(jnp.bfloat16)
    values = jnp.dot(early, cv[...], preferred_element_type=jnp.float32)
    for h in range(heads):
        part = slice(h * HEAD_DIM, (h + 1) * HEAD_DIM)
        ksend[h, 0:cut, :] = keys[:, part]
        vsend[h, :, 0:cut] = values[:, part].T.astype(jnp.bfloat16)

    def q_copy(h, to):
        qc, nq, kc, nk = axes(h)
        view = qbuf.at[h, qc]
        return pltpu.make_async_remote_copy(
            src_ref=view, dst_ref=view, send_sem=q_send.at[h, to], recv_sem=q_recv.at[h, qc],
            device_id={"seq": chip_at(h, to, kc) * 2 + core}, device_id_type=MESH,
        )

    def q_wait(h, source):
        view = qbuf.at[h, source]
        pltpu.make_async_remote_copy(
            src_ref=view, dst_ref=view, send_sem=q_send.at[h, source],
            recv_sem=q_recv.at[h, source], device_id={"seq": partner}, device_id_type=MESH,
        ).wait_recv()

    def send_queries(h, queries):
        qc, nq, kc, nk = axes(h)
        scaled = (queries * EXP_SCALE).astype(jnp.bfloat16)
        for g in range(GROUP):
            qbuf[h, qc, g * pad:(g + 1) * pad, :] = scaled[:, g * HEAD_DIM:(g + 1) * HEAD_DIM]
        each(nq, functools.partial(sends_q, h), lambda to: q_copy(h, to).start())

    queries = jnp.zeros((pad, qcols), jnp.float32)
    for c in range(HID_CHUNKS):
        part = slice(c * step, (c + 1) * step)
        hid_loads[c].wait()
        picked = jnp.dot(pick, hid[:, part], preferred_element_type=jnp.float32)
        picked = picked.astype(jnp.bfloat16)
        hq[:, part] = picked
        wq_loads[c].wait()
        queries = queries + jnp.dot(picked, wq[part, 0:qcols], preferred_element_type=jnp.float32)
        if c == min(1, HID_CHUNKS - 1):
            pl.semaphore_wait(barrier, n - 1 + kz - 1)
            send_blocks(0)
    send_queries(0, queries)
    for h in range(1, heads):
        rest_loads[h - 1].wait()
        send_queries(
            h,
            jnp.dot(
                hq[...], wq[:, h * qcols:(h + 1) * qcols], preferred_element_type=jnp.float32
            ),
        )

    pieces = 2 if tok % (2 * LANES) == 0 else 1
    half = tok // pieces

    def fold(shift):
        square = shift * shift
        folded = square[:, 0:HEAD_DIM]
        for h in range(1, heads):
            folded = folded + square[:, h * HEAD_DIM:(h + 1) * HEAD_DIM]
        return jnp.sum(folded.T, axis=0, keepdims=True)
    wk_load.wait()
    key_dev = []
    for p in range(pieces):
        rows = slice(p * half, (p + 1) * half)
        fresh = jnp.dot(hid[rows, :], wk[...], preferred_element_type=jnp.float32)
        cached = ck[rows, :].astype(jnp.float32)
        key_dev.append(fold(fresh - cached))
        mask = jnp.concatenate([chosen_ref[rows, :]] * heads, axis=1) > 0.5
        used = jnp.where(mask, fresh, cached).astype(jnp.bfloat16)
        for h in range(heads):
            kall[h, axes(h)[2], core, rows, :] = used[:, h * HEAD_DIM:(h + 1) * HEAD_DIM]
    for h in range(heads):
        forward(0, h, axes(h)[2], core, 2).start()
        ksend[h, cut:tok, :] = jnp.dot(
            last_ref[...], kall[h, axes(h)[2], core], preferred_element_type=jnp.float32
        ).astype(jnp.bfloat16)
    wv_load.wait()
    for p in range(pieces):
        rows = slice(p * half, (p + 1) * half)
        fresh = jnp.dot(hid[rows, :], wv[...], preferred_element_type=jnp.float32)
        cached = cv[rows, :].astype(jnp.float32)
        devbuf[zme, :, rows] = key_dev[p] + fold(fresh - cached)
        mask = jnp.concatenate([chosen_ref[rows, :]] * heads, axis=1) > 0.5
        used = jnp.where(mask, fresh, cached).T.astype(jnp.bfloat16)
        for h in range(heads):
            vall[h, axes(h)[2], core, 0:HEAD_DIM, rows] = used[h * HEAD_DIM:(h + 1) * HEAD_DIM, :]
    for h in range(heads):
        forward(1, h, axes(h)[2], core, 2).start()
        vsend[h, :, cut:tok] = lax.dot_general(
            vall[h, axes(h)[2], core, 0:HEAD_DIM, :], last_ref[...], NT,
            preferred_element_type=jnp.float32,
        ).astype(jnp.bfloat16)
    send_blocks(1)
    sends = []
    for d in range(1, kz):
        sends.append(
            pltpu.make_async_remote_copy(
                src_ref=devbuf.at[zme], dst_ref=devbuf.at[zme], send_sem=z_send.at[d - 1],
                recv_sem=z_recv.at[zme], device_id={"kvh": (zme + d) % kz}, device_id_type=MESH,
            )
        )
        sends[-1].start()

    cols = 2 * LANES if qrows % (2 * LANES) == 0 else LANES
    col_parts = [slice(j, j + cols) for j in range(0, qrows, cols)]

    def run(items):
        def scores_of(item):
            h, q, k, which, part, masked = item
            s = lax.dot_general(
                kall[h, k, which], qbuf[h, q, part, :], NT, preferred_element_type=jnp.float32
            )
            if masked:
                first = part.start % pad
                if cols <= pad:
                    bias = bias_ref[:, first:first + cols]
                else:
                    bias = jnp.concatenate([bias_ref[...]] * (cols // pad), axis=1)
                s = s + bias
            return s

        scores = scores_of(items[0])
        for i, (h, q, k, which, part, masked) in enumerate(items):
            following = scores_of(items[i + 1]) if i + 1 < len(items) else None
            best = jnp.max(scores, axis=0, keepdims=True)
            weights = jnp.exp2(scores - best).astype(jnp.bfloat16)
            mixed = jnp.dot(vall[h, k, which], weights, preferred_element_type=jnp.float32)
            if not masked:
                old = m_ref[h, q, 0:1, part]
                top = jnp.maximum(old, best)
                mixed = mixed * jnp.exp2(best - top)
                mixed = mixed + acc_ref[h, q, :, part] * jnp.exp2(old - top)
                best = top
            m_ref[h, q, 0:1, part] = best
            acc_ref[h, q, :, part] = mixed
            scores = following

    def both(h, q, k):
        run([(h, q, k, c, part, False) for part in col_parts for c in (core, 1 - core)])

    def p_copies(h, to):
        qc, nq, kc, nk = axes(h)
        dest = {"seq": chip_at(h, to, kc) * 2 + core}
        return [
            pltpu.make_async_remote_copy(
                src_ref=pout.at[h, to], dst_ref=pin.at[h, qc], send_sem=p_send.at[h, to, 0],
                recv_sem=p_recv.at[h, qc, 0], device_id=dest, device_id_type=MESH,
            ),
            pltpu.make_async_remote_copy(
                src_ref=pout_stat.at[h, to], dst_ref=pin_stat.at[h, qc],
                send_sem=p_send.at[h, to, 1], recv_sem=p_recv.at[h, qc, 1],
                device_id=dest, device_id_type=MESH,
            ),
        ]

    def p_wait(h, source):
        for i, buf in enumerate((pin, pin_stat)):
            view = buf.at[h, source]
            pltpu.make_async_remote_copy(
                src_ref=view, dst_ref=view, send_sem=p_send.at[h, source, i],
                recv_sem=p_recv.at[h, source, i], device_id={"seq": partner}, device_id_type=MESH,
            ).wait_recv()

    def give_back(h, to):
        pout[h, to] = acc_ref[h, to, 0:HEAD_DIM, :].astype(jnp.bfloat16)
        pout_stat[h, to, 0:1, :] = m_ref[h, to, 0:1, :]
        pout_stat[h, to, 1:2, :] = acc_ref[h, to, HEAD_DIM:HEAD_DIM + 1, :]
        for copy in p_copies(h, to):
            copy.start()

    def no_moved(h):
        qc, nq, kc, nk = axes(h)
        return kc == 0 if h % 2 == 0 else nk == 1
    run(
        [
            (h, axes(h)[0], axes(h)[2], core, part, True)
            for h in range(heads)
            for part in col_parts
        ]
    )
    forward_blocks(0)
    for h in range(heads):
        for arr in (0, 1):
            forward(arr, h, axes(h)[2], 1 - core, 2).wait_recv()
    for h in range(heads):
        def serve_own(j, h=h):
            q_wait(h, j)
            both(h, j, axes(h)[2])
            pl.when(no_moved(h))(lambda: give_back(h, j))
        each(axes(h)[1], lambda j, h=h: j > axes(h)[0], serve_own)
    forward_blocks(1)
    @pl.when(core == 1)
    def _():
        run(
            [
                (h, axes(h)[0], axes(h)[2], 0, part, False)
                for h in range(heads)
                for part in col_parts
            ]
        )
    for h in range(heads):
        def arrive(source, h=h):
            for span in (0, 1):
                for arr in (0, 1):
                    forward(arr, h, source, 1 - core, span).wait_recv()
        each(axes(h)[3], functools.partial(takes_kv, h), arrive)
    for h in range(heads):
        qc, nq, kc, nk = axes(h)

        def serve_moved(j, h=h, qc=qc, nk=nk):
            pl.when(j < qc)(lambda: q_wait(h, j))
            each(nk, functools.partial(takes_kv, h), lambda i: both(h, j, i))
            give_back(h, j)

        each(
            nq,
            lambda j, h=h: takes_q(h, j) & jnp.logical_not(no_moved(h)),
            serve_moved,
        )
    for h in range(heads):
        qc, nq, kc, nk = axes(h)
        each(nk, lambda i, kc=kc: i < kc, lambda i, h=h, qc=qc: both(h, qc, i))
    for d in range(1, kz):
        src = (zme + d) % kz
        pltpu.make_async_remote_copy(
            src_ref=devbuf.at[src], dst_ref=devbuf.at[src], send_sem=z_send.at[0],
            recv_sem=z_recv.at[src], device_id={"kvh": src}, device_id_type=MESH,
        ).wait_recv()
    lens_load.wait()
    deviation = devbuf[0]
    for z in range(1, kz):
        deviation = deviation + devbuf[z]
    position = token + me * tok
    inside = []
    end = jnp.int32(0)
    for d in range(docs):
        begin, end = end, end + lens_ref[d]
        inside.append((position >= begin) & (position < end))
    slot_row = lax.broadcasted_iota(jnp.int32, docbuf.shape[1:], 0)
    shares = jnp.zeros(docbuf.shape[1:], jnp.float32)
    for d in range(docs):
        share = jnp.sum(jnp.where(inside[d], deviation, 0.0), axis=1, keepdims=True)
        shares = jnp.where(slot_row == d, share, shares)
    docbuf[me] = shares
    for d in range(1, n):
        sends.append(
            pltpu.make_async_remote_copy(
                src_ref=docbuf.at[me], dst_ref=docbuf.at[me], send_sem=doc_send.at[d - 1],
                recv_sem=doc_recv.at[me], device_id={"seq": (me + d) % n}, device_id_type=MESH,
            )
        )
        sends[-1].start()
    for h in range(heads):
        qc, nq, kc, nk = axes(h)

        def collect(source, h=h, qc=qc):
            p_wait(h, source)
            best = m_ref[h, qc, 0:1, :]
            other = pin_stat[h, source, 0:1, :]
            top = jnp.maximum(best, other)
            fade, rise = jnp.exp2(best - top), jnp.exp2(other - top)
            m_ref[h, qc, 0:1, :] = top
            acc_ref[h, qc, 0:HEAD_DIM, :] = (
                acc_ref[h, qc, 0:HEAD_DIM, :] * fade + pin[h, source].astype(jnp.float32) * rise
            )
            acc_ref[h, qc, HEAD_DIM:HEAD_DIM + 1, :] = (
                acc_ref[h, qc, HEAD_DIM:HEAD_DIM + 1, :] * fade + pin_stat[h, source, 1:2, :] * rise
            )

        each(nq, functools.partial(sends_q, h), collect)
        done = acc_ref[h, qc, 0:HEAD_DIM, :] / acc_ref[h, qc, HEAD_DIM:HEAD_DIM + 1, :]
        for g in range(GROUP):
            head = h * GROUP + g
            rows = done[:, g * pad:(g + 1) * pad].T.astype(jnp.bfloat16)
            out_ref[:, head * HEAD_DIM:(head + 1) * HEAD_DIM] = rows[0:sel_rows]
    for d in range(1, n):
        src = (me + d) % n
        pltpu.make_async_remote_copy(
            src_ref=docbuf.at[src], dst_ref=docbuf.at[src], send_sem=doc_send.at[0],
            recv_sem=doc_recv.at[src], device_id={"seq": src}, device_id_type=MESH,
        ).wait_recv()
    totals = docbuf[0]
    for s in range(1, n):
        totals = totals + docbuf[s]
    mean = jnp.zeros((1, tok), jnp.float32)
    for d in range(docs):
        here = totals[d:d + 1, 0:1] / lens_ref[d].astype(jnp.float32)
        mean = jnp.where(inside[d], here, mean)
    score_ref[...] = deviation / (mean + 1.0)
    for send in sends:
        send.wait_send()
    for h in range(heads):
        qc, nq, kc, nk = axes(h)

        def drain_kv(to, h=h):
            for span in (0, 1):
                for arr in (0, 1):
                    move(arr, h, span, to).wait_send()

        def drain_forward(source, h=h):
            for span in (0, 1):
                for arr in (0, 1):
                    forward(arr, h, source, core, span).wait_send()

        def drain_p(to, h=h):
            for copy in p_copies(h, to):
                copy.wait_send()

        for arr in (0, 1):
            forward(arr, h, kc, core, 2).wait_send()
        each(nk, functools.partial(sends_kv, h), drain_kv)
        each(nk, functools.partial(takes_kv, h), drain_forward)
        each(nq, functools.partial(sends_q, h), lambda to, h=h: q_copy(h, to).wait_send())
        each(nq, functools.partial(takes_q, h), drain_p)


def shards(n, kz, hidden, w_query, w_key, w_value, cached_key, cached_value, doc_lengths, selected):
    tok, width = hidden.shape
    cols = w_key.shape[1]
    qcols = w_query.shape[1]
    sel_rows = selected.shape[0] // n
    docs = doc_lengths.shape[0]
    pad = round_up(sel_rows, LANES)
    heads = cols // HEAD_DIM
    qrows = GROUP * pad
    cut = (tok - sel_rows) // LANES * LANES
    side = max(split_chips(n // 2))
    bf, f32 = jnp.bfloat16, jnp.float32
    dma = pltpu.SemaphoreType.DMA
    any_space = pl.BlockSpec(memory_space=pl.ANY)
    vmem = pl.BlockSpec(memory_space=pltpu.VMEM)
    attended, score = pl.pallas_call(
        functools.partial(kernel, n, kz, docs, sel_rows),
        out_shape=(
            jax.ShapeDtypeStruct((sel_rows, qcols), bf),
            jax.ShapeDtypeStruct((1, tok), f32),
        ),
        in_specs=[any_space] * 8,
        out_specs=(vmem, vmem),
        scratch_shapes=[
            pltpu.VMEM((tok, width), bf),
            pltpu.VMEM((width, qcols), bf),
            pltpu.VMEM((width, cols), bf),
            pltpu.VMEM((width, cols), bf),
            pltpu.VMEM((tok, cols), bf),
            pltpu.VMEM((tok, cols), bf),
            pltpu.VMEM((pad, width), bf),
            pltpu.VMEM((heads, side, 2, tok, HEAD_DIM), bf),
            pltpu.VMEM((heads, side, 2, HEAD_DIM + EXTRA, tok), bf),
            pltpu.VMEM((heads, tok, HEAD_DIM), bf),
            pltpu.VMEM((heads, HEAD_DIM, tok), bf),
            pltpu.VMEM((heads, side, qrows, HEAD_DIM), bf),
            pltpu.VMEM((heads, side, HEAD_DIM, qrows), bf),
            pltpu.VMEM((heads, side, 2, qrows), f32),
            pltpu.VMEM((heads, side, HEAD_DIM, qrows), bf),
            pltpu.VMEM((heads, side, 2, qrows), f32),
            pltpu.VMEM((heads, side, 8, qrows), f32),
            pltpu.VMEM((heads, side, HEAD_DIM + EXTRA, qrows), f32),
            pltpu.VMEM((tok, pad), f32),
            pltpu.VMEM((tok, LANES), f32),
            pltpu.VMEM((tok - cut, tok), bf),
            pltpu.VMEM((kz, 1, tok), f32),
            pltpu.VMEM((n, round_up(docs, 8), 128), f32),
            pltpu.SMEM(doc_lengths.shape, jnp.int32),
            pltpu.SMEM(selected.shape, jnp.int32),
            dma((2 * HID_CHUNKS + 5 + heads,)),
            dma((heads, side)),
            dma((heads, side)),
            dma((heads, side, 2)),
            dma((heads, side, 2)),
            dma((heads, side, 2, 2)),
            dma((heads, side, 2, 2)),
            dma((heads, side, 2, 2)),
            dma((heads, side, 2, 2)),
            dma((max(1, kz - 1),)),
            dma((kz,)),
            dma((n - 1,)),
            dma((n,)),
        ],
        compiler_params=pltpu.CompilerParams(
            collective_id=0, has_side_effects=True, vmem_limit_bytes=62 * 1024 * 1024
        ),
        name="blend",
    )(hidden, w_query, w_key, w_value, cached_key, cached_value, doc_lengths, selected)
    return attended, score.reshape(tok)


def solution(mesh):
    return jax.shard_map(
        functools.partial(shards, mesh.shape["seq"], mesh.shape["kvh"]),
        mesh=mesh,
        in_specs=(
            P("seq", None),
            P(None, "kvh"),
            P(None, "kvh"),
            P(None, "kvh"),
            P("seq", "kvh"),
            P("seq", "kvh"),
            P(),
            P(),
        ),
        out_specs=(P("seq", "kvh"), P("seq")),
        check_vma=False,
    )
```

```python
import functools
import math

import jax
import jax.numpy as jnp
from jax import lax
from jax.experimental import pallas as pl
from jax.experimental.pallas import tpu as pltpu
from jax.sharding import PartitionSpec as P

HEADS = 32
KV_HEADS = 8
HEAD_DIM = 128
GROUP = HEADS // KV_HEADS
EXP_SCALE = HEAD_DIM ** (-0.5) * math.log2(math.e)
MESH = pl.DeviceIdType.MESH
NT = (((1,), (1,)), ((), ()))
LANES = 128
EXTRA = 16
HID_CHUNKS = 4


def round_up(a, b):
    return -(-a // b) * b


def q_cols(rows):
    return 2 * LANES if rows % (2 * LANES) == 0 else LANES


def split_chips(chips):
    small = max(a for a in range(1, math.isqrt(chips) + 1) if chips % a == 0)
    return small, chips // small


def kernel(
    n, kz, docs, sel_rows,
    hid_hbm, wq_hbm, wk_hbm, wv_hbm, ck_hbm, cv_hbm, lens_hbm, sel_hbm,
    out_ref, score_ref,
    hid, wq, wk, wv, ck, cv, hq, kall, vall, ksend, vsend, qbuf, pout, pout_stat, pin, pin_stat,
    kacc, vacc, m_ref, acc_ref, bias_ref, chosen_ref, last_ref, devbuf, docbuf, lens_ref, sel_ref,
    load_sem, q_send, q_recv, p_send, p_recv, mv_send, mv_recv, fw_send, fw_recv, own_send, own_recv,
    z_send, z_recv, doc_send, doc_recv,
):
    tok, width = hid.shape
    heads = wk.shape[1] // HEAD_DIM
    pad = hq.shape[0]
    qrows = GROUP * pad
    qcols = GROUP * HEAD_DIM
    plain = tok - sel_rows
    cut = plain // LANES * LANES
    spans = ((0, cut), (cut, tok - cut), (0, tok))
    rows_a, rows_b = split_chips(n // 2)
    me = lax.axis_index("seq")
    zme = lax.axis_index("kvh")
    core = me % 2
    chip = me // 2
    ia, ib = chip // rows_b, chip % rows_b
    partner = me + 1 - 2 * core
    step = width // HID_CHUNKS
    barrier = pltpu.get_barrier_semaphore()
    for d in range(1, n):
        pl.semaphore_signal(barrier, inc=1, device_id={"seq": (me + d) % n}, device_id_type=MESH)
    for d in range(1, kz):
        pl.semaphore_signal(barrier, inc=1, device_id={"kvh": (zme + d) % kz}, device_id_type=MESH)

    loads = []

    def load(src, dst):
        copy = pltpu.make_async_copy(src, dst, load_sem.at[len(loads)])
        copy.start()
        loads.append(copy)
        return copy

    sel_load = load(sel_hbm, sel_ref)
    ck_load = load(ck_hbm, ck)
    cv_load = load(cv_hbm, cv)
    lens_load = load(lens_hbm, lens_ref)
    chunk_loads = []
    for c in range(HID_CHUNKS):
        part = pl.ds(c * step, step)
        chunk_loads.append(
            (
                load(hid_hbm.at[:, part], hid.at[:, part]),
                load(wk_hbm.at[part], wk.at[part]),
                load(wv_hbm.at[part], wv.at[part]),
            )
        )
    head_order = sorted(range(heads), key=lambda h: (1 - h % 2, h))
    wq_loads = {
        h: load(wq_hbm.at[:, pl.ds(h * qcols, qcols)], wq.at[:, pl.ds(h * qcols, qcols)])
        for h in head_order
    }

    def axes(h):
        if h % 2 == 0:
            return ib, rows_b, ia, rows_a
        return ia, rows_a, ib, rows_b

    def chip_at(h, q, k):
        return k * rows_b + q if h % 2 == 0 else q * rows_b + k

    def sends_kv(h, to):
        qc, nq, kc, nk = axes(h)
        if h % 2 == 0:
            return to > kc
        return (to != kc) & ((qc < nq - 1) | (to > kc))

    def takes_kv(h, source):
        qc, nq, kc, nk = axes(h)
        if h % 2 == 0:
            return source < kc
        return (source != kc) & ((qc < nq - 1) | (source < kc))

    def sends_q(h, to):
        qc, nq, kc, nk = axes(h)
        if h % 2 == 0:
            return (to != qc) & ((to < qc) | (kc > 0))
        return to < qc

    def takes_q(h, source):
        qc, nq, kc, nk = axes(h)
        if h % 2 == 0:
            return (source != qc) & ((source > qc) | (kc > 0))
        return source > qc

    def each(count, want, body):
        def go(i, carry):
            pl.when(want(i))(functools.partial(body, i))
            return carry
        lax.fori_loop(0, count, go, 0)

    def block(arr, h, slot, which, span):
        first, rows = spans[span]
        if arr == 0:
            return kall.at[h, slot, which, pl.ds(first, rows)]
        return vall.at[h, slot, which, pl.ds(0, HEAD_DIM), pl.ds(first, rows)]

    def move(arr, h, span, to):
        qc, nq, kc, nk = axes(h)
        first, rows = spans[span]
        src = ksend.at[h, pl.ds(first, rows)] if arr == 0 else vsend.at[h, :, pl.ds(first, rows)]
        return pltpu.make_async_remote_copy(
            src_ref=src, dst_ref=block(arr, h, kc, core, span),
            send_sem=mv_send.at[h, (to - kc - 1) % nk, span, arr],
            recv_sem=mv_recv.at[h, (kc - to - 1) % nk, span, arr],
            device_id={"seq": chip_at(h, qc, to) * 2 + core}, device_id_type=MESH,
        )

    def moved(arr, h, span, source):
        qc, nq, kc, nk = axes(h)
        index = (source - kc - 1) % nk
        view = block(arr, h, source, core, span)
        return pltpu.make_async_remote_copy(
            src_ref=view, dst_ref=view, send_sem=mv_send.at[h, index, span, arr],
            recv_sem=mv_recv.at[h, index, span, arr],
            device_id={"seq": partner}, device_id_type=MESH,
        )

    def forward(arr, h, slot, which, span):
        qc, nq, kc, nk = axes(h)
        view = block(arr, h, slot, which, span)
        if span == 2:
            send_sem, recv_sem = own_send.at[h, arr], own_recv.at[h, arr]
        else:
            index = (slot - kc - 1) % nk
            send_sem, recv_sem = fw_send.at[h, index, span, arr], fw_recv.at[h, index, span, arr]
        return pltpu.make_async_remote_copy(
            src_ref=view, dst_ref=view, send_sem=send_sem, recv_sem=recv_sem,
            device_id={"seq": partner}, device_id_type=MESH,
        )

    def send_blocks(arr, span):
        for h in range(heads):
            def go(to, h=h):
                move(arr, h, span, to).start()
            each(axes(h)[3], functools.partial(sends_kv, h), go)

    def shared_link(h, source):
        qc, nq, kc, nk = axes(h)
        return (source > kc) | (qc == nq - 1)

    def forward_blocks(h, span, want):
        def go(source):
            for arr in (0, 1):
                moved(arr, h, span, source).wait_recv()
                forward(arr, h, source, core, span).start()
        each(axes(h)[3], want, go)

    def arrive(h):
        def go(source):
            for span in (0, 1):
                for arr in (0, 1):
                    forward(arr, h, source, 1 - core, span).wait_recv()
        each(axes(h)[3], functools.partial(takes_kv, h), go)

    for h in range(heads):
        for i in range(kall.shape[1]):
            for c in range(2):
                vall[h, i, c, HEAD_DIM:, :] = jnp.ones((EXTRA, tok), jnp.bfloat16)
        for j in range(m_ref.shape[1]):
            m_ref[h, j] = jnp.full(m_ref.shape[2:], -1e30, jnp.float32)
            acc_ref[h, j] = jnp.zeros(acc_ref.shape[2:], jnp.float32)

    slot = lax.broadcasted_iota(jnp.int32, (8, pad), 1)
    sel_load.wait()

    def place(r, row):
        return jnp.where(slot == r, sel_ref[me * sel_rows + r], row)

    row_pos = lax.fori_loop(0, sel_rows, place, jnp.full((8, pad), -1, jnp.int32), unroll=8)[0:1]
    ck_load.wait()
    cv_load.wait()
    row_col = jnp.broadcast_to(row_pos.astype(jnp.float32), (LANES, pad)).T
    lane = lax.broadcasted_iota(jnp.int32, (pad, LANES), 1).astype(jnp.float32)
    pick = jnp.concatenate(
        [
            jnp.where(row_col == lane + float(k * LANES), 1.0, 0.0).astype(jnp.bfloat16)
            for k in range(tok // LANES)
        ],
        axis=1,
    )
    key_row = lax.broadcasted_iota(jnp.int32, (tok, pad), 0)
    pick_t = jnp.where(key_row == row_pos, 1.0, 0.0).astype(jnp.bfloat16)
    chosen_ref[...] = jnp.dot(
        pick_t, jnp.ones((pad, LANES), jnp.bfloat16), preferred_element_type=jnp.float32
    )
    bias_ref[...] = jnp.where(key_row <= row_pos, 0.0, -1e30)

    chosen = jnp.dot(jnp.ones((16, pad), jnp.bfloat16), pick, preferred_element_type=jnp.float32)
    upper = (
        lax.broadcasted_iota(jnp.int32, (LANES, LANES), 0)
        <= lax.broadcasted_iota(jnp.int32, (LANES, LANES), 1)
    ).astype(jnp.float32).astype(jnp.bfloat16)
    counts, before = [], jnp.zeros((1, 1), jnp.float32)
    for k in range(tok // LANES):
        tile = chosen[:, k * LANES:(k + 1) * LANES].astype(jnp.bfloat16)
        inner = jnp.dot(tile, upper, preferred_element_type=jnp.float32)[0:1]
        counts.append(inner + before)
        before = before + inner[:, LANES - 1:LANES]
    count = jnp.concatenate(counts, axis=1).astype(jnp.int32)
    token = lax.broadcasted_iota(jnp.int32, (1, tok), 1)
    target = jnp.where(chosen[0:1] > 0.5, plain + count - 1, token - count)

    def order(first, rows):
        row = lax.broadcasted_iota(jnp.int32, (rows, tok), 0) + first
        return jnp.where(row == target, 1.0, 0.0).astype(jnp.bfloat16)

    last_ref[...] = order(cut, tok - cut)
    early = order(0, cut)
    keys = jnp.dot(early, ck[...], preferred_element_type=jnp.float32).astype(jnp.bfloat16)
    values = jnp.dot(early, cv[...], preferred_element_type=jnp.float32)
    for h in range(heads):
        part = slice(h * HEAD_DIM, (h + 1) * HEAD_DIM)
        ksend[h, 0:cut, :] = keys[:, part]
        vsend[h, :, 0:cut] = values[:, part].T.astype(jnp.bfloat16)

    cols = q_cols(qrows)
    col_parts = [slice(j, j + cols) for j in range(0, qrows, cols)]

    def q_copy(h, to, index):
        qc, nq, kc, nk = axes(h)
        view = qbuf.at[h, qc, pl.ds(index * cols, cols)]
        return pltpu.make_async_remote_copy(
            src_ref=view, dst_ref=view, send_sem=q_send.at[h, (to - qc - 1) % nq, index],
            recv_sem=q_recv.at[h, (qc - to - 1) % nq, index],
            device_id={"seq": chip_at(h, to, kc) * 2 + core}, device_id_type=MESH,
        )

    def q_wait(h, source, index):
        qc, nq, kc, nk = axes(h)
        place = (source - qc - 1) % nq
        view = qbuf.at[h, source, pl.ds(index * cols, cols)]
        pltpu.make_async_remote_copy(
            src_ref=view, dst_ref=view, send_sem=q_send.at[h, place, index],
            recv_sem=q_recv.at[h, place, index], device_id={"seq": partner}, device_id_type=MESH,
        ).wait_recv()

    def send_queries(h, queries):
        qc, nq, kc, nk = axes(h)
        scaled = (queries * EXP_SCALE).astype(jnp.bfloat16)
        for g in range(GROUP):
            qbuf[h, qc, g * pad:(g + 1) * pad, :] = scaled[:, g * HEAD_DIM:(g + 1) * HEAD_DIM]

        def go(to):
            for index in range(len(col_parts)):
                q_copy(h, to, index).start()

        each(nq, functools.partial(sends_q, h), go)

    pieces = 2 if tok % (2 * LANES) == 0 else 1
    half = tok // pieces

    def fold(shift):
        square = shift * shift
        folded = square[:, 0:HEAD_DIM]
        for h in range(1, heads):
            folded = folded + square[:, h * HEAD_DIM:(h + 1) * HEAD_DIM]
        return jnp.sum(folded.T, axis=0, keepdims=True)

    def project(h):
        return jnp.dot(
            hq[...], wq[:, h * qcols:(h + 1) * qcols], preferred_element_type=jnp.float32
        )

    def project_chunk(c):
        part = slice(c * step, (c + 1) * step)
        for weight, total in ((wk, kacc), (wv, vacc)):
            fresh = jnp.dot(hid[:, part], weight[part, :], preferred_element_type=jnp.float32)
            total[...] = fresh if c == 0 else total[...] + fresh
        picked = jnp.dot(pick, hid[:, part], preferred_element_type=jnp.float32)
        hq[:, part] = picked.astype(jnp.bfloat16)

    for c in range(HID_CHUNKS):
        for copy in chunk_loads[c]:
            copy.wait()
        project_chunk(c)
        if c == 0:
            pl.semaphore_wait(barrier, n - 1 + kz - 1)
            send_blocks(0, 0)
            send_blocks(1, 0)
    wq_loads[head_order[0]].wait()
    queries = project(head_order[0])
    for p in range(pieces):
        rows = slice(p * half, (p + 1) * half)
        cached_k = ck[rows, :].astype(jnp.float32)
        cached_v = cv[rows, :].astype(jnp.float32)
        mask = jnp.concatenate([chosen_ref[rows, :]] * heads, axis=1) > 0.5
        used_k = jnp.where(mask, kacc[rows, :], cached_k).astype(jnp.bfloat16)
        used_v = jnp.where(mask, vacc[rows, :], cached_v).T.astype(jnp.bfloat16)
        for h in range(heads):
            part = slice(h * HEAD_DIM, (h + 1) * HEAD_DIM)
            kall[h, axes(h)[2], core, rows, :] = used_k[:, part]
            vall[h, axes(h)[2], core, 0:HEAD_DIM, rows] = used_v[part, :]
        devbuf[zme, :, rows] = fold(kacc[rows, :] - cached_k) + fold(vacc[rows, :] - cached_v)
    send_queries(head_order[0], queries)
    for h in range(heads):
        for arr in (0, 1):
            forward(arr, h, axes(h)[2], core, 2).start()
    sends = []
    for d in range(1, kz):
        sends.append(
            pltpu.make_async_remote_copy(
                src_ref=devbuf.at[zme], dst_ref=devbuf.at[zme], send_sem=z_send.at[d - 1],
                recv_sem=z_recv.at[kz - d - 1], device_id={"kvh": (zme + d) % kz}, device_id_type=MESH,
            )
        )
        sends[-1].start()
    for h in head_order[1:]:
        wq_loads[h].wait()
    others = [project(h) for h in head_order[1:]]
    for h in range(heads):
        ksend[h, cut:tok, :] = jnp.dot(
            last_ref[...], kall[h, axes(h)[2], core], preferred_element_type=jnp.float32
        ).astype(jnp.bfloat16)
        vsend[h, :, cut:tok] = lax.dot_general(
            vall[h, axes(h)[2], core, 0:HEAD_DIM, :], last_ref[...], NT,
            preferred_element_type=jnp.float32,
        ).astype(jnp.bfloat16)
    send_blocks(0, 1)
    send_blocks(1, 1)
    for h, queries in zip(head_order[1:], others):
        send_queries(h, queries)

    def run(items):
        def scores_of(item):
            h, q, k, which, part, masked = item
            s = lax.dot_general(
                kall[h, k, which], qbuf[h, q, part, :], NT, preferred_element_type=jnp.float32
            )
            if masked:
                first = part.start % pad
                if cols <= pad:
                    bias = bias_ref[:, first:first + cols]
                else:
                    bias = jnp.concatenate([bias_ref[...]] * (cols // pad), axis=1)
                s = s + bias
            return s

        scores = scores_of(items[0])
        for i, (h, q, k, which, part, masked) in enumerate(items):
            following = scores_of(items[i + 1]) if i + 1 < len(items) else None
            best = jnp.max(scores, axis=0, keepdims=True)
            weights = jnp.exp2(scores - best).astype(jnp.bfloat16)
            mixed = jnp.dot(vall[h, k, which], weights, preferred_element_type=jnp.float32)
            if not masked:
                old = m_ref[h, q, 0:1, part]
                top = jnp.maximum(old, best)
                mixed = mixed * jnp.exp2(best - top)
                mixed = mixed + acc_ref[h, q, :, part] * jnp.exp2(old - top)
                best = top
            m_ref[h, q, 0:1, part] = best
            acc_ref[h, q, :, part] = mixed
            scores = following

    lanes = (core, 1 - core)

    def both(h, q, k):
        run([(h, q, k, c, part, False) for part in col_parts for c in lanes])

    def serve(h, q, k, lanes, wait=False, answer=False):
        for index, part in enumerate(col_parts):
            if wait:
                q_wait(h, q, index)
            run([(h, q, k, c, part, False) for c in lanes])
            if answer:
                give_back(h, q, index)

    def p_copies(h, to, index):
        qc, nq, kc, nk = axes(h)
        dest = {"seq": chip_at(h, to, kc) * 2 + core}
        part = pl.ds(index * cols, cols)
        return [
            pltpu.make_async_remote_copy(
                src_ref=pout.at[h, to, :, part], dst_ref=pin.at[h, qc, :, part],
                send_sem=p_send.at[h, (to - qc - 1) % nq, index, 0],
                recv_sem=p_recv.at[h, (qc - to - 1) % nq, index, 0],
                device_id=dest, device_id_type=MESH,
            ),
            pltpu.make_async_remote_copy(
                src_ref=pout_stat.at[h, to, :, part], dst_ref=pin_stat.at[h, qc, :, part],
                send_sem=p_send.at[h, (to - qc - 1) % nq, index, 1],
                recv_sem=p_recv.at[h, (qc - to - 1) % nq, index, 1],
                device_id=dest, device_id_type=MESH,
            ),
        ]

    def p_wait(h, source, index):
        qc, nq, kc, nk = axes(h)
        part = pl.ds(index * cols, cols)
        place = (source - qc - 1) % nq
        for i, buf in enumerate((pin, pin_stat)):
            view = buf.at[h, source, :, part]
            pltpu.make_async_remote_copy(
                src_ref=view, dst_ref=view, send_sem=p_send.at[h, place, index, i],
                recv_sem=p_recv.at[h, place, index, i], device_id={"seq": partner},
                device_id_type=MESH,
            ).wait_recv()

    def give_back(h, to, index):
        part = col_parts[index]
        pout[h, to, :, part] = acc_ref[h, to, 0:HEAD_DIM, part].astype(jnp.bfloat16)
        pout_stat[h, to, 0:1, part] = m_ref[h, to, 0:1, part]
        pout_stat[h, to, 1:2, part] = acc_ref[h, to, HEAD_DIM:HEAD_DIM + 1, part]
        for copy in p_copies(h, to, index):
            copy.start()

    def no_moved(h):
        qc, nq, kc, nk = axes(h)
        return kc == 0 if h % 2 == 0 else nk == 1
    run(
        [
            (h, axes(h)[0], axes(h)[2], core, part, True)
            for h in range(heads)
            for part in col_parts
        ]
    )
    for h in range(heads):
        for arr in (0, 1):
            forward(arr, h, axes(h)[2], 1 - core, 2).wait_recv()
    @pl.when(core == 1)
    def _():
        run(
            [
                (h, axes(h)[0], axes(h)[2], 0, part, False)
                for h in range(heads)
                for part in col_parts
            ]
        )
    for h in range(heads):
        forward_blocks(h, 0, functools.partial(takes_kv, h))
        if h % 2 == 0:
            forward_blocks(h, 1, functools.partial(takes_kv, h))
        else:
            forward_blocks(
                h, 1, lambda i, h=h: takes_kv(h, i) & jnp.logical_not(shared_link(h, i))
            )
    def serve_own(h):
        qc, nq, kc, nk = axes(h)
        alone = no_moved(h)

        def go(j):
            pl.when(alone)(lambda: serve(h, j, kc, lanes, True, True))
            pl.when(jnp.logical_not(alone))(lambda: serve(h, j, kc, lanes, True))

        each(nq, lambda j: j > qc, go)

    def serve_moved(h):
        qc, nq, kc, nk = axes(h)

        def wanted(j):
            return takes_q(h, j) & jnp.logical_not(no_moved(h))

        def late(j):
            for index in range(len(col_parts)):
                q_wait(h, j, index)

        if nk == 2 and h % 2 == 1:
            each(nq, wanted, lambda j: serve(h, j, 1 - kc, lanes[:1]))
            arrive(h)
            each(nq, wanted, lambda j: serve(h, j, 1 - kc, lanes[1:], False, True))
        elif nk == 2:
            arrive(h)
            each(nq, lambda j: wanted(j) & (j < qc), lambda j: serve(h, j, 1 - kc, lanes, True, True))
            each(nq, lambda j: wanted(j) & (j > qc), lambda j: serve(h, j, 1 - kc, lanes, False, True))
        else:
            def go(j):
                pl.when(j < qc)(lambda: late(j))
                each(nk, functools.partial(takes_kv, h), lambda i: both(h, j, i))
                for index in range(len(col_parts)):
                    give_back(h, j, index)

            arrive(h)
            each(nq, wanted, go)
    for h in range(1, heads, 2):
        serve_own(h)
    for h in range(1, heads, 2):
        forward_blocks(h, 1, lambda i, h=h: takes_kv(h, i) & shared_link(h, i))
    for h in range(1, heads, 2):
        serve_moved(h)
    for h in range(0, heads, 2):
        serve_own(h)
    for d in range(1, kz):
        src = (zme + d) % kz
        pltpu.make_async_remote_copy(
            src_ref=devbuf.at[src], dst_ref=devbuf.at[src], send_sem=z_send.at[0],
            recv_sem=z_recv.at[d - 1], device_id={"kvh": src}, device_id_type=MESH,
        ).wait_recv()
    lens_load.wait()
    deviation = devbuf[0]
    for z in range(1, kz):
        deviation = deviation + devbuf[z]
    position = token + me * tok
    inside = []
    end = jnp.int32(0)
    for d in range(docs):
        begin, end = end, end + lens_ref[d]
        inside.append((position >= begin) & (position < end))
    slot_row = lax.broadcasted_iota(jnp.int32, docbuf.shape[1:], 0)
    shares = jnp.zeros(docbuf.shape[1:], jnp.float32)
    for d in range(docs):
        share = jnp.sum(jnp.where(inside[d], deviation, 0.0), axis=1, keepdims=True)
        shares = jnp.where(slot_row == d, share, shares)
    docbuf[me] = shares
    for d in range(1, n):
        sends.append(
            pltpu.make_async_remote_copy(
                src_ref=docbuf.at[me], dst_ref=docbuf.at[me], send_sem=doc_send.at[d - 1],
                recv_sem=doc_recv.at[n - d - 1], device_id={"seq": (me + d) % n}, device_id_type=MESH,
            )
        )
        sends[-1].start()
    for h in range(0, heads, 2):
        serve_moved(h)
    for h in range(heads):
        qc, nq, kc, nk = axes(h)
        each(nk, lambda i, kc=kc: i < kc, lambda i, h=h, qc=qc: both(h, qc, i))
    for h in range(heads):
        qc, nq, kc, nk = axes(h)

        def collect(source, h=h, qc=qc):
            for index, part in enumerate(col_parts):
                p_wait(h, source, index)
                best = m_ref[h, qc, 0:1, part]
                other = pin_stat[h, source, 0:1, part]
                top = jnp.maximum(best, other)
                fade, rise = jnp.exp2(best - top), jnp.exp2(other - top)
                m_ref[h, qc, 0:1, part] = top
                acc_ref[h, qc, 0:HEAD_DIM, part] = (
                    acc_ref[h, qc, 0:HEAD_DIM, part] * fade
                    + pin[h, source, :, part].astype(jnp.float32) * rise
                )
                acc_ref[h, qc, HEAD_DIM:HEAD_DIM + 1, part] = (
                    acc_ref[h, qc, HEAD_DIM:HEAD_DIM + 1, part] * fade
                    + pin_stat[h, source, 1:2, part] * rise
                )

        each(nq, functools.partial(sends_q, h), collect)
        done = acc_ref[h, qc, 0:HEAD_DIM, :] / acc_ref[h, qc, HEAD_DIM:HEAD_DIM + 1, :]
        for g in range(GROUP):
            head = h * GROUP + g
            rows = done[:, g * pad:(g + 1) * pad].T.astype(jnp.bfloat16)
            out_ref[:, head * HEAD_DIM:(head + 1) * HEAD_DIM] = rows[0:sel_rows]
    for d in range(1, n):
        src = (me + d) % n
        pltpu.make_async_remote_copy(
            src_ref=docbuf.at[src], dst_ref=docbuf.at[src], send_sem=doc_send.at[0],
            recv_sem=doc_recv.at[d - 1], device_id={"seq": src}, device_id_type=MESH,
        ).wait_recv()
    totals = docbuf[0]
    for s in range(1, n):
        totals = totals + docbuf[s]
    mean = jnp.zeros((1, tok), jnp.float32)
    for d in range(docs):
        here = totals[d:d + 1, 0:1] / lens_ref[d].astype(jnp.float32)
        mean = jnp.where(inside[d], here, mean)
    score_ref[...] = deviation / (mean + 1.0)
    for send in sends:
        send.wait_send()
    for h in range(heads):
        qc, nq, kc, nk = axes(h)

        def drain_kv(to, h=h):
            for span in (0, 1):
                for arr in (0, 1):
                    move(arr, h, span, to).wait_send()

        def drain_forward(source, h=h):
            for span in (0, 1):
                for arr in (0, 1):
                    forward(arr, h, source, core, span).wait_send()

        def drain_p(to, h=h):
            for index in range(len(col_parts)):
                for copy in p_copies(h, to, index):
                    copy.wait_send()

        for arr in (0, 1):
            forward(arr, h, kc, core, 2).wait_send()
        each(nk, functools.partial(sends_kv, h), drain_kv)
        each(nk, functools.partial(takes_kv, h), drain_forward)

        def drain_q(to, h=h):
            for index in range(len(col_parts)):
                q_copy(h, to, index).wait_send()

        each(nq, functools.partial(sends_q, h), drain_q)
        each(nq, functools.partial(takes_q, h), drain_p)


def shards(n, kz, hidden, w_query, w_key, w_value, cached_key, cached_value, doc_lengths, selected):
    tok, width = hidden.shape
    cols = w_key.shape[1]
    qcols = w_query.shape[1]
    sel_rows = selected.shape[0] // n
    docs = doc_lengths.shape[0]
    pad = round_up(sel_rows, LANES)
    heads = cols // HEAD_DIM
    qrows = GROUP * pad
    cut = (tok - sel_rows) // LANES * LANES
    side = max(split_chips(n // 2))
    others = max(1, side - 1)
    bf, f32 = jnp.bfloat16, jnp.float32
    dma = pltpu.SemaphoreType.DMA
    hbm = pl.BlockSpec(memory_space=pltpu.HBM)
    vmem = pl.BlockSpec(memory_space=pltpu.VMEM)
    attended, score = pl.pallas_call(
        functools.partial(kernel, n, kz, docs, sel_rows),
        out_shape=(
            pltpu.VMEM((sel_rows, qcols), bf),
            pltpu.VMEM((1, tok), f32),
        ),
        in_specs=[hbm] * 8,
        out_specs=(vmem, vmem),
        scratch_shapes=[
            pltpu.VMEM((tok, width), bf),
            pltpu.VMEM((width, qcols), bf),
            pltpu.VMEM((width, cols), bf),
            pltpu.VMEM((width, cols), bf),
            pltpu.VMEM((tok, cols), bf),
            pltpu.VMEM((tok, cols), bf),
            pltpu.VMEM((pad, width), bf),
            pltpu.VMEM((heads, side, 2, tok, HEAD_DIM), bf),
            pltpu.VMEM((heads, side, 2, HEAD_DIM + EXTRA, tok), bf),
            pltpu.VMEM((heads, tok, HEAD_DIM), bf),
            pltpu.VMEM((heads, HEAD_DIM, tok), bf),
            pltpu.VMEM((heads, side, qrows, HEAD_DIM), bf),
            pltpu.VMEM((heads, side, HEAD_DIM, qrows), bf),
            pltpu.VMEM((heads, side, 2, qrows), f32),
            pltpu.VMEM((heads, side, HEAD_DIM, qrows), bf),
            pltpu.VMEM((heads, side, 2, qrows), f32),
            pltpu.VMEM((tok, cols), f32),
            pltpu.VMEM((tok, cols), f32),
            pltpu.VMEM((heads, side, 8, qrows), f32),
            pltpu.VMEM((heads, side, HEAD_DIM + EXTRA, qrows), f32),
            pltpu.VMEM((tok, pad), f32),
            pltpu.VMEM((tok, LANES), f32),
            pltpu.VMEM((tok - cut, tok), bf),
            pltpu.VMEM((kz, 1, tok), f32),
            pltpu.VMEM((n, round_up(docs, 8), 128), f32),
            pltpu.SMEM(doc_lengths.shape, jnp.int32),
            pltpu.SMEM(selected.shape, jnp.int32),
            dma((3 * HID_CHUNKS + 4 + heads,)),
            dma((heads, others, GROUP * pad // q_cols(GROUP * pad))),
            dma((heads, others, GROUP * pad // q_cols(GROUP * pad))),
            dma((heads, others, GROUP * pad // q_cols(GROUP * pad), 2)),
            dma((heads, others, GROUP * pad // q_cols(GROUP * pad), 2)),
            dma((heads, others, 2, 2)),
            dma((heads, others, 2, 2)),
            dma((heads, others, 2, 2)),
            dma((heads, others, 2, 2)),
            dma((heads, 2)),
            dma((heads, 2)),
            dma((max(1, kz - 1),)),
            dma((max(1, kz - 1),)),
            dma((n - 1,)),
            dma((n - 1,)),
        ],
        compiler_params=pltpu.CompilerParams(
            collective_id=0, has_side_effects=True, vmem_limit_bytes=56 * 1024 * 1024
        ),
        name="blend",
    )(hidden, w_query, w_key, w_value, cached_key, cached_value, doc_lengths, selected)
    return attended, score.reshape(tok)


def solution(mesh):
    return jax.shard_map(
        functools.partial(shards, mesh.shape["seq"], mesh.shape["kvh"]),
        mesh=mesh,
        in_specs=(
            P("seq", None),
            P(None, "kvh"),
            P(None, "kvh"),
            P(None, "kvh"),
            P("seq", "kvh"),
            P("seq", "kvh"),
            P(),
            P(),
        ),
        out_specs=(P("seq", "kvh"), P("seq")),
        check_vma=False,
    )
```

```python
import functools
import math

import jax
import jax.numpy as jnp
from jax import lax
from jax.experimental import pallas as pl
from jax.experimental.pallas import tpu as pltpu
from jax.sharding import PartitionSpec as P

HEADS = 32
KV_HEADS = 8
HEAD_DIM = 128
GROUP = HEADS // KV_HEADS
EXP_SCALE = HEAD_DIM ** (-0.5) * math.log2(math.e)
MESH = pl.DeviceIdType.MESH
NT = (((1,), (1,)), ((), ()))
LANES = 128
EXTRA = 16
HID_CHUNKS = 4


def round_up(a, b):
    return -(-a // b) * b


def q_cols(rows):
    return 2 * LANES if rows % (2 * LANES) == 0 else LANES


def split_chips(chips):
    small = max(a for a in range(1, math.isqrt(chips) + 1) if chips % a == 0)
    return small, chips // small


def kernel(
    n, kz, docs, sel_rows,
    hid_hbm, wq_hbm, wk_hbm, wv_hbm, ck_hbm, cv_hbm, lens_hbm, sel_hbm,
    out_ref, score_ref,
    hid, wq, wk, wv, ck, cv, hq, kall, vall, ksend, vsend, qbuf, pout, pout_stat, pin, pin_stat,
    kacc, vacc, m_ref, acc_ref, bias_ref, chosen_ref, last_ref, devbuf, docbuf, lens_ref, sel_ref,
    load_sem, q_send, q_recv, p_send, p_recv, mv_send, mv_recv, fw_send, fw_recv, own_send, own_recv,
    z_send, z_recv, doc_send, doc_recv,
):
    tok, width = hid.shape
    heads = wk.shape[1] // HEAD_DIM
    pad = hq.shape[0]
    qrows = GROUP * pad
    qcols = GROUP * HEAD_DIM
    plain = tok - sel_rows
    cut = plain // LANES * LANES
    spans = ((0, cut), (cut, tok - cut), (0, tok))
    rows_a, rows_b = split_chips(n // 2)
    me = lax.axis_index("seq")
    zme = lax.axis_index("kvh")
    core = me % 2
    chip = me // 2
    ia, ib = chip // rows_b, chip % rows_b
    partner = me + 1 - 2 * core
    step = width // HID_CHUNKS
    barrier = pltpu.get_barrier_semaphore()
    for d in range(1, n):
        pl.semaphore_signal(barrier, inc=1, device_id={"seq": (me + d) % n}, device_id_type=MESH)
    for d in range(1, kz):
        pl.semaphore_signal(barrier, inc=1, device_id={"kvh": (zme + d) % kz}, device_id_type=MESH)

    loads = []

    def load(src, dst):
        copy = pltpu.make_async_copy(src, dst, load_sem.at[len(loads)])
        copy.start()
        loads.append(copy)
        return copy

    sel_load = load(sel_hbm, sel_ref)
    ck_load = load(ck_hbm, ck)
    cv_load = load(cv_hbm, cv)
    lens_load = load(lens_hbm, lens_ref)
    chunk_loads = []
    for c in range(HID_CHUNKS):
        part = pl.ds(c * step, step)
        chunk_loads.append(
            (
                load(hid_hbm.at[:, part], hid.at[:, part]),
                load(wk_hbm.at[part], wk.at[part]),
                load(wv_hbm.at[part], wv.at[part]),
            )
        )
    head_order = sorted(range(heads), key=lambda h: (1 - h % 2, h))
    wq_loads = {
        h: load(wq_hbm.at[:, pl.ds(h * qcols, qcols)], wq.at[:, pl.ds(h * qcols, qcols)])
        for h in head_order
    }

    def axes(h):
        if h % 2 == 0:
            return ib, rows_b, ia, rows_a
        return ia, rows_a, ib, rows_b

    def chip_at(h, q, k):
        return k * rows_b + q if h % 2 == 0 else q * rows_b + k

    def sends_kv(h, to):
        qc, nq, kc, nk = axes(h)
        if h % 2 == 0:
            return to > kc
        return (to != kc) & ((qc < nq - 1) | (to > kc))

    def takes_kv(h, source):
        qc, nq, kc, nk = axes(h)
        if h % 2 == 0:
            return source < kc
        return (source != kc) & ((qc < nq - 1) | (source < kc))

    def sends_q(h, to):
        qc, nq, kc, nk = axes(h)
        if h % 2 == 0:
            return (to != qc) & ((to < qc) | (kc > 0))
        return to < qc

    def takes_q(h, source):
        qc, nq, kc, nk = axes(h)
        if h % 2 == 0:
            return (source != qc) & ((source > qc) | (kc > 0))
        return source > qc

    def each(mine, count, want, body):
        def go(i, carry):
            pl.when(want(i))(functools.partial(body, i))
            return carry
        if count == 2:
            go(1 - mine, 0)
        else:
            lax.fori_loop(0, count, go, 0)

    def each_q(h, want, body):
        each(axes(h)[0], axes(h)[1], want, body)

    def each_k(h, want, body):
        each(axes(h)[2], axes(h)[3], want, body)

    def block(arr, h, slot, which, span):
        first, rows = spans[span]
        if arr == 0:
            return kall.at[h, slot, which, pl.ds(first, rows)]
        return vall.at[h, slot, which, pl.ds(0, HEAD_DIM), pl.ds(first, rows)]

    def move(arr, h, span, to):
        qc, nq, kc, nk = axes(h)
        first, rows = spans[span]
        src = ksend.at[h, pl.ds(first, rows)] if arr == 0 else vsend.at[h, :, pl.ds(first, rows)]
        return pltpu.make_async_remote_copy(
            src_ref=src, dst_ref=block(arr, h, kc, core, span),
            send_sem=mv_send.at[h, (to - kc - 1) % nk, span, arr],
            recv_sem=mv_recv.at[h, (kc - to - 1) % nk, span, arr],
            device_id={"seq": chip_at(h, qc, to) * 2 + core}, device_id_type=MESH,
        )

    def moved(arr, h, span, source):
        qc, nq, kc, nk = axes(h)
        index = (source - kc - 1) % nk
        view = block(arr, h, source, core, span)
        return pltpu.make_async_remote_copy(
            src_ref=view, dst_ref=view, send_sem=mv_send.at[h, index, span, arr],
            recv_sem=mv_recv.at[h, index, span, arr],
            device_id={"seq": partner}, device_id_type=MESH,
        )

    def forward(arr, h, slot, which, span):
        qc, nq, kc, nk = axes(h)
        view = block(arr, h, slot, which, span)
        if span == 2:
            send_sem, recv_sem = own_send.at[h, arr], own_recv.at[h, arr]
        else:
            index = (slot - kc - 1) % nk
            send_sem, recv_sem = fw_send.at[h, index, span, arr], fw_recv.at[h, index, span, arr]
        return pltpu.make_async_remote_copy(
            src_ref=view, dst_ref=view, send_sem=send_sem, recv_sem=recv_sem,
            device_id={"seq": partner}, device_id_type=MESH,
        )

    def send_blocks(arr, span):
        for h in range(heads):
            def go(to, h=h):
                move(arr, h, span, to).start()
            each_k(h, functools.partial(sends_kv, h), go)

    def shared_link(h, source):
        qc, nq, kc, nk = axes(h)
        return (source > kc) | (qc == nq - 1)

    def forward_blocks(h, span, want):
        def go(source):
            for arr in (0, 1):
                moved(arr, h, span, source).wait_recv()
                forward(arr, h, source, core, span).start()
        each_k(h, want, go)

    def arrive(h):
        def go(source):
            for span in (0, 1):
                for arr in (0, 1):
                    forward(arr, h, source, 1 - core, span).wait_recv()
        each_k(h, functools.partial(takes_kv, h), go)

    for h in range(heads):
        for i in range(kall.shape[1]):
            for c in range(2):
                vall[h, i, c, HEAD_DIM:, :] = jnp.ones((EXTRA, tok), jnp.bfloat16)
        for j in range(m_ref.shape[1]):
            m_ref[h, j] = jnp.full(m_ref.shape[2:], -1e30, jnp.float32)
            acc_ref[h, j] = jnp.zeros(acc_ref.shape[2:], jnp.float32)

    slot = lax.broadcasted_iota(jnp.int32, (8, pad), 1)
    sel_load.wait()

    def place(r, row):
        return jnp.where(slot == r, sel_ref[me * sel_rows + r], row)

    row_pos = lax.fori_loop(0, sel_rows, place, jnp.full((8, pad), -1, jnp.int32), unroll=8)[0:1]
    ck_load.wait()
    cv_load.wait()
    row_col = jnp.broadcast_to(row_pos.astype(jnp.float32), (LANES, pad)).T
    lane = lax.broadcasted_iota(jnp.int32, (pad, LANES), 1).astype(jnp.float32)
    pick = jnp.concatenate(
        [
            jnp.where(row_col == lane + float(k * LANES), 1.0, 0.0).astype(jnp.bfloat16)
            for k in range(tok // LANES)
        ],
        axis=1,
    )
    key_row = lax.broadcasted_iota(jnp.int32, (tok, pad), 0)
    pick_t = jnp.where(key_row == row_pos, 1.0, 0.0).astype(jnp.bfloat16)
    chosen_ref[...] = jnp.dot(
        pick_t, jnp.ones((pad, LANES), jnp.bfloat16), preferred_element_type=jnp.float32
    )
    bias_ref[...] = jnp.where(key_row <= row_pos, 0.0, -1e30)

    chosen = jnp.dot(jnp.ones((16, pad), jnp.bfloat16), pick, preferred_element_type=jnp.float32)
    upper = (
        lax.broadcasted_iota(jnp.int32, (LANES, LANES), 0)
        <= lax.broadcasted_iota(jnp.int32, (LANES, LANES), 1)
    ).astype(jnp.float32).astype(jnp.bfloat16)
    counts, before = [], jnp.zeros((1, 1), jnp.float32)
    for k in range(tok // LANES):
        tile = chosen[:, k * LANES:(k + 1) * LANES].astype(jnp.bfloat16)
        inner = jnp.dot(tile, upper, preferred_element_type=jnp.float32)[0:1]
        counts.append(inner + before)
        before = before + inner[:, LANES - 1:LANES]
    count = jnp.concatenate(counts, axis=1).astype(jnp.int32)
    token = lax.broadcasted_iota(jnp.int32, (1, tok), 1)
    target = jnp.where(chosen[0:1] > 0.5, plain + count - 1, token - count)

    def order(first, rows):
        row = lax.broadcasted_iota(jnp.int32, (rows, tok), 0) + first
        return jnp.where(row == target, 1.0, 0.0).astype(jnp.bfloat16)

    last_ref[...] = order(cut, tok - cut)
    early = order(0, cut)
    keys = jnp.dot(early, ck[...], preferred_element_type=jnp.float32).astype(jnp.bfloat16)
    values = jnp.dot(early, cv[...], preferred_element_type=jnp.float32)
    for h in range(heads):
        part = slice(h * HEAD_DIM, (h + 1) * HEAD_DIM)
        ksend[h, 0:cut, :] = keys[:, part]
        vsend[h, :, 0:cut] = values[:, part].T.astype(jnp.bfloat16)

    cols = q_cols(qrows)
    col_parts = [slice(j, j + cols) for j in range(0, qrows, cols)]

    def q_copy(h, to, index):
        qc, nq, kc, nk = axes(h)
        view = qbuf.at[h, qc, pl.ds(index * cols, cols)]
        return pltpu.make_async_remote_copy(
            src_ref=view, dst_ref=view, send_sem=q_send.at[h, (to - qc - 1) % nq, index],
            recv_sem=q_recv.at[h, (qc - to - 1) % nq, index],
            device_id={"seq": chip_at(h, to, kc) * 2 + core}, device_id_type=MESH,
        )

    def q_wait(h, source, index):
        qc, nq, kc, nk = axes(h)
        place = (source - qc - 1) % nq
        view = qbuf.at[h, source, pl.ds(index * cols, cols)]
        pltpu.make_async_remote_copy(
            src_ref=view, dst_ref=view, send_sem=q_send.at[h, place, index],
            recv_sem=q_recv.at[h, place, index], device_id={"seq": partner}, device_id_type=MESH,
        ).wait_recv()

    def store_queries(h, queries):
        scaled = (queries * EXP_SCALE).astype(jnp.bfloat16)
        for g in range(GROUP):
            qbuf[h, axes(h)[0], g * pad:(g + 1) * pad, :] = scaled[
                :, g * HEAD_DIM:(g + 1) * HEAD_DIM
            ]

    def send_queries(h):
        def go(to):
            for index in range(len(col_parts)):
                q_copy(h, to, index).start()

        each_q(h, functools.partial(sends_q, h), go)

    pieces = 2 if tok % (2 * LANES) == 0 else 1
    half = tok // pieces

    def fold(shift):
        square = shift * shift
        folded = square[:, 0:HEAD_DIM]
        for h in range(1, heads):
            folded = folded + square[:, h * HEAD_DIM:(h + 1) * HEAD_DIM]
        return jnp.sum(folded.T, axis=0, keepdims=True)

    def project(h):
        return jnp.dot(
            hq[...], wq[:, h * qcols:(h + 1) * qcols], preferred_element_type=jnp.float32
        )

    def project_chunk(c):
        part = slice(c * step, (c + 1) * step)
        for weight, total in ((wk, kacc), (wv, vacc)):
            fresh = jnp.dot(hid[:, part], weight[part, :], preferred_element_type=jnp.float32)
            total[...] = fresh if c == 0 else total[...] + fresh
        picked = jnp.dot(pick, hid[:, part], preferred_element_type=jnp.float32)
        hq[:, part] = picked.astype(jnp.bfloat16)

    for c in range(HID_CHUNKS):
        for copy in chunk_loads[c]:
            copy.wait()
        project_chunk(c)
        if c == 0:
            pl.semaphore_wait(barrier, n - 1 + kz - 1)
            send_blocks(0, 0)
            send_blocks(1, 0)

    first, rest = head_order[0], head_order[1:]
    wq_loads[first].wait()
    queries = project(first)
    mask = [
        jnp.concatenate([chosen_ref[p * half:(p + 1) * half, :]] * heads, axis=1) > 0.5
        for p in range(pieces)
    ]
    for p in range(pieces):
        rows = slice(p * half, (p + 1) * half)
        cached = ck[rows, :].astype(jnp.float32)
        used = jnp.where(mask[p], kacc[rows, :], cached).astype(jnp.bfloat16)
        for h in range(heads):
            kall[h, axes(h)[2], core, rows, :] = used[:, h * HEAD_DIM:(h + 1) * HEAD_DIM]
    store_queries(first, queries)
    send_queries(first)
    for h in range(heads):
        forward(0, h, axes(h)[2], core, 2).start()
    for h in rest:
        wq_loads[h].wait()
    queries = {h: project(h) for h in rest}
    for p in range(pieces):
        rows = slice(p * half, (p + 1) * half)
        cached_k = ck[rows, :].astype(jnp.float32)
        cached_v = cv[rows, :].astype(jnp.float32)
        used = jnp.where(mask[p], vacc[rows, :], cached_v).T.astype(jnp.bfloat16)
        for h in range(heads):
            part = slice(h * HEAD_DIM, (h + 1) * HEAD_DIM)
            vall[h, axes(h)[2], core, 0:HEAD_DIM, rows] = used[part, :]
        devbuf[zme, :, rows] = fold(kacc[rows, :] - cached_k) + fold(vacc[rows, :] - cached_v)
    for h in range(heads):
        ksend[h, cut:tok, :] = jnp.dot(
            last_ref[...], kall[h, axes(h)[2], core], preferred_element_type=jnp.float32
        ).astype(jnp.bfloat16)
        vsend[h, :, cut:tok] = lax.dot_general(
            vall[h, axes(h)[2], core, 0:HEAD_DIM, :], last_ref[...], NT,
            preferred_element_type=jnp.float32,
        ).astype(jnp.bfloat16)
    for h in rest:
        store_queries(h, queries[h])
    for h in range(heads):
        forward(1, h, axes(h)[2], core, 2).start()
    send_blocks(0, 1)
    send_blocks(1, 1)
    for h in rest:
        send_queries(h)
    sends = []
    for d in range(1, kz):
        sends.append(
            pltpu.make_async_remote_copy(
                src_ref=devbuf.at[zme], dst_ref=devbuf.at[zme], send_sem=z_send.at[d - 1],
                recv_sem=z_recv.at[kz - d - 1], device_id={"kvh": (zme + d) % kz},
                device_id_type=MESH,
            )
        )
        sends[-1].start()

    def run(items, answers=()):
        def scores_of(item):
            h, q, k, which, part, masked = item
            s = lax.dot_general(
                kall[h, k, which], qbuf[h, q, part, :], NT, preferred_element_type=jnp.float32
            )
            if masked:
                s = s + jnp.concatenate([bias_ref[...]] * GROUP, axis=1)
            return s

        scores = scores_of(items[0])
        for i, (h, q, k, which, part, masked) in enumerate(items):
            following = scores_of(items[i + 1]) if i + 1 < len(items) else None
            best = jnp.max(scores, axis=0, keepdims=True)
            weights = jnp.exp2(scores - best).astype(jnp.bfloat16)
            mixed = jnp.dot(vall[h, k, which], weights, preferred_element_type=jnp.float32)
            if not masked:
                old = m_ref[h, q, 0:1, part]
                top = jnp.maximum(old, best)
                mixed = mixed * jnp.exp2(best - top)
                mixed = mixed + acc_ref[h, q, :, part] * jnp.exp2(old - top)
                best = top
            m_ref[h, q, 0:1, part] = best
            acc_ref[h, q, :, part] = mixed
            scores = following
            if answers and (i + 1) % (len(items) // len(answers)) == 0:
                give_back(h, q, answers[i * len(answers) // len(items)])

    lanes = (core, 1 - core)
    wide = slice(0, qrows)

    def both(h, q, k):
        run([(h, q, k, c, wide, False) for c in lanes])

    every = range(len(col_parts))

    def serve(h, q, k, lanes, wait=False, answer=False, indices=every):
        items = {x: [(h, q, k, c, col_parts[x], False) for c in lanes] for x in indices}
        if wait:
            for index in indices:
                q_wait(h, q, index)
                run(items[index], [index] if answer else ())
            return
        run(sum(items.values(), []), indices if answer else ())

    def p_copies(h, to, index):
        qc, nq, kc, nk = axes(h)
        dest = {"seq": chip_at(h, to, kc) * 2 + core}
        return [
            pltpu.make_async_remote_copy(
                src_ref=pout.at[h, to, index], dst_ref=pin.at[h, qc, index],
                send_sem=p_send.at[h, (to - qc - 1) % nq, index, 0],
                recv_sem=p_recv.at[h, (qc - to - 1) % nq, index, 0],
                device_id=dest, device_id_type=MESH,
            ),
            pltpu.make_async_remote_copy(
                src_ref=pout_stat.at[h, to, index], dst_ref=pin_stat.at[h, qc, index],
                send_sem=p_send.at[h, (to - qc - 1) % nq, index, 1],
                recv_sem=p_recv.at[h, (qc - to - 1) % nq, index, 1],
                device_id=dest, device_id_type=MESH,
            ),
        ]

    def p_wait(h, source, index):
        qc, nq, kc, nk = axes(h)
        place = (source - qc - 1) % nq
        for i, buf in enumerate((pin, pin_stat)):
            view = buf.at[h, source, index]
            pltpu.make_async_remote_copy(
                src_ref=view, dst_ref=view, send_sem=p_send.at[h, place, index, i],
                recv_sem=p_recv.at[h, place, index, i], device_id={"seq": partner},
                device_id_type=MESH,
            ).wait_recv()

    def give_back(h, to, index):
        part = col_parts[index]
        pout[h, to, index] = acc_ref[h, to, 0:HEAD_DIM, part].astype(jnp.bfloat16)
        pout_stat[h, to, index, 0:1, :] = m_ref[h, to, 0:1, part]
        pout_stat[h, to, index, 1:2, :] = acc_ref[h, to, HEAD_DIM:HEAD_DIM + 1, part]
        for copy in p_copies(h, to, index):
            copy.start()

    def no_moved(h):
        qc, nq, kc, nk = axes(h)
        return kc == 0 if h % 2 == 0 else nk == 1
    run(
        [
            (h, axes(h)[0], axes(h)[2], core, wide, True)
            for h in range(heads)
        ]
    )
    for h in range(heads):
        for arr in (0, 1):
            forward(arr, h, axes(h)[2], 1 - core, 2).wait_recv()
    @pl.when(core == 1)
    def _():
        run(
            [
                (h, axes(h)[0], axes(h)[2], 0, wide, False)
                for h in range(heads)
            ]
        )

    def serve_own(h, indices=every):
        qc, nq, kc, nk = axes(h)
        alone = no_moved(h)

        def go(j):
            pl.when(alone)(lambda: serve(h, j, kc, lanes, True, True, indices))
            if indices[-1] == every[-1]:
                pl.when(jnp.logical_not(alone))(lambda: serve(h, j, kc, lanes, True))

        each_q(h, lambda j: j > qc, go)

    def moved_wanted(h, j):
        return takes_q(h, j) & jnp.logical_not(no_moved(h))

    def near_lane(h):
        qc, nq, kc, nk = axes(h)
        if nk == 2:
            each_q(
                h, functools.partial(moved_wanted, h), lambda j: serve(h, j, 1 - kc, lanes[:1])
            )

    def far_lane(h):
        qc, nq, kc, nk = axes(h)

        def go(j):
            each_k(h, functools.partial(takes_kv, h), lambda i: both(h, j, i))
            for index in every:
                give_back(h, j, index)

        arrive(h)
        if nk == 2:
            each_q(
                h, functools.partial(moved_wanted, h),
                lambda j: serve(h, j, 1 - kc, lanes[1:], False, True),
            )
        else:
            each_q(h, functools.partial(moved_wanted, h), go)

    def serve_moved(h):
        qc, nq, kc, nk = axes(h)

        def go(j):
            @pl.when(j < qc)
            def _():
                for index in every:
                    q_wait(h, j, index)
            each_k(h, functools.partial(takes_kv, h), lambda i: both(h, j, i))
            for index in every:
                give_back(h, j, index)

        arrive(h)
        if nk == 2:
            each_q(
                h, lambda j: moved_wanted(h, j) & (j < qc),
                lambda j: serve(h, j, 1 - kc, lanes, True, True),
            )
            each_q(
                h, lambda j: moved_wanted(h, j) & (j > qc),
                lambda j: serve(h, j, 1 - kc, lanes, False, True),
            )
        else:
            each_q(h, functools.partial(moved_wanted, h), go)
    for h in range(1, heads, 2):
        serve_own(h)
    for h in range(heads):
        forward_blocks(h, 0, functools.partial(takes_kv, h))
        if h % 2 == 0:
            forward_blocks(h, 1, functools.partial(takes_kv, h))
        else:
            forward_blocks(
                h, 1, lambda i, h=h: takes_kv(h, i) & jnp.logical_not(shared_link(h, i))
            )
    for d in range(1, kz):
        src = (zme + d) % kz
        pltpu.make_async_remote_copy(
            src_ref=devbuf.at[src], dst_ref=devbuf.at[src], send_sem=z_send.at[0],
            recv_sem=z_recv.at[d - 1], device_id={"kvh": src}, device_id_type=MESH,
        ).wait_recv()
    lens_load.wait()
    deviation = devbuf[0]
    for z in range(1, kz):
        deviation = deviation + devbuf[z]
    position = token + me * tok
    inside = []
    end = jnp.int32(0)
    for d in range(docs):
        begin, end = end, end + lens_ref[d]
        inside.append((position >= begin) & (position < end))
    slot_row = lax.broadcasted_iota(jnp.int32, docbuf.shape[1:], 0)
    shares = jnp.zeros(docbuf.shape[1:], jnp.float32)
    for d in range(docs):
        share = jnp.sum(jnp.where(inside[d], deviation, 0.0), axis=1, keepdims=True)
        shares = jnp.where(slot_row == d, share, shares)
    docbuf[me] = shares
    for d in range(1, n):
        sends.append(
            pltpu.make_async_remote_copy(
                src_ref=docbuf.at[me], dst_ref=docbuf.at[me], send_sem=doc_send.at[d - 1],
                recv_sem=doc_recv.at[n - d - 1], device_id={"seq": (me + d) % n}, device_id_type=MESH,
            )
        )
        sends[-1].start()
    for h in range(1, heads, 2):
        forward_blocks(h, 1, lambda i, h=h: takes_kv(h, i) & shared_link(h, i))
    for h in range(1, heads, 2):
        near_lane(h)
    for h in range(0, heads, 2):
        serve_own(h, every[:1])
    for h in range(1, heads, 2):
        far_lane(h)
    for h in range(0, heads, 2):
        serve_own(h, every[1:])
    for h in range(0, heads, 2):
        serve_moved(h)
    for h in range(heads):
        qc, nq, kc, nk = axes(h)
        each_k(h, lambda i, kc=kc: i < kc, lambda i, h=h, qc=qc: both(h, qc, i))
    for h in range(heads):
        qc, nq, kc, nk = axes(h)

        def collect(source, h=h, qc=qc):
            for index, part in enumerate(col_parts):
                p_wait(h, source, index)
                best = m_ref[h, qc, 0:1, part]
                other = pin_stat[h, source, index, 0:1, :]
                top = jnp.maximum(best, other)
                fade, rise = jnp.exp2(best - top), jnp.exp2(other - top)
                m_ref[h, qc, 0:1, part] = top
                acc_ref[h, qc, 0:HEAD_DIM, part] = (
                    acc_ref[h, qc, 0:HEAD_DIM, part] * fade
                    + pin[h, source, index].astype(jnp.float32) * rise
                )
                acc_ref[h, qc, HEAD_DIM:HEAD_DIM + 1, part] = (
                    acc_ref[h, qc, HEAD_DIM:HEAD_DIM + 1, part] * fade
                    + pin_stat[h, source, index, 1:2, :] * rise
                )

        each_q(h, functools.partial(sends_q, h), collect)
        done = acc_ref[h, qc, 0:HEAD_DIM, :] / acc_ref[h, qc, HEAD_DIM:HEAD_DIM + 1, :]
        for g in range(GROUP):
            head = h * GROUP + g
            rows = done[:, g * pad:(g + 1) * pad].T.astype(jnp.bfloat16)
            out_ref[:, head * HEAD_DIM:(head + 1) * HEAD_DIM] = rows[0:sel_rows]
    for d in range(1, n):
        src = (me + d) % n
        pltpu.make_async_remote_copy(
            src_ref=docbuf.at[src], dst_ref=docbuf.at[src], send_sem=doc_send.at[0],
            recv_sem=doc_recv.at[d - 1], device_id={"seq": src}, device_id_type=MESH,
        ).wait_recv()
    totals = docbuf[0]
    for s in range(1, n):
        totals = totals + docbuf[s]
    mean = jnp.zeros((1, tok), jnp.float32)
    for d in range(docs):
        here = totals[d:d + 1, 0:1] / lens_ref[d].astype(jnp.float32)
        mean = jnp.where(inside[d], here, mean)
    score_ref[...] = deviation / (mean + 1.0)
    for send in sends:
        send.wait_send()
    for h in range(heads):
        qc, nq, kc, nk = axes(h)

        def drain_kv(to, h=h):
            for span in (0, 1):
                for arr in (0, 1):
                    move(arr, h, span, to).wait_send()

        def drain_forward(source, h=h):
            for span in (0, 1):
                for arr in (0, 1):
                    forward(arr, h, source, core, span).wait_send()

        def drain_p(to, h=h):
            for index in range(len(col_parts)):
                for copy in p_copies(h, to, index):
                    copy.wait_send()

        for arr in (0, 1):
            forward(arr, h, kc, core, 2).wait_send()
        each_k(h, functools.partial(sends_kv, h), drain_kv)
        each_k(h, functools.partial(takes_kv, h), drain_forward)

        def drain_q(to, h=h):
            for index in range(len(col_parts)):
                q_copy(h, to, index).wait_send()

        each_q(h, functools.partial(sends_q, h), drain_q)
        each_q(h, functools.partial(takes_q, h), drain_p)


def shards(n, kz, hidden, w_query, w_key, w_value, cached_key, cached_value, doc_lengths, selected):
    tok, width = hidden.shape
    cols = w_key.shape[1]
    qcols = w_query.shape[1]
    sel_rows = selected.shape[0] // n
    docs = doc_lengths.shape[0]
    pad = round_up(sel_rows, LANES)
    heads = cols // HEAD_DIM
    qrows = GROUP * pad
    cut = (tok - sel_rows) // LANES * LANES
    cut_q = q_cols(qrows)
    side = max(split_chips(n // 2))
    others = max(1, side - 1)
    bf, f32 = jnp.bfloat16, jnp.float32
    dma = pltpu.SemaphoreType.DMA
    hbm = pl.BlockSpec(memory_space=pltpu.HBM)
    vmem = pl.BlockSpec(memory_space=pltpu.VMEM)
    attended, score = pl.pallas_call(
        functools.partial(kernel, n, kz, docs, sel_rows),
        out_shape=(
            pltpu.VMEM((sel_rows, qcols), bf),
            pltpu.VMEM((1, tok), f32),
        ),
        in_specs=[hbm] * 8,
        out_specs=(vmem, vmem),
        scratch_shapes=[
            pltpu.VMEM((tok, width), bf),
            pltpu.VMEM((width, qcols), bf),
            pltpu.VMEM((width, cols), bf),
            pltpu.VMEM((width, cols), bf),
            pltpu.VMEM((tok, cols), bf),
            pltpu.VMEM((tok, cols), bf),
            pltpu.VMEM((pad, width), bf),
            pltpu.VMEM((heads, side, 2, tok, HEAD_DIM), bf),
            pltpu.VMEM((heads, side, 2, HEAD_DIM + EXTRA, tok), bf),
            pltpu.VMEM((heads, tok, HEAD_DIM), bf),
            pltpu.VMEM((heads, HEAD_DIM, tok), bf),
            pltpu.VMEM((heads, side, qrows, HEAD_DIM), bf),
            pltpu.VMEM((heads, side, qrows // cut_q, HEAD_DIM, cut_q), bf),
            pltpu.VMEM((heads, side, qrows // cut_q, 2, cut_q), f32),
            pltpu.VMEM((heads, side, qrows // cut_q, HEAD_DIM, cut_q), bf),
            pltpu.VMEM((heads, side, qrows // cut_q, 2, cut_q), f32),
            pltpu.VMEM((tok, cols), f32),
            pltpu.VMEM((tok, cols), f32),
            pltpu.VMEM((heads, side, 8, qrows), f32),
            pltpu.VMEM((heads, side, HEAD_DIM + EXTRA, qrows), f32),
            pltpu.VMEM((tok, pad), f32),
            pltpu.VMEM((tok, LANES), f32),
            pltpu.VMEM((tok - cut, tok), bf),
            pltpu.VMEM((kz, 1, tok), f32),
            pltpu.VMEM((n, round_up(docs, 8), 128), f32),
            pltpu.SMEM(doc_lengths.shape, jnp.int32),
            pltpu.SMEM(selected.shape, jnp.int32),
            dma((3 * HID_CHUNKS + 4 + heads,)),
            dma((heads, others, qrows // cut_q)),
            dma((heads, others, qrows // cut_q)),
            dma((heads, others, qrows // cut_q, 2)),
            dma((heads, others, qrows // cut_q, 2)),
            dma((heads, others, 2, 2)),
            dma((heads, others, 2, 2)),
            dma((heads, others, 2, 2)),
            dma((heads, others, 2, 2)),
            dma((heads, 2)),
            dma((heads, 2)),
            dma((max(1, kz - 1),)),
            dma((max(1, kz - 1),)),
            dma((n - 1,)),
            dma((n - 1,)),
        ],
        compiler_params=pltpu.CompilerParams(
            collective_id=0, has_side_effects=True, vmem_limit_bytes=56 * 1024 * 1024
        ),
        name="blend",
    )(hidden, w_query, w_key, w_value, cached_key, cached_value, doc_lengths, selected)
    return attended, score.reshape(tok)


def solution(mesh):
    return jax.shard_map(
        functools.partial(shards, mesh.shape["seq"], mesh.shape["kvh"]),
        mesh=mesh,
        in_specs=(
            P("seq", None),
            P(None, "kvh"),
            P(None, "kvh"),
            P(None, "kvh"),
            P("seq", "kvh"),
            P("seq", "kvh"),
            P(),
            P(),
        ),
        out_specs=(P("seq", "kvh"), P("seq")),
        check_vma=False,
    )
```

```python
import functools
import math

import jax
import jax.numpy as jnp
from jax import lax
from jax.experimental import pallas as pl
from jax.experimental.pallas import tpu as pltpu
from jax.sharding import PartitionSpec as P

HEADS = 32
KV_HEADS = 8
HEAD_DIM = 128
GROUP = HEADS // KV_HEADS
EXP_SCALE = HEAD_DIM ** (-0.5) * math.log2(math.e)
MESH = pl.DeviceIdType.MESH
NT = (((1,), (1,)), ((), ()))
LANES = 128
EXTRA = 16
HID_CHUNKS = 4


def round_up(a, b):
    return -(-a // b) * b


def q_cols(rows):
    return 2 * LANES if rows % (2 * LANES) == 0 else LANES


def split_chips(chips):
    small = max(a for a in range(1, math.isqrt(chips) + 1) if chips % a == 0)
    return small, chips // small


def kernel(
    n, kz, docs, sel_rows,
    hid_hbm, wq_hbm, wk_hbm, wv_hbm, ck_hbm, cv_hbm, lens_hbm, sel_hbm,
    out_ref, score_ref,
    hid, wq, wk, wv, ck, cv, hq, kall, vall, ksend, vsend, qbuf, pout, pout_stat, pin, pin_stat,
    kacc, vacc, m_ref, acc_ref, bias_ref, chosen_ref, last_ref, devbuf, docbuf, lens_ref, sel_ref,
    load_sem, q_send, q_recv, p_send, p_recv, mv_send, mv_recv, fw_send, fw_recv, own_send, own_recv,
    z_send, z_recv, doc_send, doc_recv, ready,
):
    tok, width = hid.shape
    heads = wk.shape[1] // HEAD_DIM
    pad = hq.shape[0]
    qrows = GROUP * pad
    qcols = GROUP * HEAD_DIM
    plain = tok - sel_rows
    cut = plain // LANES * LANES
    spans = ((0, cut), (cut, tok - cut), (0, tok))
    rows_a, rows_b = split_chips(n // 2)
    me = lax.axis_index("seq")
    zme = lax.axis_index("kvh")
    core = me % 2
    chip = me // 2
    ia, ib = chip // rows_b, chip % rows_b
    partner = me + 1 - 2 * core
    step = width // HID_CHUNKS
    barrier = pltpu.get_barrier_semaphore()
    for c in range(n // 2):
        @pl.when(me != 2 * c + 1)
        def _():
            pl.semaphore_signal(
                barrier, inc=1, device_id={"seq": 2 * c + 1}, device_id_type=MESH
            )
    for d in range(1, kz):
        pl.semaphore_signal(
            barrier, inc=1, device_id={"seq": 2 * chip, "kvh": (zme + d) % kz},
            device_id_type=MESH,
        )

    def tell(hearing, count):
        @pl.when(core == hearing)
        def _():
            pl.semaphore_wait(barrier, count)
            pl.semaphore_signal(ready, inc=1, device_id={"seq": partner}, device_id_type=MESH)

    def hear(hearing):
        pl.when(core != hearing)(lambda: pl.semaphore_wait(ready, 1))

    loads = []

    def load(src, dst):
        copy = pltpu.make_async_copy(src, dst, load_sem.at[len(loads)])
        copy.start()
        loads.append(copy)
        return copy

    sel_load = load(sel_hbm, sel_ref)
    ck_load = load(ck_hbm, ck)
    cv_load = load(cv_hbm, cv)
    lens_load = load(lens_hbm, lens_ref)
    chunk_loads = []
    for c in range(HID_CHUNKS):
        part = pl.ds(c * step, step)
        chunk_loads.append(
            (
                load(hid_hbm.at[:, part], hid.at[:, part]),
                load(wk_hbm.at[part], wk.at[part]),
                load(wv_hbm.at[part], wv.at[part]),
            )
        )
    head_order = sorted(range(heads), key=lambda h: (1 - h % 2, h))
    wq_loads = {
        h: load(wq_hbm.at[:, pl.ds(h * qcols, qcols)], wq.at[:, pl.ds(h * qcols, qcols)])
        for h in head_order
    }

    def axes(h):
        if h % 2 == 0:
            return ib, rows_b, ia, rows_a
        return ia, rows_a, ib, rows_b

    def chip_at(h, q, k):
        return k * rows_b + q if h % 2 == 0 else q * rows_b + k

    def sends_kv(h, to):
        qc, nq, kc, nk = axes(h)
        if h % 2 == 0:
            return to > kc
        return (to != kc) & ((qc < nq - 1) | (to > kc))

    def takes_kv(h, source):
        qc, nq, kc, nk = axes(h)
        if h % 2 == 0:
            return source < kc
        return (source != kc) & ((qc < nq - 1) | (source < kc))

    def sends_q(h, to):
        qc, nq, kc, nk = axes(h)
        if h % 2 == 0:
            return (to != qc) & ((to < qc) | (kc > 0))
        return to < qc

    def takes_q(h, source):
        qc, nq, kc, nk = axes(h)
        if h % 2 == 0:
            return (source != qc) & ((source > qc) | (kc > 0))
        return source > qc

    def each(mine, count, want, body):
        def go(i, carry):
            pl.when(want(i))(functools.partial(body, i))
            return carry
        if count == 2:
            go(1 - mine, 0)
        else:
            lax.fori_loop(0, count, go, 0)

    def each_q(h, want, body):
        each(axes(h)[0], axes(h)[1], want, body)

    def each_k(h, want, body):
        each(axes(h)[2], axes(h)[3], want, body)

    def block(arr, h, slot, which, span):
        first, rows = spans[span]
        if arr == 0:
            return kall.at[h, slot, which, pl.ds(first, rows)]
        return vall.at[h, slot, which, pl.ds(0, HEAD_DIM), pl.ds(first, rows)]

    def move(arr, h, span, to):
        qc, nq, kc, nk = axes(h)
        first, rows = spans[span]
        src = ksend.at[h, pl.ds(first, rows)] if arr == 0 else vsend.at[h, :, pl.ds(first, rows)]
        return pltpu.make_async_remote_copy(
            src_ref=src, dst_ref=block(arr, h, kc, core, span),
            send_sem=mv_send.at[h, (to - kc - 1) % nk, span, arr],
            recv_sem=mv_recv.at[h, (kc - to - 1) % nk, span, arr],
            device_id={"seq": chip_at(h, qc, to) * 2 + core}, device_id_type=MESH,
        )

    def moved(arr, h, span, source):
        qc, nq, kc, nk = axes(h)
        index = (source - kc - 1) % nk
        view = block(arr, h, source, core, span)
        return pltpu.make_async_remote_copy(
            src_ref=view, dst_ref=view, send_sem=mv_send.at[h, index, span, arr],
            recv_sem=mv_recv.at[h, index, span, arr],
            device_id={"seq": partner}, device_id_type=MESH,
        )

    def forward(arr, h, slot, which, span):
        qc, nq, kc, nk = axes(h)
        view = block(arr, h, slot, which, span)
        if span == 2:
            send_sem, recv_sem = own_send.at[h, arr], own_recv.at[h, arr]
        else:
            index = (slot - kc - 1) % nk
            send_sem, recv_sem = fw_send.at[h, index, span, arr], fw_recv.at[h, index, span, arr]
        return pltpu.make_async_remote_copy(
            src_ref=view, dst_ref=view, send_sem=send_sem, recv_sem=recv_sem,
            device_id={"seq": partner}, device_id_type=MESH,
        )

    def urgent(h):
        return True if h % 2 == 0 else ia < rows_a - 1

    def send_blocks(arr, span, want=lambda h: True, only=range(2)):
        for h in range(heads):
            if h % 2 not in only:
                continue
            def go(to, h=h):
                move(arr, h, span, to).start()
            each_k(h, lambda to, h=h: sends_kv(h, to) & want(h), go)

    def shared_link(h, source):
        qc, nq, kc, nk = axes(h)
        return (source > kc) | (qc == nq - 1)

    def forward_blocks(h, span, want):
        def go(source):
            for arr in (0, 1):
                moved(arr, h, span, source).wait_recv()
                forward(arr, h, source, core, span).start()
        each_k(h, want, go)

    def arrive(h):
        def go(source):
            for span in (0, 1):
                for arr in (0, 1):
                    forward(arr, h, source, 1 - core, span).wait_recv()
        each_k(h, functools.partial(takes_kv, h), go)

    for h in range(heads):
        for i in range(kall.shape[1]):
            for c in range(2):
                vall[h, i, c, HEAD_DIM:, :] = jnp.ones((EXTRA, tok), jnp.bfloat16)
        for j in range(m_ref.shape[1]):
            m_ref[h, j] = jnp.full(m_ref.shape[2:], -1e30, jnp.float32)
            acc_ref[h, j] = jnp.zeros(acc_ref.shape[2:], jnp.float32)

    slot = lax.broadcasted_iota(jnp.int32, (8, pad), 1)
    sel_load.wait()

    def place(r, row):
        return jnp.where(slot == r, sel_ref[me * sel_rows + r], row)

    row_pos = lax.fori_loop(0, sel_rows, place, jnp.full((8, pad), -1, jnp.int32), unroll=8)[0:1]
    ck_load.wait()
    cv_load.wait()
    row_col = jnp.broadcast_to(row_pos.astype(jnp.float32), (LANES, pad)).T
    lane = lax.broadcasted_iota(jnp.int32, (pad, LANES), 1).astype(jnp.float32)
    pick = jnp.concatenate(
        [
            jnp.where(row_col == lane + float(k * LANES), 1.0, 0.0).astype(jnp.bfloat16)
            for k in range(tok // LANES)
        ],
        axis=1,
    )
    key_row = lax.broadcasted_iota(jnp.int32, (tok, pad), 0)
    pick_t = jnp.where(key_row == row_pos, 1.0, 0.0).astype(jnp.bfloat16)
    chosen_ref[...] = jnp.dot(
        pick_t, jnp.ones((pad, LANES), jnp.bfloat16), preferred_element_type=jnp.float32
    )
    bias_ref[...] = jnp.where(key_row <= row_pos, 0.0, -1e30)

    chosen = jnp.dot(jnp.ones((16, pad), jnp.bfloat16), pick, preferred_element_type=jnp.float32)
    upper = (
        lax.broadcasted_iota(jnp.int32, (LANES, LANES), 0)
        <= lax.broadcasted_iota(jnp.int32, (LANES, LANES), 1)
    ).astype(jnp.float32).astype(jnp.bfloat16)
    counts, before = [], jnp.zeros((1, 1), jnp.float32)
    for k in range(tok // LANES):
        tile = chosen[:, k * LANES:(k + 1) * LANES].astype(jnp.bfloat16)
        inner = jnp.dot(tile, upper, preferred_element_type=jnp.float32)[0:1]
        counts.append(inner + before)
        before = before + inner[:, LANES - 1:LANES]
    count = jnp.concatenate(counts, axis=1).astype(jnp.int32)
    token = lax.broadcasted_iota(jnp.int32, (1, tok), 1)
    target = jnp.where(chosen[0:1] > 0.5, plain + count - 1, token - count)

    def order(first, rows):
        row = lax.broadcasted_iota(jnp.int32, (rows, tok), 0) + first
        return jnp.where(row == target, 1.0, 0.0).astype(jnp.bfloat16)

    last_ref[...] = order(cut, tok - cut)
    early = order(0, cut)
    keys = jnp.dot(early, ck[...], preferred_element_type=jnp.float32).astype(jnp.bfloat16)
    values = jnp.dot(early, cv[...], preferred_element_type=jnp.float32)
    for h in range(heads):
        part = slice(h * HEAD_DIM, (h + 1) * HEAD_DIM)
        ksend[h, 0:cut, :] = keys[:, part]
        vsend[h, :, 0:cut] = values[:, part].T.astype(jnp.bfloat16)

    cols = q_cols(qrows)
    col_parts = [slice(j, j + cols) for j in range(0, qrows, cols)]

    def q_copy(h, to, index):
        qc, nq, kc, nk = axes(h)
        view = qbuf.at[h, qc, pl.ds(index * cols, cols)]
        return pltpu.make_async_remote_copy(
            src_ref=view, dst_ref=view, send_sem=q_send.at[h, (to - qc - 1) % nq, index],
            recv_sem=q_recv.at[h, (qc - to - 1) % nq, index],
            device_id={"seq": chip_at(h, to, kc) * 2 + core}, device_id_type=MESH,
        )

    def q_wait(h, source, index):
        qc, nq, kc, nk = axes(h)
        place = (source - qc - 1) % nq
        view = qbuf.at[h, source, pl.ds(index * cols, cols)]
        pltpu.make_async_remote_copy(
            src_ref=view, dst_ref=view, send_sem=q_send.at[h, place, index],
            recv_sem=q_recv.at[h, place, index], device_id={"seq": partner}, device_id_type=MESH,
        ).wait_recv()

    def store_queries(h, queries):
        scaled = (queries * EXP_SCALE).astype(jnp.bfloat16)
        for g in range(GROUP):
            qbuf[h, axes(h)[0], g * pad:(g + 1) * pad, :] = scaled[
                :, g * HEAD_DIM:(g + 1) * HEAD_DIM
            ]

    def send_queries(h):
        def go(to):
            for index in range(len(col_parts)):
                q_copy(h, to, index).start()

        each_q(h, functools.partial(sends_q, h), go)

    pieces = 2 if tok % (2 * LANES) == 0 else 1
    half = tok // pieces

    def fold(shift):
        square = shift * shift
        folded = square[:, 0:HEAD_DIM]
        for h in range(1, heads):
            folded = folded + square[:, h * HEAD_DIM:(h + 1) * HEAD_DIM]
        return jnp.sum(folded.T, axis=0, keepdims=True)

    def project(h):
        return jnp.dot(
            hq[...], wq[:, h * qcols:(h + 1) * qcols], preferred_element_type=jnp.float32
        )

    def project_chunk(c):
        part = slice(c * step, (c + 1) * step)
        for weight, total in ((wk, kacc), (wv, vacc)):
            fresh = jnp.dot(hid[:, part], weight[part, :], preferred_element_type=jnp.float32)
            total[...] = fresh if c == 0 else total[...] + fresh
        picked = jnp.dot(pick, hid[:, part], preferred_element_type=jnp.float32)
        hq[:, part] = picked.astype(jnp.bfloat16)
    tell(1, n - 1)
    hear(1)
    send_blocks(0, 0)
    send_blocks(1, 0)
    for c in range(HID_CHUNKS):
        for copy in chunk_loads[c]:
            copy.wait()
        project_chunk(c)
    if kz > 1:
        tell(0, 2 * (kz - 1))
    first, rest = head_order[0], head_order[1:]
    wq_loads[first].wait()
    queries = project(first)
    mask = [
        jnp.concatenate([chosen_ref[p * half:(p + 1) * half, :]] * heads, axis=1) > 0.5
        for p in range(pieces)
    ]
    for p in range(pieces):
        rows = slice(p * half, (p + 1) * half)
        cached = ck[rows, :].astype(jnp.float32)
        used = jnp.where(mask[p], kacc[rows, :], cached).astype(jnp.bfloat16)
        for h in range(heads):
            kall[h, axes(h)[2], core, rows, :] = used[:, h * HEAD_DIM:(h + 1) * HEAD_DIM]
    store_queries(first, queries)
    send_queries(first)
    for h in range(heads):
        forward(0, h, axes(h)[2], core, 2).start()
    for h in rest:
        wq_loads[h].wait()
    queries = {h: project(h) for h in rest}
    for p in range(pieces):
        rows = slice(p * half, (p + 1) * half)
        cached_k = ck[rows, :].astype(jnp.float32)
        cached_v = cv[rows, :].astype(jnp.float32)
        used = jnp.where(mask[p], vacc[rows, :], cached_v).T.astype(jnp.bfloat16)
        for h in range(heads):
            part = slice(h * HEAD_DIM, (h + 1) * HEAD_DIM)
            vall[h, axes(h)[2], core, 0:HEAD_DIM, rows] = used[part, :]
        devbuf[zme, :, rows] = fold(kacc[rows, :] - cached_k) + fold(vacc[rows, :] - cached_v)
    for h in range(heads):
        ksend[h, cut:tok, :] = jnp.dot(
            last_ref[...], kall[h, axes(h)[2], core], preferred_element_type=jnp.float32
        ).astype(jnp.bfloat16)
        vsend[h, :, cut:tok] = lax.dot_general(
            vall[h, axes(h)[2], core, 0:HEAD_DIM, :], last_ref[...], NT,
            preferred_element_type=jnp.float32,
        ).astype(jnp.bfloat16)
    for h in rest:
        store_queries(h, queries[h])
    for h in range(heads):
        forward(1, h, axes(h)[2], core, 2).start()
    send_blocks(0, 1, urgent)
    send_blocks(1, 1, urgent)
    for h in rest:
        send_queries(h)
    for arr in (0, 1):
        send_blocks(arr, 1, lambda h: jnp.logical_not(urgent(h)), (1,))
    sends = []
    if kz > 1:
        hear(0)
    for d in range(1, kz):
        sends.append(
            pltpu.make_async_remote_copy(
                src_ref=devbuf.at[zme], dst_ref=devbuf.at[zme], send_sem=z_send.at[d - 1],
                recv_sem=z_recv.at[kz - d - 1], device_id={"kvh": (zme + d) % kz},
                device_id_type=MESH,
            )
        )
        sends[-1].start()

    def run(items, answers=()):
        def scores_of(item):
            h, q, k, which, part, masked = item
            s = lax.dot_general(
                kall[h, k, which], qbuf[h, q, part, :], NT, preferred_element_type=jnp.float32
            )
            if masked:
                s = s + jnp.concatenate([bias_ref[...]] * GROUP, axis=1)
            return s

        scores = scores_of(items[0])
        for i, (h, q, k, which, part, masked) in enumerate(items):
            following = scores_of(items[i + 1]) if i + 1 < len(items) else None
            best = jnp.max(scores, axis=0, keepdims=True)
            weights = jnp.exp2(scores - best).astype(jnp.bfloat16)
            mixed = jnp.dot(vall[h, k, which], weights, preferred_element_type=jnp.float32)
            if not masked:
                old = m_ref[h, q, 0:1, part]
                top = jnp.maximum(old, best)
                mixed = mixed * jnp.exp2(best - top)
                mixed = mixed + acc_ref[h, q, :, part] * jnp.exp2(old - top)
                best = top
            m_ref[h, q, 0:1, part] = best
            acc_ref[h, q, :, part] = mixed
            scores = following
            if answers and (i + 1) % (len(items) // len(answers)) == 0:
                give_back(h, q, answers[i * len(answers) // len(items)])

    lanes = (core, 1 - core)
    wide = slice(0, qrows)

    def both(h, q, k):
        run([(h, q, k, c, wide, False) for c in lanes])

    every = range(len(col_parts))

    def serve(h, q, k, lanes, wait=False, answer=False, indices=every):
        items = {x: [(h, q, k, c, col_parts[x], False) for c in lanes] for x in indices}
        if wait:
            for index in indices:
                q_wait(h, q, index)
                run(items[index], [index] if answer else ())
            return
        run(sum(items.values(), []), indices if answer else ())

    def p_copies(h, to, index):
        qc, nq, kc, nk = axes(h)
        dest = {"seq": chip_at(h, to, kc) * 2 + core}
        return [
            pltpu.make_async_remote_copy(
                src_ref=pout.at[h, to, index], dst_ref=pin.at[h, qc, index],
                send_sem=p_send.at[h, (to - qc - 1) % nq, index, 0],
                recv_sem=p_recv.at[h, (qc - to - 1) % nq, index, 0],
                device_id=dest, device_id_type=MESH,
            ),
            pltpu.make_async_remote_copy(
                src_ref=pout_stat.at[h, to, index], dst_ref=pin_stat.at[h, qc, index],
                send_sem=p_send.at[h, (to - qc - 1) % nq, index, 1],
                recv_sem=p_recv.at[h, (qc - to - 1) % nq, index, 1],
                device_id=dest, device_id_type=MESH,
            ),
        ]

    def p_wait(h, source, index):
        qc, nq, kc, nk = axes(h)
        place = (source - qc - 1) % nq
        for i, buf in enumerate((pin, pin_stat)):
            view = buf.at[h, source, index]
            pltpu.make_async_remote_copy(
                src_ref=view, dst_ref=view, send_sem=p_send.at[h, place, index, i],
                recv_sem=p_recv.at[h, place, index, i], device_id={"seq": partner},
                device_id_type=MESH,
            ).wait_recv()

    def give_back(h, to, index):
        part = col_parts[index]
        pout[h, to, index] = acc_ref[h, to, 0:HEAD_DIM, part].astype(jnp.bfloat16)
        pout_stat[h, to, index, 0:1, :] = m_ref[h, to, 0:1, part]
        pout_stat[h, to, index, 1:2, :] = acc_ref[h, to, HEAD_DIM:HEAD_DIM + 1, part]
        for copy in p_copies(h, to, index):
            copy.start()

    def no_moved(h):
        qc, nq, kc, nk = axes(h)
        return kc == 0 if h % 2 == 0 else nk == 1
    run(
        [
            (h, axes(h)[0], axes(h)[2], core, wide, True)
            for h in range(heads)
        ]
    )
    for h in range(heads):
        for arr in (0, 1):
            forward(arr, h, axes(h)[2], 1 - core, 2).wait_recv()
    @pl.when(core == 1)
    def _():
        run(
            [
                (h, axes(h)[0], axes(h)[2], 0, wide, False)
                for h in range(heads)
            ]
        )

    def serve_own(h, indices=every):
        qc, nq, kc, nk = axes(h)
        alone = no_moved(h)

        def go(j):
            pl.when(alone)(lambda: serve(h, j, kc, lanes, True, True, indices))
            if indices[-1] == every[-1]:
                pl.when(jnp.logical_not(alone))(lambda: serve(h, j, kc, lanes, True))

        each_q(h, lambda j: j > qc, go)

    def moved_wanted(h, j):
        return takes_q(h, j) & jnp.logical_not(no_moved(h))

    def near_lane(h):
        qc, nq, kc, nk = axes(h)
        if nk == 2:
            each_q(
                h, functools.partial(moved_wanted, h), lambda j: serve(h, j, 1 - kc, lanes[:1])
            )

    def far_lane(h):
        qc, nq, kc, nk = axes(h)

        def go(j):
            each_k(h, functools.partial(takes_kv, h), lambda i: both(h, j, i))
            for index in every:
                give_back(h, j, index)

        pl.when(ia < rows_a - 1)(lambda: arrive(h))
        if nk == 2:
            each_q(
                h, functools.partial(moved_wanted, h),
                lambda j: serve(h, j, 1 - kc, lanes[1:], False, True),
            )
        else:
            each_q(h, functools.partial(moved_wanted, h), go)

    def serve_moved(h):
        qc, nq, kc, nk = axes(h)

        def go(j):
            @pl.when(j < qc)
            def _():
                for index in every:
                    q_wait(h, j, index)
            each_k(h, functools.partial(takes_kv, h), lambda i: both(h, j, i))
            for index in every:
                give_back(h, j, index)

        arrive(h)
        if nk == 2:
            each_q(
                h, lambda j: moved_wanted(h, j) & (j < qc),
                lambda j: serve(h, j, 1 - kc, lanes, True, True),
            )
            each_q(
                h, lambda j: moved_wanted(h, j) & (j > qc),
                lambda j: serve(h, j, 1 - kc, lanes, False, True),
            )
        else:
            each_q(h, functools.partial(moved_wanted, h), go)
    for h in range(1, heads, 2):
        serve_own(h)
    for h in range(heads):
        forward_blocks(h, 0, functools.partial(takes_kv, h))
        if h % 2 == 0:
            forward_blocks(h, 1, functools.partial(takes_kv, h))
        else:
            forward_blocks(
                h, 1, lambda i, h=h: takes_kv(h, i) & jnp.logical_not(shared_link(h, i))
            )
    for d in range(1, kz):
        src = (zme + d) % kz
        pltpu.make_async_remote_copy(
            src_ref=devbuf.at[src], dst_ref=devbuf.at[src], send_sem=z_send.at[0],
            recv_sem=z_recv.at[d - 1], device_id={"kvh": src}, device_id_type=MESH,
        ).wait_recv()
    lens_load.wait()
    deviation = devbuf[0]
    for z in range(1, kz):
        deviation = deviation + devbuf[z]
    position = token + me * tok
    inside = []
    end = jnp.int32(0)
    for d in range(docs):
        begin, end = end, end + lens_ref[d]
        inside.append((position >= begin) & (position < end))
    slot_row = lax.broadcasted_iota(jnp.int32, docbuf.shape[1:], 0)
    shares = jnp.zeros(docbuf.shape[1:], jnp.float32)
    for d in range(docs):
        share = jnp.sum(jnp.where(inside[d], deviation, 0.0), axis=1, keepdims=True)
        shares = jnp.where(slot_row == d, share, shares)
    docbuf[me] = shares
    for d in range(1, n):
        sends.append(
            pltpu.make_async_remote_copy(
                src_ref=docbuf.at[me], dst_ref=docbuf.at[me], send_sem=doc_send.at[d - 1],
                recv_sem=doc_recv.at[n - d - 1], device_id={"seq": (me + d) % n}, device_id_type=MESH,
            )
        )
        sends[-1].start()
    for h in range(1, heads, 2):
        forward_blocks(
            h, 1, lambda i, h=h: takes_kv(h, i) & shared_link(h, i) & (ia < rows_a - 1)
        )
    for h in range(1, heads, 2):
        near_lane(h)
    for h in range(0, heads, 2):
        serve_own(h, every[:1])
    for h in range(1, heads, 2):
        far_lane(h)
    for h in range(0, heads, 2):
        serve_own(h, every[1:])
    for h in range(0, heads, 2):
        serve_moved(h)
    for h in range(heads):
        qc, nq, kc, nk = axes(h)
        if h % 2 == 1:
            @pl.when(ia == rows_a - 1)
            def _():
                forward_blocks(h, 1, functools.partial(takes_kv, h))
                arrive(h)
        each_k(h, lambda i, kc=kc: i < kc, lambda i, h=h, qc=qc: both(h, qc, i))
    for h in range(heads):
        qc, nq, kc, nk = axes(h)

        def collect(source, h=h, qc=qc):
            for index, part in enumerate(col_parts):
                p_wait(h, source, index)
                best = m_ref[h, qc, 0:1, part]
                other = pin_stat[h, source, index, 0:1, :]
                top = jnp.maximum(best, other)
                fade, rise = jnp.exp2(best - top), jnp.exp2(other - top)
                m_ref[h, qc, 0:1, part] = top
                acc_ref[h, qc, 0:HEAD_DIM, part] = (
                    acc_ref[h, qc, 0:HEAD_DIM, part] * fade
                    + pin[h, source, index].astype(jnp.float32) * rise
                )
                acc_ref[h, qc, HEAD_DIM:HEAD_DIM + 1, part] = (
                    acc_ref[h, qc, HEAD_DIM:HEAD_DIM + 1, part] * fade
                    + pin_stat[h, source, index, 1:2, :] * rise
                )

        each_q(h, functools.partial(sends_q, h), collect)
        done = acc_ref[h, qc, 0:HEAD_DIM, :] / acc_ref[h, qc, HEAD_DIM:HEAD_DIM + 1, :]
        for g in range(GROUP):
            head = h * GROUP + g
            rows = done[:, g * pad:(g + 1) * pad].T.astype(jnp.bfloat16)
            out_ref[:, head * HEAD_DIM:(head + 1) * HEAD_DIM] = rows[0:sel_rows]
    for d in range(1, n):
        src = (me + d) % n
        pltpu.make_async_remote_copy(
            src_ref=docbuf.at[src], dst_ref=docbuf.at[src], send_sem=doc_send.at[0],
            recv_sem=doc_recv.at[d - 1], device_id={"seq": src}, device_id_type=MESH,
        ).wait_recv()
    totals = docbuf[0]
    for s in range(1, n):
        totals = totals + docbuf[s]
    mean = jnp.zeros((1, tok), jnp.float32)
    for d in range(docs):
        here = totals[d:d + 1, 0:1] / lens_ref[d].astype(jnp.float32)
        mean = jnp.where(inside[d], here, mean)
    score_ref[...] = deviation / (mean + 1.0)
    for send in sends:
        send.wait_send()
    for h in range(heads):
        qc, nq, kc, nk = axes(h)

        def drain_kv(to, h=h):
            for span in (0, 1):
                for arr in (0, 1):
                    move(arr, h, span, to).wait_send()

        def drain_forward(source, h=h):
            for span in (0, 1):
                for arr in (0, 1):
                    forward(arr, h, source, core, span).wait_send()

        def drain_p(to, h=h):
            for index in range(len(col_parts)):
                for copy in p_copies(h, to, index):
                    copy.wait_send()

        for arr in (0, 1):
            forward(arr, h, kc, core, 2).wait_send()
        each_k(h, functools.partial(sends_kv, h), drain_kv)
        each_k(h, functools.partial(takes_kv, h), drain_forward)

        def drain_q(to, h=h):
            for index in range(len(col_parts)):
                q_copy(h, to, index).wait_send()

        each_q(h, functools.partial(sends_q, h), drain_q)
        each_q(h, functools.partial(takes_q, h), drain_p)


def shards(n, kz, hidden, w_query, w_key, w_value, cached_key, cached_value, doc_lengths, selected):
    tok, width = hidden.shape
    cols = w_key.shape[1]
    qcols = w_query.shape[1]
    sel_rows = selected.shape[0] // n
    docs = doc_lengths.shape[0]
    pad = round_up(sel_rows, LANES)
    heads = cols // HEAD_DIM
    qrows = GROUP * pad
    cut = (tok - sel_rows) // LANES * LANES
    cut_q = q_cols(qrows)
    side = max(split_chips(n // 2))
    others = max(1, side - 1)
    bf, f32 = jnp.bfloat16, jnp.float32
    dma = pltpu.SemaphoreType.DMA
    hbm = pl.BlockSpec(memory_space=pltpu.HBM)
    vmem = pl.BlockSpec(memory_space=pltpu.VMEM)
    attended, score = pl.pallas_call(
        functools.partial(kernel, n, kz, docs, sel_rows),
        out_shape=(
            pltpu.VMEM((sel_rows, qcols), bf),
            pltpu.VMEM((1, tok), f32),
        ),
        in_specs=[hbm] * 8,
        out_specs=(vmem, vmem),
        scratch_shapes=[
            pltpu.VMEM((tok, width), bf),
            pltpu.VMEM((width, qcols), bf),
            pltpu.VMEM((width, cols), bf),
            pltpu.VMEM((width, cols), bf),
            pltpu.VMEM((tok, cols), bf),
            pltpu.VMEM((tok, cols), bf),
            pltpu.VMEM((pad, width), bf),
            pltpu.VMEM((heads, side, 2, tok, HEAD_DIM), bf),
            pltpu.VMEM((heads, side, 2, HEAD_DIM + EXTRA, tok), bf),
            pltpu.VMEM((heads, tok, HEAD_DIM), bf),
            pltpu.VMEM((heads, HEAD_DIM, tok), bf),
            pltpu.VMEM((heads, side, qrows, HEAD_DIM), bf),
            pltpu.VMEM((heads, side, qrows // cut_q, HEAD_DIM, cut_q), bf),
            pltpu.VMEM((heads, side, qrows // cut_q, 2, cut_q), f32),
            pltpu.VMEM((heads, side, qrows // cut_q, HEAD_DIM, cut_q), bf),
            pltpu.VMEM((heads, side, qrows // cut_q, 2, cut_q), f32),
            pltpu.VMEM((tok, cols), f32),
            pltpu.VMEM((tok, cols), f32),
            pltpu.VMEM((heads, side, 8, qrows), f32),
            pltpu.VMEM((heads, side, HEAD_DIM + EXTRA, qrows), f32),
            pltpu.VMEM((tok, pad), f32),
            pltpu.VMEM((tok, LANES), f32),
            pltpu.VMEM((tok - cut, tok), bf),
            pltpu.VMEM((kz, 1, tok), f32),
            pltpu.VMEM((n, round_up(docs, 8), 128), f32),
            pltpu.SMEM(doc_lengths.shape, jnp.int32),
            pltpu.SMEM(selected.shape, jnp.int32),
            dma((3 * HID_CHUNKS + 4 + heads,)),
            dma((heads, others, qrows // cut_q)),
            dma((heads, others, qrows // cut_q)),
            dma((heads, others, qrows // cut_q, 2)),
            dma((heads, others, qrows // cut_q, 2)),
            dma((heads, others, 2, 2)),
            dma((heads, others, 2, 2)),
            dma((heads, others, 2, 2)),
            dma((heads, others, 2, 2)),
            dma((heads, 2)),
            dma((heads, 2)),
            dma((max(1, kz - 1),)),
            dma((max(1, kz - 1),)),
            dma((n - 1,)),
            dma((n - 1,)),
            pltpu.SemaphoreType.REGULAR,
        ],
        compiler_params=pltpu.CompilerParams(
            collective_id=0, has_side_effects=True, vmem_limit_bytes=56 * 1024 * 1024
        ),
        name="blend",
    )(hidden, w_query, w_key, w_value, cached_key, cached_value, doc_lengths, selected)
    return attended, score.reshape(tok)


def solution(mesh):
    return jax.shard_map(
        functools.partial(shards, mesh.shape["seq"], mesh.shape["kvh"]),
        mesh=mesh,
        in_specs=(
            P("seq", None),
            P(None, "kvh"),
            P(None, "kvh"),
            P(None, "kvh"),
            P("seq", "kvh"),
            P("seq", "kvh"),
            P(),
            P(),
        ),
        out_specs=(P("seq", "kvh"), P("seq")),
        check_vma=False,
    )
```

```python
import functools
import math

import jax
import jax.numpy as jnp
from jax import lax
from jax.experimental import pallas as pl
from jax.experimental.pallas import tpu as pltpu
from jax.sharding import PartitionSpec as P

HEADS = 32
KV_HEADS = 8
HEAD_DIM = 128
GROUP = HEADS // KV_HEADS
EXP_SCALE = HEAD_DIM ** (-0.5) * math.log2(math.e)
MESH = pl.DeviceIdType.MESH
NT = (((1,), (1,)), ((), ()))
LANES = 128
EXTRA = 16
HID_CHUNKS = 4


def round_up(a, b):
    return -(-a // b) * b


def q_cols(rows):
    return 2 * LANES if rows % (2 * LANES) == 0 else LANES


def split_chips(chips):
    small = max(a for a in range(1, math.isqrt(chips) + 1) if chips % a == 0)
    return small, chips // small


def kernel(
    n, kz, docs, sel_rows,
    hid_hbm, wq_hbm, wk_hbm, wv_hbm, ck_hbm, cv_hbm, lens_hbm, sel_hbm,
    out_ref, score_ref,
    hid, wq, wk, wv, ck, cv, hq, kall, vall, ksend, vsend, qbuf, pout, pout_stat, pin, pin_stat,
    kacc, vacc, m_ref, acc_ref, bias_ref, chosen_ref, last_ref, dev_ref, devbuf, docbuf, lens_ref, sel_ref,
    load_sem, q_send, q_recv, p_send, p_recv, mv_send, mv_recv, fw_send, fw_recv, own_send, own_recv,
    z_send, z_recv, doc_send, doc_recv, ready,
):
    tok, width = hid.shape
    heads = wk.shape[1] // HEAD_DIM
    pad = hq.shape[0]
    qrows = GROUP * pad
    qcols = GROUP * HEAD_DIM
    plain = tok - sel_rows
    cut = plain // LANES * LANES
    spans = ((0, cut), (cut, tok - cut), (0, tok))
    rows_a, rows_b = split_chips(n // 2)
    me = lax.axis_index("seq")
    zme = lax.axis_index("kvh")
    core = me % 2
    chip = me // 2
    ia, ib = chip // rows_b, chip % rows_b
    partner = me + 1 - 2 * core
    step = width // HID_CHUNKS
    barrier = pltpu.get_barrier_semaphore()
    for c in range(n // 2):
        @pl.when(me != 2 * c + 1)
        def _():
            pl.semaphore_signal(
                barrier, inc=1, device_id={"seq": 2 * c + 1}, device_id_type=MESH
            )
    for d in range(1, kz):
        pl.semaphore_signal(
            barrier, inc=1, device_id={"seq": 2 * chip, "kvh": (zme + d) % kz},
            device_id_type=MESH,
        )

    def tell(hearing, count):
        @pl.when(core == hearing)
        def _():
            pl.semaphore_wait(barrier, count)
            pl.semaphore_signal(ready, inc=1, device_id={"seq": partner}, device_id_type=MESH)

    def hear(hearing):
        pl.when(core != hearing)(lambda: pl.semaphore_wait(ready, 1))

    loads = []

    def load(src, dst):
        copy = pltpu.make_async_copy(src, dst, load_sem.at[len(loads)])
        copy.start()
        loads.append(copy)
        return copy

    sel_load = load(sel_hbm, sel_ref)
    ck_load = load(ck_hbm, ck)
    cv_load = load(cv_hbm, cv)
    lens_load = load(lens_hbm, lens_ref)
    chunk_loads = []
    for c in range(HID_CHUNKS):
        part = pl.ds(c * step, step)
        chunk_loads.append(
            (
                load(hid_hbm.at[:, part], hid.at[:, part]),
                load(wk_hbm.at[part], wk.at[part]),
                load(wv_hbm.at[part], wv.at[part]),
            )
        )
    head_order = sorted(range(heads), key=lambda h: (1 - h % 2, h))
    wq_loads = {
        h: load(wq_hbm.at[:, pl.ds(h * qcols, qcols)], wq.at[:, pl.ds(h * qcols, qcols)])
        for h in head_order
    }

    def axes(h):
        if h % 2 == 0:
            return ib, rows_b, ia, rows_a
        return ia, rows_a, ib, rows_b

    def chip_at(h, q, k):
        return k * rows_b + q if h % 2 == 0 else q * rows_b + k

    def sends_kv(h, to):
        qc, nq, kc, nk = axes(h)
        if h % 2 == 0:
            return to > kc
        return (to != kc) & ((qc < nq - 1) | (to > kc))

    def takes_kv(h, source):
        qc, nq, kc, nk = axes(h)
        if h % 2 == 0:
            return source < kc
        return (source != kc) & ((qc < nq - 1) | (source < kc))

    def sends_q(h, to):
        qc, nq, kc, nk = axes(h)
        if h % 2 == 0:
            return (to != qc) & ((to < qc) | (kc > 0))
        return to < qc

    def takes_q(h, source):
        qc, nq, kc, nk = axes(h)
        if h % 2 == 0:
            return (source != qc) & ((source > qc) | (kc > 0))
        return source > qc

    def each(mine, count, want, body):
        def go(i, carry):
            pl.when(want(i))(functools.partial(body, i))
            return carry
        if count == 2:
            go(1 - mine, 0)
        else:
            lax.fori_loop(0, count, go, 0)

    def each_q(h, want, body):
        each(axes(h)[0], axes(h)[1], want, body)

    def each_k(h, want, body):
        each(axes(h)[2], axes(h)[3], want, body)

    def block(arr, h, slot, which, span):
        first, rows = spans[span]
        if arr == 0:
            return kall.at[h, slot, which, pl.ds(first, rows)]
        return vall.at[h, slot, which, pl.ds(0, HEAD_DIM), pl.ds(first, rows)]

    def move(arr, h, span, to):
        qc, nq, kc, nk = axes(h)
        first, rows = spans[span]
        src = ksend.at[h, pl.ds(first, rows)] if arr == 0 else vsend.at[h, :, pl.ds(first, rows)]
        return pltpu.make_async_remote_copy(
            src_ref=src, dst_ref=block(arr, h, kc, core, span),
            send_sem=mv_send.at[h, (to - kc - 1) % nk, span, arr],
            recv_sem=mv_recv.at[h, (kc - to - 1) % nk, span, arr],
            device_id={"seq": chip_at(h, qc, to) * 2 + core}, device_id_type=MESH,
        )

    def moved(arr, h, span, source):
        qc, nq, kc, nk = axes(h)
        index = (source - kc - 1) % nk
        view = block(arr, h, source, core, span)
        return pltpu.make_async_remote_copy(
            src_ref=view, dst_ref=view, send_sem=mv_send.at[h, index, span, arr],
            recv_sem=mv_recv.at[h, index, span, arr],
            device_id={"seq": partner}, device_id_type=MESH,
        )

    def forward(arr, h, slot, which, span):
        qc, nq, kc, nk = axes(h)
        view = block(arr, h, slot, which, span)
        if span == 2:
            send_sem, recv_sem = own_send.at[h, arr], own_recv.at[h, arr]
        else:
            index = (slot - kc - 1) % nk
            send_sem, recv_sem = fw_send.at[h, index, span, arr], fw_recv.at[h, index, span, arr]
        return pltpu.make_async_remote_copy(
            src_ref=view, dst_ref=view, send_sem=send_sem, recv_sem=recv_sem,
            device_id={"seq": partner}, device_id_type=MESH,
        )

    def urgent(h):
        return True if h % 2 == 0 else ia < rows_a - 1

    def send_blocks(arr, span, want=lambda h: True, only=range(2)):
        for h in range(heads):
            if h % 2 not in only:
                continue
            def go(to, h=h):
                move(arr, h, span, to).start()
            each_k(h, lambda to, h=h: sends_kv(h, to) & want(h), go)

    def shared_link(h, source):
        qc, nq, kc, nk = axes(h)
        return (source > kc) | (qc == nq - 1)

    def forward_blocks(h, span, want):
        def go(source):
            for arr in (0, 1):
                moved(arr, h, span, source).wait_recv()
                forward(arr, h, source, core, span).start()
        each_k(h, want, go)

    def arrive(h):
        def go(source):
            for span in (0, 1):
                for arr in (0, 1):
                    forward(arr, h, source, 1 - core, span).wait_recv()
        each_k(h, functools.partial(takes_kv, h), go)

    for h in range(heads):
        for i in range(kall.shape[1]):
            for c in range(2):
                vall[h, i, c, HEAD_DIM:, :] = jnp.ones((EXTRA, tok), jnp.bfloat16)
        for j in range(m_ref.shape[1]):
            m_ref[h, j] = jnp.full(m_ref.shape[2:], -1e30, jnp.float32)
            acc_ref[h, j] = jnp.zeros(acc_ref.shape[2:], jnp.float32)

    slot = lax.broadcasted_iota(jnp.int32, (8, pad), 1)
    sel_load.wait()

    def place(r, row):
        return jnp.where(slot == r, sel_ref[me * sel_rows + r], row)

    row_pos = lax.fori_loop(0, sel_rows, place, jnp.full((8, pad), -1, jnp.int32), unroll=8)[0:1]
    ck_load.wait()
    cv_load.wait()
    row_col = jnp.broadcast_to(row_pos.astype(jnp.float32), (LANES, pad)).T
    lane = lax.broadcasted_iota(jnp.int32, (pad, LANES), 1).astype(jnp.float32)
    pick = jnp.concatenate(
        [
            jnp.where(row_col == lane + float(k * LANES), 1.0, 0.0).astype(jnp.bfloat16)
            for k in range(tok // LANES)
        ],
        axis=1,
    )
    key_row = lax.broadcasted_iota(jnp.int32, (tok, pad), 0)
    pick_t = jnp.where(key_row == row_pos, 1.0, 0.0).astype(jnp.bfloat16)
    chosen_ref[...] = jnp.dot(
        pick_t, jnp.ones((pad, LANES), jnp.bfloat16), preferred_element_type=jnp.float32
    )
    bias_ref[...] = jnp.where(key_row <= row_pos, 0.0, -1e30)

    chosen = jnp.dot(jnp.ones((16, pad), jnp.bfloat16), pick, preferred_element_type=jnp.float32)
    upper = (
        lax.broadcasted_iota(jnp.int32, (LANES, LANES), 0)
        <= lax.broadcasted_iota(jnp.int32, (LANES, LANES), 1)
    ).astype(jnp.float32).astype(jnp.bfloat16)
    counts, before = [], jnp.zeros((1, 1), jnp.float32)
    for k in range(tok // LANES):
        tile = chosen[:, k * LANES:(k + 1) * LANES].astype(jnp.bfloat16)
        inner = jnp.dot(tile, upper, preferred_element_type=jnp.float32)[0:1]
        counts.append(inner + before)
        before = before + inner[:, LANES - 1:LANES]
    count = jnp.concatenate(counts, axis=1).astype(jnp.int32)
    token = lax.broadcasted_iota(jnp.int32, (1, tok), 1)
    target = jnp.where(chosen[0:1] > 0.5, plain + count - 1, token - count)

    def order(first, rows):
        row = lax.broadcasted_iota(jnp.int32, (rows, tok), 0) + first
        return jnp.where(row == target, 1.0, 0.0).astype(jnp.bfloat16)

    last_ref[...] = order(cut, tok - cut)
    early = order(0, cut)
    keys = jnp.dot(early, ck[...], preferred_element_type=jnp.float32).astype(jnp.bfloat16)
    values = jnp.dot(early, cv[...], preferred_element_type=jnp.float32)
    for h in range(heads):
        part = slice(h * HEAD_DIM, (h + 1) * HEAD_DIM)
        ksend[h, 0:cut, :] = keys[:, part]
        vsend[h, :, 0:cut] = values[:, part].T.astype(jnp.bfloat16)

    cols = q_cols(qrows)
    col_parts = [slice(j, j + cols) for j in range(0, qrows, cols)]

    def q_copy(h, to, index):
        qc, nq, kc, nk = axes(h)
        view = qbuf.at[h, qc, pl.ds(index * cols, cols)]
        return pltpu.make_async_remote_copy(
            src_ref=view, dst_ref=view, send_sem=q_send.at[h, (to - qc - 1) % nq, index],
            recv_sem=q_recv.at[h, (qc - to - 1) % nq, index],
            device_id={"seq": chip_at(h, to, kc) * 2 + core}, device_id_type=MESH,
        )

    def q_wait(h, source, index):
        qc, nq, kc, nk = axes(h)
        place = (source - qc - 1) % nq
        view = qbuf.at[h, source, pl.ds(index * cols, cols)]
        pltpu.make_async_remote_copy(
            src_ref=view, dst_ref=view, send_sem=q_send.at[h, place, index],
            recv_sem=q_recv.at[h, place, index], device_id={"seq": partner}, device_id_type=MESH,
        ).wait_recv()

    def store_queries(h, queries):
        scaled = (queries * EXP_SCALE).astype(jnp.bfloat16)
        for g in range(GROUP):
            qbuf[h, axes(h)[0], g * pad:(g + 1) * pad, :] = scaled[
                :, g * HEAD_DIM:(g + 1) * HEAD_DIM
            ]

    def send_queries(h):
        def go(to):
            for index in range(len(col_parts)):
                q_copy(h, to, index).start()

        each_q(h, functools.partial(sends_q, h), go)

    pieces = 2 if tok % (2 * LANES) == 0 else 1
    half = tok // pieces

    def fold(shift):
        square = shift * shift
        folded = square[:, 0:HEAD_DIM]
        for h in range(1, heads):
            folded = folded + square[:, h * HEAD_DIM:(h + 1) * HEAD_DIM]
        return jnp.sum(folded.T, axis=0, keepdims=True)

    def project(h):
        return jnp.dot(
            hq[...], wq[:, h * qcols:(h + 1) * qcols], preferred_element_type=jnp.float32
        )

    def project_chunk(c):
        part = slice(c * step, (c + 1) * step)
        for weight, total in ((wk, kacc), (wv, vacc)):
            fresh = jnp.dot(hid[:, part], weight[part, :], preferred_element_type=jnp.float32)
            total[...] = fresh if c == 0 else total[...] + fresh
        picked = jnp.dot(pick, hid[:, part], preferred_element_type=jnp.float32)
        hq[:, part] = picked.astype(jnp.bfloat16)
    tell(1, n - 1)
    hear(1)
    send_blocks(0, 0)
    send_blocks(1, 0)
    for c in range(HID_CHUNKS):
        for copy in chunk_loads[c]:
            copy.wait()
        project_chunk(c)
    if kz > 1:
        tell(0, 2 * (kz - 1))
    first, rest = head_order[0], head_order[1:]
    wq_loads[first].wait()
    queries = project(first)
    mask = [
        jnp.concatenate([chosen_ref[p * half:(p + 1) * half, :]] * heads, axis=1) > 0.5
        for p in range(pieces)
    ]
    for p in range(pieces):
        rows = slice(p * half, (p + 1) * half)
        cached = ck[rows, :].astype(jnp.float32)
        used = jnp.where(mask[p], kacc[rows, :], cached).astype(jnp.bfloat16)
        for h in range(heads):
            kall[h, axes(h)[2], core, rows, :] = used[:, h * HEAD_DIM:(h + 1) * HEAD_DIM]
    store_queries(first, queries)
    send_queries(first)
    for h in range(heads):
        forward(0, h, axes(h)[2], core, 2).start()
    for h in rest:
        wq_loads[h].wait()
    queries = {h: project(h) for h in rest}
    for p in range(pieces):
        rows = slice(p * half, (p + 1) * half)
        cached_k = ck[rows, :].astype(jnp.float32)
        cached_v = cv[rows, :].astype(jnp.float32)
        used = jnp.where(mask[p], vacc[rows, :], cached_v).T.astype(jnp.bfloat16)
        for h in range(heads):
            part = slice(h * HEAD_DIM, (h + 1) * HEAD_DIM)
            vall[h, axes(h)[2], core, 0:HEAD_DIM, rows] = used[part, :]
        devbuf[zme, :, rows] = fold(kacc[rows, :] - cached_k) + fold(vacc[rows, :] - cached_v)
    for h in range(heads):
        ksend[h, cut:tok, :] = jnp.dot(
            last_ref[...], kall[h, axes(h)[2], core], preferred_element_type=jnp.float32
        ).astype(jnp.bfloat16)
        vsend[h, :, cut:tok] = lax.dot_general(
            vall[h, axes(h)[2], core, 0:HEAD_DIM, :], last_ref[...], NT,
            preferred_element_type=jnp.float32,
        ).astype(jnp.bfloat16)
    for h in rest:
        store_queries(h, queries[h])
    for h in range(heads):
        forward(1, h, axes(h)[2], core, 2).start()
    send_blocks(0, 1, urgent)
    send_blocks(1, 1, urgent)
    for h in rest:
        send_queries(h)
    for arr in (0, 1):
        send_blocks(arr, 1, lambda h: jnp.logical_not(urgent(h)), (1,))
    sends = []
    if kz > 1:
        hear(0)
    for d in range(1, kz):
        sends.append(
            pltpu.make_async_remote_copy(
                src_ref=devbuf.at[zme], dst_ref=devbuf.at[zme], send_sem=z_send.at[d - 1],
                recv_sem=z_recv.at[kz - d - 1], device_id={"kvh": (zme + d) % kz},
                device_id_type=MESH,
            )
        )
        sends[-1].start()

    def run(items, answers=()):
        def scores_of(item):
            h, q, k, which, part, masked = item
            s = lax.dot_general(
                kall[h, k, which], qbuf[h, q, part, :], NT, preferred_element_type=jnp.float32
            )
            if masked:
                s = s + jnp.concatenate([bias_ref[...]] * GROUP, axis=1)
            return s

        scores = scores_of(items[0])
        for i, (h, q, k, which, part, masked) in enumerate(items):
            following = scores_of(items[i + 1]) if i + 1 < len(items) else None
            best = jnp.max(scores, axis=0, keepdims=True)
            weights = jnp.exp2(scores - best).astype(jnp.bfloat16)
            mixed = jnp.dot(vall[h, k, which], weights, preferred_element_type=jnp.float32)
            if not masked:
                old = m_ref[h, q, 0:1, part]
                top = jnp.maximum(old, best)
                mixed = mixed * jnp.exp2(best - top)
                mixed = mixed + acc_ref[h, q, :, part] * jnp.exp2(old - top)
                best = top
            m_ref[h, q, 0:1, part] = best
            acc_ref[h, q, :, part] = mixed
            scores = following
            if answers and (i + 1) % (len(items) // len(answers)) == 0:
                give_back(h, q, answers[i * len(answers) // len(items)])

    lanes = (core, 1 - core)
    wide = slice(0, qrows)

    def both(h, q, k):
        run([(h, q, k, c, wide, False) for c in lanes])

    every = range(len(col_parts))

    def serve(h, q, k, lanes, wait=False, answer=False, indices=every):
        items = {x: [(h, q, k, c, col_parts[x], False) for c in lanes] for x in indices}
        if wait:
            for index in indices:
                q_wait(h, q, index)
                run(items[index], [index] if answer else ())
            return
        run(sum(items.values(), []), indices if answer else ())

    def p_copies(h, to, index):
        qc, nq, kc, nk = axes(h)
        dest = {"seq": chip_at(h, to, kc) * 2 + core}
        return [
            pltpu.make_async_remote_copy(
                src_ref=pout.at[h, to, index], dst_ref=pin.at[h, qc, index],
                send_sem=p_send.at[h, (to - qc - 1) % nq, index, 0],
                recv_sem=p_recv.at[h, (qc - to - 1) % nq, index, 0],
                device_id=dest, device_id_type=MESH,
            ),
            pltpu.make_async_remote_copy(
                src_ref=pout_stat.at[h, to, index], dst_ref=pin_stat.at[h, qc, index],
                send_sem=p_send.at[h, (to - qc - 1) % nq, index, 1],
                recv_sem=p_recv.at[h, (qc - to - 1) % nq, index, 1],
                device_id=dest, device_id_type=MESH,
            ),
        ]

    def p_wait(h, source, index):
        qc, nq, kc, nk = axes(h)
        place = (source - qc - 1) % nq
        for i, buf in enumerate((pin, pin_stat)):
            view = buf.at[h, source, index]
            pltpu.make_async_remote_copy(
                src_ref=view, dst_ref=view, send_sem=p_send.at[h, place, index, i],
                recv_sem=p_recv.at[h, place, index, i], device_id={"seq": partner},
                device_id_type=MESH,
            ).wait_recv()

    def give_back(h, to, index):
        part = col_parts[index]
        pout[h, to, index] = acc_ref[h, to, 0:HEAD_DIM, part].astype(jnp.bfloat16)
        pout_stat[h, to, index, 0:1, :] = m_ref[h, to, 0:1, part]
        pout_stat[h, to, index, 1:2, :] = acc_ref[h, to, HEAD_DIM:HEAD_DIM + 1, part]
        for copy in p_copies(h, to, index):
            copy.start()

    def no_moved(h):
        qc, nq, kc, nk = axes(h)
        return kc == 0 if h % 2 == 0 else nk == 1
    run(
        [
            (h, axes(h)[0], axes(h)[2], core, wide, True)
            for h in range(heads)
        ]
    )
    for h in range(heads):
        for arr in (0, 1):
            forward(arr, h, axes(h)[2], 1 - core, 2).wait_recv()
    @pl.when(core == 1)
    def _():
        run(
            [
                (h, axes(h)[0], axes(h)[2], 0, wide, False)
                for h in range(heads)
            ]
        )

    def serve_own(h, early):
        qc, nq, kc, nk = axes(h)
        alone = no_moved(h)

        def part(j, index):
            serve(h, j, kc, lanes, True, False, (index,))

        def answer(j, index):
            pl.when(alone)(lambda: give_back(h, j, index))

        def go(j):
            if early:
                @pl.when(alone)
                def _():
                    part(j, 0)
                    give_back(h, j, 0)
                return
            pl.when(jnp.logical_not(alone))(lambda: part(j, 0))
            for index in every[1:]:
                part(j, index)
                answer(j, index)

        each_q(h, lambda j: j > qc, go)

    def moved_wanted(h, j):
        return takes_q(h, j) & jnp.logical_not(no_moved(h))

    def near_lane(h):
        qc, nq, kc, nk = axes(h)
        if nk == 2:
            each_q(
                h, functools.partial(moved_wanted, h), lambda j: serve(h, j, 1 - kc, lanes[:1])
            )

    def far_lane(h):
        qc, nq, kc, nk = axes(h)

        def go(j):
            each_k(h, functools.partial(takes_kv, h), lambda i: both(h, j, i))
            for index in every:
                give_back(h, j, index)

        pl.when(ia < rows_a - 1)(lambda: arrive(h))
        if nk == 2:
            each_q(
                h, functools.partial(moved_wanted, h),
                lambda j: serve(h, j, 1 - kc, lanes[1:], False, True),
            )
        else:
            each_q(h, functools.partial(moved_wanted, h), go)

    def earlier(h, j):
        other = 1 - axes(h)[2]
        serve(h, j, other, lanes, True, True, every[:1])
        if h == 0 and halved:
            pl.when(corner)(exchange)
        serve(h, j, other, lanes, True, True, every[1:])

    def serve_moved(h):
        qc, nq, kc, nk = axes(h)

        def go(j):
            @pl.when(j < qc)
            def _():
                for index in every:
                    q_wait(h, j, index)
            each_k(h, functools.partial(takes_kv, h), lambda i: both(h, j, i))
            for index in every:
                give_back(h, j, index)

        arrive(h)
        if nk == 2:
            each_q(
                h, lambda j: moved_wanted(h, j) & (j < qc),
                functools.partial(earlier, h),
            )
            each_q(
                h, lambda j: moved_wanted(h, j) & (j > qc),
                lambda j: serve(h, j, 1 - kc, lanes, False, True),
            )
        else:
            each_q(h, functools.partial(moved_wanted, h), go)

    def spans_of():
        position = token + me * tok
        inside = []
        end = jnp.int32(0)
        for d in range(docs):
            begin, end = end, end + lens_ref[d]
            inside.append((position >= begin) & (position < end))
        return inside

    def doc_copy(d):
        return pltpu.make_async_remote_copy(
            src_ref=docbuf.at[me], dst_ref=docbuf.at[me], send_sem=doc_send.at[d - 1],
            recv_sem=doc_recv.at[n - d - 1], device_id={"seq": (me + d) % n},
            device_id_type=MESH,
        )

    def exchange():
        for d in range(1, kz):
            src = (zme + d) % kz
            pltpu.make_async_remote_copy(
                src_ref=devbuf.at[src], dst_ref=devbuf.at[src], send_sem=z_send.at[0],
                recv_sem=z_recv.at[d - 1], device_id={"kvh": src}, device_id_type=MESH,
            ).wait_recv()
        deviation = devbuf[0]
        for z in range(1, kz):
            deviation = deviation + devbuf[z]
        dev_ref[...] = deviation
        inside = spans_of()
        slot_row = lax.broadcasted_iota(jnp.int32, docbuf.shape[1:], 0)
        shares = jnp.zeros(docbuf.shape[1:], jnp.float32)
        for d in range(docs):
            share = jnp.sum(jnp.where(inside[d], deviation, 0.0), axis=1, keepdims=True)
            shares = jnp.where(slot_row == d, share, shares)
        docbuf[me] = shares
        for d in range(1, n):
            doc_copy(d).start()

    lens_load.wait()
    for h in range(1, heads, 2):
        serve_own(h, True)
        serve_own(h, False)
    for h in range(heads):
        forward_blocks(h, 0, functools.partial(takes_kv, h))
        if h % 2 == 0:
            forward_blocks(h, 1, functools.partial(takes_kv, h))
        else:
            forward_blocks(
                h, 1, lambda i, h=h: takes_kv(h, i) & jnp.logical_not(shared_link(h, i))
            )
    for h in range(1, heads, 2):
        forward_blocks(
            h, 1, lambda i, h=h: takes_kv(h, i) & shared_link(h, i) & (ia < rows_a - 1)
        )
    for h in range(1, heads, 2):
        near_lane(h)
    pl.when(ia < rows_a - 1)(exchange)
    for h in range(0, heads, 2):
        serve_own(h, True)
    for h in range(1, heads, 2):
        far_lane(h)
    for h in range(0, heads, 2):
        serve_own(h, False)
    last_row = ia == rows_a - 1
    halved = rows_a == 2 and rows_b == 2 and len(col_parts) > 1
    corner = last_row & (ib == rows_b - 1) if halved else False
    pl.when(last_row & jnp.logical_not(corner))(exchange)
    for h in range(0, heads, 2):
        serve_moved(h)
    for h in range(1, heads, 2):
        forward_blocks(h, 1, lambda i, h=h: takes_kv(h, i) & (ia == rows_a - 1))
    for h in range(heads):
        qc, nq, kc, nk = axes(h)
        if h % 2 == 1:
            pl.when(ia == rows_a - 1)(functools.partial(arrive, h))
        each_k(h, lambda i, kc=kc: i < kc, lambda i, h=h, qc=qc: both(h, qc, i))
    for h in range(heads):
        qc, nq, kc, nk = axes(h)

        def collect(source, h=h, qc=qc):
            for index, part in enumerate(col_parts):
                p_wait(h, source, index)
                best = m_ref[h, qc, 0:1, part]
                other = pin_stat[h, source, index, 0:1, :]
                top = jnp.maximum(best, other)
                fade, rise = jnp.exp2(best - top), jnp.exp2(other - top)
                m_ref[h, qc, 0:1, part] = top
                acc_ref[h, qc, 0:HEAD_DIM, part] = (
                    acc_ref[h, qc, 0:HEAD_DIM, part] * fade
                    + pin[h, source, index].astype(jnp.float32) * rise
                )
                acc_ref[h, qc, HEAD_DIM:HEAD_DIM + 1, part] = (
                    acc_ref[h, qc, HEAD_DIM:HEAD_DIM + 1, part] * fade
                    + pin_stat[h, source, index, 1:2, :] * rise
                )

        each_q(h, functools.partial(sends_q, h), collect)
        done = acc_ref[h, qc, 0:HEAD_DIM, :] / acc_ref[h, qc, HEAD_DIM:HEAD_DIM + 1, :]
        for g in range(GROUP):
            head = h * GROUP + g
            rows = done[:, g * pad:(g + 1) * pad].T.astype(jnp.bfloat16)
            out_ref[:, head * HEAD_DIM:(head + 1) * HEAD_DIM] = rows[0:sel_rows]
    for d in range(1, n):
        src = (me + d) % n
        pltpu.make_async_remote_copy(
            src_ref=docbuf.at[src], dst_ref=docbuf.at[src], send_sem=doc_send.at[0],
            recv_sem=doc_recv.at[d - 1], device_id={"seq": src}, device_id_type=MESH,
        ).wait_recv()
    inside = spans_of()
    totals = docbuf[0]
    for s in range(1, n):
        totals = totals + docbuf[s]
    mean = jnp.zeros((1, tok), jnp.float32)
    for d in range(docs):
        here = totals[d:d + 1, 0:1] / lens_ref[d].astype(jnp.float32)
        mean = jnp.where(inside[d], here, mean)
    score_ref[...] = dev_ref[...] / (mean + 1.0)
    for send in sends:
        send.wait_send()
    for d in range(1, n):
        doc_copy(d).wait_send()
    for h in range(heads):
        qc, nq, kc, nk = axes(h)

        def drain_kv(to, h=h):
            for span in (0, 1):
                for arr in (0, 1):
                    move(arr, h, span, to).wait_send()

        def drain_forward(source, h=h):
            for span in (0, 1):
                for arr in (0, 1):
                    forward(arr, h, source, core, span).wait_send()

        def drain_p(to, h=h):
            for index in range(len(col_parts)):
                for copy in p_copies(h, to, index):
                    copy.wait_send()

        for arr in (0, 1):
            forward(arr, h, kc, core, 2).wait_send()
        each_k(h, functools.partial(sends_kv, h), drain_kv)
        each_k(h, functools.partial(takes_kv, h), drain_forward)

        def drain_q(to, h=h):
            for index in range(len(col_parts)):
                q_copy(h, to, index).wait_send()

        each_q(h, functools.partial(sends_q, h), drain_q)
        each_q(h, functools.partial(takes_q, h), drain_p)


def shards(n, kz, hidden, w_query, w_key, w_value, cached_key, cached_value, doc_lengths, selected):
    tok, width = hidden.shape
    cols = w_key.shape[1]
    qcols = w_query.shape[1]
    sel_rows = selected.shape[0] // n
    docs = doc_lengths.shape[0]
    pad = round_up(sel_rows, LANES)
    heads = cols // HEAD_DIM
    qrows = GROUP * pad
    cut = (tok - sel_rows) // LANES * LANES
    cut_q = q_cols(qrows)
    side = max(split_chips(n // 2))
    others = max(1, side - 1)
    bf, f32 = jnp.bfloat16, jnp.float32
    dma = pltpu.SemaphoreType.DMA
    hbm = pl.BlockSpec(memory_space=pltpu.HBM)
    vmem = pl.BlockSpec(memory_space=pltpu.VMEM)
    attended, score = pl.pallas_call(
        functools.partial(kernel, n, kz, docs, sel_rows),
        out_shape=(
            pltpu.VMEM((sel_rows, qcols), bf),
            pltpu.VMEM((1, tok), f32),
        ),
        in_specs=[hbm] * 8,
        out_specs=(vmem, vmem),
        scratch_shapes=[
            pltpu.VMEM((tok, width), bf),
            pltpu.VMEM((width, qcols), bf),
            pltpu.VMEM((width, cols), bf),
            pltpu.VMEM((width, cols), bf),
            pltpu.VMEM((tok, cols), bf),
            pltpu.VMEM((tok, cols), bf),
            pltpu.VMEM((pad, width), bf),
            pltpu.VMEM((heads, side, 2, tok, HEAD_DIM), bf),
            pltpu.VMEM((heads, side, 2, HEAD_DIM + EXTRA, tok), bf),
            pltpu.VMEM((heads, tok, HEAD_DIM), bf),
            pltpu.VMEM((heads, HEAD_DIM, tok), bf),
            pltpu.VMEM((heads, side, qrows, HEAD_DIM), bf),
            pltpu.VMEM((heads, side, qrows // cut_q, HEAD_DIM, cut_q), bf),
            pltpu.VMEM((heads, side, qrows // cut_q, 2, cut_q), f32),
            pltpu.VMEM((heads, side, qrows // cut_q, HEAD_DIM, cut_q), bf),
            pltpu.VMEM((heads, side, qrows // cut_q, 2, cut_q), f32),
            pltpu.VMEM((tok, cols), f32),
            pltpu.VMEM((tok, cols), f32),
            pltpu.VMEM((heads, side, 8, qrows), f32),
            pltpu.VMEM((heads, side, HEAD_DIM + EXTRA, qrows), f32),
            pltpu.VMEM((tok, pad), f32),
            pltpu.VMEM((tok, LANES), f32),
            pltpu.VMEM((tok - cut, tok), bf),
            pltpu.VMEM((1, tok), f32),
            pltpu.VMEM((kz, 1, tok), f32),
            pltpu.VMEM((n, round_up(docs, 8), 128), f32),
            pltpu.SMEM(doc_lengths.shape, jnp.int32),
            pltpu.SMEM(selected.shape, jnp.int32),
            dma((3 * HID_CHUNKS + 4 + heads,)),
            dma((heads, others, qrows // cut_q)),
            dma((heads, others, qrows // cut_q)),
            dma((heads, others, qrows // cut_q, 2)),
            dma((heads, others, qrows // cut_q, 2)),
            dma((heads, others, 2, 2)),
            dma((heads, others, 2, 2)),
            dma((heads, others, 2, 2)),
            dma((heads, others, 2, 2)),
            dma((heads, 2)),
            dma((heads, 2)),
            dma((max(1, kz - 1),)),
            dma((max(1, kz - 1),)),
            dma((n - 1,)),
            dma((n - 1,)),
            pltpu.SemaphoreType.REGULAR,
        ],
        compiler_params=pltpu.CompilerParams(
            collective_id=0, has_side_effects=True, vmem_limit_bytes=56 * 1024 * 1024
        ),
        name="blend",
    )(hidden, w_query, w_key, w_value, cached_key, cached_value, doc_lengths, selected)
    return attended, score.reshape(tok)


def solution(mesh):
    return jax.shard_map(
        functools.partial(shards, mesh.shape["seq"], mesh.shape["kvh"]),
        mesh=mesh,
        in_specs=(
            P("seq", None),
            P(None, "kvh"),
            P(None, "kvh"),
            P(None, "kvh"),
            P("seq", "kvh"),
            P("seq", "kvh"),
            P(),
            P(),
        ),
        out_specs=(P("seq", "kvh"), P("seq")),
        check_vma=False,
    )
```

```python
import functools
import math

import jax
import jax.numpy as jnp
from jax import lax
from jax.experimental import pallas as pl
from jax.experimental.pallas import tpu as pltpu
from jax.sharding import PartitionSpec as P

HEADS = 32
KV_HEADS = 8
HEAD_DIM = 128
GROUP = HEADS // KV_HEADS
EXP_SCALE = HEAD_DIM ** (-0.5) * math.log2(math.e)
MESH = pl.DeviceIdType.MESH
NT = (((1,), (1,)), ((), ()))
LANES = 128
EXTRA = 16
HID_CHUNKS = 4


def round_up(a, b):
    return -(-a // b) * b


def q_cols(rows):
    return 2 * LANES if rows % (2 * LANES) == 0 else LANES


def split_chips(chips):
    small = max(a for a in range(1, math.isqrt(chips) + 1) if chips % a == 0)
    return small, chips // small


def kernel(
    n, kz, docs, sel_rows,
    hid_hbm, wq_hbm, wk_hbm, wv_hbm, ck_hbm, cv_hbm, lens_hbm, sel_hbm,
    out_ref, score_ref,
    hid, wq, wk, wv, ck, cv, hq, kall, vall, ksend, vsend, qbuf, pout, pout_stat, pin, pin_stat,
    kacc, vacc, m_ref, acc_ref, bias_ref, chosen_ref, last_ref, dev_ref, devbuf, docbuf, lens_ref, sel_ref,
    load_sem, q_send, q_recv, p_send, p_recv, mv_send, mv_recv, fw_send, fw_recv, own_send, own_recv,
    z_send, z_recv, doc_send, doc_recv, ready,
):
    tok, width = hid.shape
    heads = wk.shape[1] // HEAD_DIM
    pad = hq.shape[0]
    qrows = GROUP * pad
    qcols = GROUP * HEAD_DIM
    plain = tok - sel_rows
    cut = plain // LANES * LANES
    spans = ((0, cut), (cut, tok - cut), (0, tok))
    rows_a, rows_b = split_chips(n // 2)
    me = lax.axis_index("seq")
    zme = lax.axis_index("kvh")
    core = me % 2
    chip = me // 2
    ia, ib = chip // rows_b, chip % rows_b
    partner = me + 1 - 2 * core
    step = width // HID_CHUNKS
    barrier = pltpu.get_barrier_semaphore()
    for c in range(n // 2):
        @pl.when(me != 2 * c + 1)
        def _():
            pl.semaphore_signal(
                barrier, inc=1, device_id={"seq": 2 * c + 1}, device_id_type=MESH
            )
    for d in range(1, kz):
        pl.semaphore_signal(
            barrier, inc=1, device_id={"seq": 2 * chip, "kvh": (zme + d) % kz},
            device_id_type=MESH,
        )

    def tell(hearing, count):
        @pl.when(core == hearing)
        def _():
            pl.semaphore_wait(barrier, count)
            pl.semaphore_signal(ready, inc=1, device_id={"seq": partner}, device_id_type=MESH)

    def hear(hearing):
        pl.when(core != hearing)(lambda: pl.semaphore_wait(ready, 1))

    loads = []

    def load(src, dst):
        copy = pltpu.make_async_copy(src, dst, load_sem.at[len(loads)])
        copy.start()
        loads.append(copy)
        return copy

    sel_load = load(sel_hbm, sel_ref)
    ck_load = load(ck_hbm, ck)
    cv_load = load(cv_hbm, cv)
    lens_load = load(lens_hbm, lens_ref)
    chunk_loads = []
    for c in range(HID_CHUNKS):
        part = pl.ds(c * step, step)
        chunk_loads.append(
            (
                load(hid_hbm.at[:, part], hid.at[:, part]),
                load(wk_hbm.at[part], wk.at[part]),
                load(wv_hbm.at[part], wv.at[part]),
            )
        )
    head_order = sorted(range(heads), key=lambda h: (1 - h % 2, h))
    wq_loads = {
        h: load(wq_hbm.at[:, pl.ds(h * qcols, qcols)], wq.at[:, pl.ds(h * qcols, qcols)])
        for h in head_order
    }

    def axes(h):
        if h % 2 == 0:
            return ib, rows_b, ia, rows_a
        return ia, rows_a, ib, rows_b

    def chip_at(h, q, k):
        return k * rows_b + q if h % 2 == 0 else q * rows_b + k

    def sends_kv(h, to):
        qc, nq, kc, nk = axes(h)
        if h % 2 == 0:
            return to > kc
        return (to != kc) & ((qc < nq - 1) | (to > kc))

    def takes_kv(h, source):
        qc, nq, kc, nk = axes(h)
        if h % 2 == 0:
            return source < kc
        return (source != kc) & ((qc < nq - 1) | (source < kc))

    def sends_q(h, to):
        qc, nq, kc, nk = axes(h)
        if h % 2 == 0:
            return (to != qc) & ((to < qc) | (kc > 0))
        return to < qc

    def takes_q(h, source):
        qc, nq, kc, nk = axes(h)
        if h % 2 == 0:
            return (source != qc) & ((source > qc) | (kc > 0))
        return source > qc

    def each(mine, count, want, body):
        def go(i, carry):
            pl.when(want(i))(functools.partial(body, i))
            return carry
        if count == 2:
            go(1 - mine, 0)
        else:
            lax.fori_loop(0, count, go, 0)

    def each_q(h, want, body):
        each(axes(h)[0], axes(h)[1], want, body)

    def each_k(h, want, body):
        each(axes(h)[2], axes(h)[3], want, body)

    def block(arr, h, slot, which, span):
        first, rows = spans[span]
        if arr == 0:
            return kall.at[h, slot, which, pl.ds(first, rows)]
        return vall.at[h, slot, which, pl.ds(0, HEAD_DIM), pl.ds(first, rows)]

    def move(arr, h, span, to):
        qc, nq, kc, nk = axes(h)
        first, rows = spans[span]
        src = ksend.at[h, pl.ds(first, rows)] if arr == 0 else vsend.at[h, :, pl.ds(first, rows)]
        return pltpu.make_async_remote_copy(
            src_ref=src, dst_ref=block(arr, h, kc, core, span),
            send_sem=mv_send.at[h, (to - kc - 1) % nk, span, arr],
            recv_sem=mv_recv.at[h, (kc - to - 1) % nk, span, arr],
            device_id={"seq": chip_at(h, qc, to) * 2 + core}, device_id_type=MESH,
        )

    def moved(arr, h, span, source):
        qc, nq, kc, nk = axes(h)
        index = (source - kc - 1) % nk
        view = block(arr, h, source, core, span)
        return pltpu.make_async_remote_copy(
            src_ref=view, dst_ref=view, send_sem=mv_send.at[h, index, span, arr],
            recv_sem=mv_recv.at[h, index, span, arr],
            device_id={"seq": partner}, device_id_type=MESH,
        )

    def forward(arr, h, slot, which, span):
        qc, nq, kc, nk = axes(h)
        view = block(arr, h, slot, which, span)
        if span == 2:
            send_sem, recv_sem = own_send.at[h, arr], own_recv.at[h, arr]
        else:
            index = (slot - kc - 1) % nk
            send_sem, recv_sem = fw_send.at[h, index, span, arr], fw_recv.at[h, index, span, arr]
        return pltpu.make_async_remote_copy(
            src_ref=view, dst_ref=view, send_sem=send_sem, recv_sem=recv_sem,
            device_id={"seq": partner}, device_id_type=MESH,
        )

    def urgent(h):
        return True if h % 2 == 0 else ia < rows_a - 1

    def send_blocks(arr, span, want=lambda h: True, only=range(2)):
        for h in range(heads):
            if h % 2 not in only:
                continue
            def go(to, h=h):
                move(arr, h, span, to).start()
            each_k(h, lambda to, h=h: sends_kv(h, to) & want(h), go)

    def shared_link(h, source):
        qc, nq, kc, nk = axes(h)
        return (source > kc) | (qc == nq - 1)

    def forward_blocks(h, span, want):
        def go(source):
            for arr in (0, 1):
                moved(arr, h, span, source).wait_recv()
                forward(arr, h, source, core, span).start()
        each_k(h, want, go)

    def arrive(h):
        def go(source):
            for span in (0, 1):
                for arr in (0, 1):
                    forward(arr, h, source, 1 - core, span).wait_recv()
        each_k(h, functools.partial(takes_kv, h), go)

    for h in range(heads):
        for i in range(kall.shape[1]):
            for c in range(2):
                vall[h, i, c, HEAD_DIM:, :] = jnp.ones((EXTRA, tok), jnp.bfloat16)
        for j in range(m_ref.shape[1]):
            m_ref[h, j] = jnp.full(m_ref.shape[2:], -1e30, jnp.float32)
            acc_ref[h, j] = jnp.zeros(acc_ref.shape[2:], jnp.float32)

    slot = lax.broadcasted_iota(jnp.int32, (8, pad), 1)
    sel_load.wait()

    def place(r, row):
        return jnp.where(slot == r, sel_ref[me * sel_rows + r], row)

    row_pos = lax.fori_loop(0, sel_rows, place, jnp.full((8, pad), -1, jnp.int32), unroll=8)[0:1]
    ck_load.wait()
    cv_load.wait()
    row_col = jnp.broadcast_to(row_pos.astype(jnp.float32), (LANES, pad)).T
    lane = lax.broadcasted_iota(jnp.int32, (pad, LANES), 1).astype(jnp.float32)
    pick = jnp.concatenate(
        [
            jnp.where(row_col == lane + float(k * LANES), 1.0, 0.0).astype(jnp.bfloat16)
            for k in range(tok // LANES)
        ],
        axis=1,
    )
    key_row = lax.broadcasted_iota(jnp.int32, (tok, pad), 0)
    pick_t = jnp.where(key_row == row_pos, 1.0, 0.0).astype(jnp.bfloat16)
    chosen_ref[...] = jnp.dot(
        pick_t, jnp.ones((pad, LANES), jnp.bfloat16), preferred_element_type=jnp.float32
    )
    bias_ref[...] = jnp.where(key_row <= row_pos, 0.0, -1e30)

    chosen = jnp.dot(jnp.ones((16, pad), jnp.bfloat16), pick, preferred_element_type=jnp.float32)
    upper = (
        lax.broadcasted_iota(jnp.int32, (LANES, LANES), 0)
        <= lax.broadcasted_iota(jnp.int32, (LANES, LANES), 1)
    ).astype(jnp.float32).astype(jnp.bfloat16)
    counts, before = [], jnp.zeros((1, 1), jnp.float32)
    for k in range(tok // LANES):
        tile = chosen[:, k * LANES:(k + 1) * LANES].astype(jnp.bfloat16)
        inner = jnp.dot(tile, upper, preferred_element_type=jnp.float32)[0:1]
        counts.append(inner + before)
        before = before + inner[:, LANES - 1:LANES]
    count = jnp.concatenate(counts, axis=1).astype(jnp.int32)
    token = lax.broadcasted_iota(jnp.int32, (1, tok), 1)
    target = jnp.where(chosen[0:1] > 0.5, plain + count - 1, token - count)

    def order(first, rows):
        row = lax.broadcasted_iota(jnp.int32, (rows, tok), 0) + first
        return jnp.where(row == target, 1.0, 0.0).astype(jnp.bfloat16)

    last_ref[...] = order(cut, tok - cut)
    early = order(0, cut)
    keys = jnp.dot(early, ck[...], preferred_element_type=jnp.float32).astype(jnp.bfloat16)
    values = jnp.dot(early, cv[...], preferred_element_type=jnp.float32)
    for h in range(heads):
        part = slice(h * HEAD_DIM, (h + 1) * HEAD_DIM)
        ksend[h, 0:cut, :] = keys[:, part]
        vsend[h, :, 0:cut] = values[:, part].T.astype(jnp.bfloat16)

    cols = q_cols(qrows)
    col_parts = [slice(j, j + cols) for j in range(0, qrows, cols)]

    def q_copy(h, to, index):
        qc, nq, kc, nk = axes(h)
        view = qbuf.at[h, qc, pl.ds(index * cols, cols)]
        return pltpu.make_async_remote_copy(
            src_ref=view, dst_ref=view, send_sem=q_send.at[h, (to - qc - 1) % nq, index],
            recv_sem=q_recv.at[h, (qc - to - 1) % nq, index],
            device_id={"seq": chip_at(h, to, kc) * 2 + core}, device_id_type=MESH,
        )

    def q_wait(h, source, index):
        qc, nq, kc, nk = axes(h)
        place = (source - qc - 1) % nq
        view = qbuf.at[h, source, pl.ds(index * cols, cols)]
        pltpu.make_async_remote_copy(
            src_ref=view, dst_ref=view, send_sem=q_send.at[h, place, index],
            recv_sem=q_recv.at[h, place, index], device_id={"seq": partner}, device_id_type=MESH,
        ).wait_recv()

    def store_queries(h, queries):
        scaled = (queries * EXP_SCALE).astype(jnp.bfloat16)
        for g in range(GROUP):
            qbuf[h, axes(h)[0], g * pad:(g + 1) * pad, :] = scaled[
                :, g * HEAD_DIM:(g + 1) * HEAD_DIM
            ]

    def send_queries(h):
        def go(to):
            for index in range(len(col_parts)):
                q_copy(h, to, index).start()

        each_q(h, functools.partial(sends_q, h), go)

    pieces = 2 if tok % (2 * LANES) == 0 else 1
    half = tok // pieces

    def fold(shift):
        square = shift * shift
        folded = square[:, 0:HEAD_DIM]
        for h in range(1, heads):
            folded = folded + square[:, h * HEAD_DIM:(h + 1) * HEAD_DIM]
        return jnp.sum(folded.T, axis=0, keepdims=True)

    def project(h):
        return jnp.dot(
            hq[...], wq[:, h * qcols:(h + 1) * qcols], preferred_element_type=jnp.float32
        )

    def project_chunk(c):
        part = slice(c * step, (c + 1) * step)
        for weight, total in ((wk, kacc), (wv, vacc)):
            fresh = jnp.dot(hid[:, part], weight[part, :], preferred_element_type=jnp.float32)
            total[...] = fresh if c == 0 else total[...] + fresh
        picked = jnp.dot(pick, hid[:, part], preferred_element_type=jnp.float32)
        hq[:, part] = picked.astype(jnp.bfloat16)
    tell(1, n - 1)
    hear(1)
    send_blocks(0, 0)
    send_blocks(1, 0)
    for c in range(HID_CHUNKS):
        for copy in chunk_loads[c]:
            copy.wait()
        project_chunk(c)
    if kz > 1:
        tell(0, 2 * (kz - 1))
    first, rest = head_order[0], head_order[1:]
    wq_loads[first].wait()
    queries = project(first)
    mask = [
        jnp.concatenate([chosen_ref[p * half:(p + 1) * half, :]] * heads, axis=1) > 0.5
        for p in range(pieces)
    ]
    for p in range(pieces):
        rows = slice(p * half, (p + 1) * half)
        cached = ck[rows, :].astype(jnp.float32)
        used = jnp.where(mask[p], kacc[rows, :], cached).astype(jnp.bfloat16)
        for h in range(heads):
            kall[h, axes(h)[2], core, rows, :] = used[:, h * HEAD_DIM:(h + 1) * HEAD_DIM]
    store_queries(first, queries)
    send_queries(first)
    for h in range(heads):
        forward(0, h, axes(h)[2], core, 2).start()
    for h in rest:
        wq_loads[h].wait()
    queries = {h: project(h) for h in rest}
    for p in range(pieces):
        rows = slice(p * half, (p + 1) * half)
        cached_k = ck[rows, :].astype(jnp.float32)
        cached_v = cv[rows, :].astype(jnp.float32)
        used = jnp.where(mask[p], vacc[rows, :], cached_v).T.astype(jnp.bfloat16)
        for h in range(heads):
            part = slice(h * HEAD_DIM, (h + 1) * HEAD_DIM)
            vall[h, axes(h)[2], core, 0:HEAD_DIM, rows] = used[part, :]
        devbuf[zme, :, rows] = fold(kacc[rows, :] - cached_k) + fold(vacc[rows, :] - cached_v)
    for h in range(heads):
        ksend[h, cut:tok, :] = jnp.dot(
            last_ref[...], kall[h, axes(h)[2], core], preferred_element_type=jnp.float32
        ).astype(jnp.bfloat16)
        vsend[h, :, cut:tok] = lax.dot_general(
            vall[h, axes(h)[2], core, 0:HEAD_DIM, :], last_ref[...], NT,
            preferred_element_type=jnp.float32,
        ).astype(jnp.bfloat16)
    for h in rest:
        store_queries(h, queries[h])
    for h in range(heads):
        forward(1, h, axes(h)[2], core, 2).start()
    send_blocks(0, 1, urgent)
    send_blocks(1, 1, urgent)
    for h in rest:
        send_queries(h)
    for arr in (0, 1):
        send_blocks(arr, 1, lambda h: jnp.logical_not(urgent(h)), (1,))
    sends = []
    if kz > 1:
        hear(0)
    for d in range(1, kz):
        sends.append(
            pltpu.make_async_remote_copy(
                src_ref=devbuf.at[zme], dst_ref=devbuf.at[zme], send_sem=z_send.at[d - 1],
                recv_sem=z_recv.at[kz - d - 1], device_id={"kvh": (zme + d) % kz},
                device_id_type=MESH,
            )
        )
        sends[-1].start()

    def run(items, answers=()):
        def scores_of(item):
            h, q, k, which, part, masked = item
            s = lax.dot_general(
                kall[h, k, which], qbuf[h, q, part, :], NT, preferred_element_type=jnp.float32
            )
            if masked:
                s = s + jnp.concatenate([bias_ref[...]] * GROUP, axis=1)
            return s

        scores = scores_of(items[0])
        for i, (h, q, k, which, part, masked) in enumerate(items):
            following = scores_of(items[i + 1]) if i + 1 < len(items) else None
            best = jnp.max(scores, axis=0, keepdims=True)
            weights = jnp.exp2(scores - best).astype(jnp.bfloat16)
            mixed = jnp.dot(vall[h, k, which], weights, preferred_element_type=jnp.float32)
            if not masked:
                old = m_ref[h, q, 0:1, part]
                top = jnp.maximum(old, best)
                mixed = mixed * jnp.exp2(best - top)
                mixed = mixed + acc_ref[h, q, :, part] * jnp.exp2(old - top)
                best = top
            m_ref[h, q, 0:1, part] = best
            acc_ref[h, q, :, part] = mixed
            scores = following
            if answers and (i + 1) % (len(items) // len(answers)) == 0:
                give_back(h, q, answers[i * len(answers) // len(items)])

    lanes = (core, 1 - core)
    wide = slice(0, qrows)

    def both(h, q, k):
        run([(h, q, k, c, wide, False) for c in lanes])

    every = range(len(col_parts))

    def serve(h, q, k, lanes, wait=False, answer=False, indices=every):
        items = {x: [(h, q, k, c, col_parts[x], False) for c in lanes] for x in indices}
        if wait:
            for index in indices:
                q_wait(h, q, index)
                run(items[index], [index] if answer else ())
            return
        run(sum(items.values(), []), indices if answer else ())

    def p_copies(h, to, index):
        qc, nq, kc, nk = axes(h)
        dest = {"seq": chip_at(h, to, kc) * 2 + core}
        return [
            pltpu.make_async_remote_copy(
                src_ref=pout.at[h, to, index], dst_ref=pin.at[h, qc, index],
                send_sem=p_send.at[h, (to - qc - 1) % nq, index, 0],
                recv_sem=p_recv.at[h, (qc - to - 1) % nq, index, 0],
                device_id=dest, device_id_type=MESH,
            ),
            pltpu.make_async_remote_copy(
                src_ref=pout_stat.at[h, to, index], dst_ref=pin_stat.at[h, qc, index],
                send_sem=p_send.at[h, (to - qc - 1) % nq, index, 1],
                recv_sem=p_recv.at[h, (qc - to - 1) % nq, index, 1],
                device_id=dest, device_id_type=MESH,
            ),
        ]

    def p_wait(h, source, index):
        qc, nq, kc, nk = axes(h)
        place = (source - qc - 1) % nq
        for i, buf in enumerate((pin, pin_stat)):
            view = buf.at[h, source, index]
            pltpu.make_async_remote_copy(
                src_ref=view, dst_ref=view, send_sem=p_send.at[h, place, index, i],
                recv_sem=p_recv.at[h, place, index, i], device_id={"seq": partner},
                device_id_type=MESH,
            ).wait_recv()

    def give_back(h, to, index):
        part = col_parts[index]
        pout[h, to, index] = acc_ref[h, to, 0:HEAD_DIM, part].astype(jnp.bfloat16)
        pout_stat[h, to, index, 0:1, :] = m_ref[h, to, 0:1, part]
        pout_stat[h, to, index, 1:2, :] = acc_ref[h, to, HEAD_DIM:HEAD_DIM + 1, part]
        for copy in p_copies(h, to, index):
            copy.start()

    def no_moved(h):
        qc, nq, kc, nk = axes(h)
        return kc == 0 if h % 2 == 0 else nk == 1
    run(
        [
            (h, axes(h)[0], axes(h)[2], core, wide, True)
            for h in range(heads)
        ]
    )
    for h in range(heads):
        for arr in (0, 1):
            forward(arr, h, axes(h)[2], 1 - core, 2).wait_recv()
    @pl.when(core == 1)
    def _():
        run(
            [
                (h, axes(h)[0], axes(h)[2], 0, wide, False)
                for h in range(heads)
            ]
        )

    def serve_own(h, early):
        qc, nq, kc, nk = axes(h)
        alone = no_moved(h)

        def part(j, index):
            serve(h, j, kc, lanes, True, False, (index,))

        def answer(j, index):
            pl.when(alone)(lambda: give_back(h, j, index))

        def go(j):
            if early:
                @pl.when(alone)
                def _():
                    part(j, 0)
                    give_back(h, j, 0)
                return
            pl.when(jnp.logical_not(alone))(lambda: part(j, 0))
            for index in every[1:]:
                part(j, index)
                answer(j, index)

        each_q(h, lambda j: j > qc, go)

    def moved_wanted(h, j):
        return takes_q(h, j) & jnp.logical_not(no_moved(h))

    def near_lane(h):
        qc, nq, kc, nk = axes(h)
        if nk == 2:
            each_q(
                h, functools.partial(moved_wanted, h), lambda j: serve(h, j, 1 - kc, lanes[:1])
            )

    def far_lane(h):
        qc, nq, kc, nk = axes(h)

        def go(j):
            each_k(h, functools.partial(takes_kv, h), lambda i: both(h, j, i))
            for index in every:
                give_back(h, j, index)

        pl.when(ia < rows_a - 1)(lambda: arrive(h))
        if nk == 2:
            each_q(
                h, functools.partial(moved_wanted, h),
                lambda j: serve(h, j, 1 - kc, lanes[1:], False, True),
            )
        else:
            each_q(h, functools.partial(moved_wanted, h), go)

    def earlier(h, j):
        other = 1 - axes(h)[2]
        serve(h, j, other, lanes, True, False, every[:1])
        if h == 0 and halved:
            pl.when(corner)(exchange)
        give_back(h, j, 0)
        serve(h, j, other, lanes, True, True, every[1:])

    def serve_moved(h):
        qc, nq, kc, nk = axes(h)

        def go(j):
            @pl.when(j < qc)
            def _():
                for index in every:
                    q_wait(h, j, index)
            each_k(h, functools.partial(takes_kv, h), lambda i: both(h, j, i))
            for index in every:
                give_back(h, j, index)

        arrive(h)
        if nk == 2:
            each_q(
                h, lambda j: moved_wanted(h, j) & (j < qc),
                functools.partial(earlier, h),
            )
            each_q(
                h, lambda j: moved_wanted(h, j) & (j > qc),
                lambda j: serve(h, j, 1 - kc, lanes, False, True),
            )
        else:
            each_q(h, functools.partial(moved_wanted, h), go)

    def spans_of():
        position = token + me * tok
        inside = []
        end = jnp.int32(0)
        for d in range(docs):
            begin, end = end, end + lens_ref[d]
            inside.append((position >= begin) & (position < end))
        return inside

    def doc_copy(d):
        return pltpu.make_async_remote_copy(
            src_ref=docbuf.at[me], dst_ref=docbuf.at[me], send_sem=doc_send.at[d - 1],
            recv_sem=doc_recv.at[n - d - 1], device_id={"seq": (me + d) % n},
            device_id_type=MESH,
        )

    def exchange():
        for d in range(1, kz):
            src = (zme + d) % kz
            pltpu.make_async_remote_copy(
                src_ref=devbuf.at[src], dst_ref=devbuf.at[src], send_sem=z_send.at[0],
                recv_sem=z_recv.at[d - 1], device_id={"kvh": src}, device_id_type=MESH,
            ).wait_recv()
        deviation = devbuf[0]
        for z in range(1, kz):
            deviation = deviation + devbuf[z]
        dev_ref[...] = deviation
        inside = spans_of()
        slot_row = lax.broadcasted_iota(jnp.int32, docbuf.shape[1:], 0)
        shares = jnp.zeros(docbuf.shape[1:], jnp.float32)
        for d in range(docs):
            share = jnp.sum(jnp.where(inside[d], deviation, 0.0), axis=1, keepdims=True)
            shares = jnp.where(slot_row == d, share, shares)
        docbuf[me] = shares
        for d in range(1, n):
            doc_copy(d).start()

    lens_load.wait()
    for h in range(1, heads, 2):
        serve_own(h, True)
        serve_own(h, False)
    for h in range(heads):
        forward_blocks(h, 0, functools.partial(takes_kv, h))
        if h % 2 == 0:
            forward_blocks(h, 1, functools.partial(takes_kv, h))
        else:
            forward_blocks(
                h, 1, lambda i, h=h: takes_kv(h, i) & jnp.logical_not(shared_link(h, i))
            )
    for h in range(1, heads, 2):
        forward_blocks(
            h, 1, lambda i, h=h: takes_kv(h, i) & shared_link(h, i) & (ia < rows_a - 1)
        )
    for h in range(1, heads, 2):
        near_lane(h)
    pl.when(ia < rows_a - 1)(exchange)
    for h in range(0, heads, 2):
        serve_own(h, True)
    for h in range(1, heads, 2):
        far_lane(h)
    for h in range(0, heads, 2):
        serve_own(h, False)
    last_row = ia == rows_a - 1
    halved = rows_a == 2 and rows_b == 2 and len(col_parts) > 1
    corner = last_row & (ib == rows_b - 1) if halved else False
    pl.when(last_row & jnp.logical_not(corner))(exchange)
    for h in range(0, heads, 2):
        serve_moved(h)
    for h in range(1, heads, 2):
        forward_blocks(h, 1, lambda i, h=h: takes_kv(h, i) & (ia == rows_a - 1))
    for h in range(heads):
        qc, nq, kc, nk = axes(h)
        if h % 2 == 1:
            pl.when(ia == rows_a - 1)(functools.partial(arrive, h))
        each_k(h, lambda i, kc=kc: i < kc, lambda i, h=h, qc=qc: both(h, qc, i))
    for h in range(heads):
        qc, nq, kc, nk = axes(h)

        def collect(source, h=h, qc=qc):
            for index, part in enumerate(col_parts):
                p_wait(h, source, index)
                best = m_ref[h, qc, 0:1, part]
                other = pin_stat[h, source, index, 0:1, :]
                top = jnp.maximum(best, other)
                fade, rise = jnp.exp2(best - top), jnp.exp2(other - top)
                m_ref[h, qc, 0:1, part] = top
                acc_ref[h, qc, 0:HEAD_DIM, part] = (
                    acc_ref[h, qc, 0:HEAD_DIM, part] * fade
                    + pin[h, source, index].astype(jnp.float32) * rise
                )
                acc_ref[h, qc, HEAD_DIM:HEAD_DIM + 1, part] = (
                    acc_ref[h, qc, HEAD_DIM:HEAD_DIM + 1, part] * fade
                    + pin_stat[h, source, index, 1:2, :] * rise
                )

        each_q(h, functools.partial(sends_q, h), collect)
        done = acc_ref[h, qc, 0:HEAD_DIM, :] / acc_ref[h, qc, HEAD_DIM:HEAD_DIM + 1, :]
        for g in range(GROUP):
            head = h * GROUP + g
            rows = done[:, g * pad:(g + 1) * pad].T.astype(jnp.bfloat16)
            out_ref[:, head * HEAD_DIM:(head + 1) * HEAD_DIM] = rows[0:sel_rows]
    for d in range(1, n):
        src = (me + d) % n
        pltpu.make_async_remote_copy(
            src_ref=docbuf.at[src], dst_ref=docbuf.at[src], send_sem=doc_send.at[0],
            recv_sem=doc_recv.at[d - 1], device_id={"seq": src}, device_id_type=MESH,
        ).wait_recv()
    inside = spans_of()
    totals = docbuf[0]
    for s in range(1, n):
        totals = totals + docbuf[s]
    mean = jnp.zeros((1, tok), jnp.float32)
    for d in range(docs):
        here = totals[d:d + 1, 0:1] / lens_ref[d].astype(jnp.float32)
        mean = jnp.where(inside[d], here, mean)
    score_ref[...] = dev_ref[...] / (mean + 1.0)
    for send in sends:
        send.wait_send()
    for d in range(1, n):
        doc_copy(d).wait_send()
    for h in range(heads):
        qc, nq, kc, nk = axes(h)

        def drain_kv(to, h=h):
            for span in (0, 1):
                for arr in (0, 1):
                    move(arr, h, span, to).wait_send()

        def drain_forward(source, h=h):
            for span in (0, 1):
                for arr in (0, 1):
                    forward(arr, h, source, core, span).wait_send()

        def drain_p(to, h=h):
            for index in range(len(col_parts)):
                for copy in p_copies(h, to, index):
                    copy.wait_send()

        for arr in (0, 1):
            forward(arr, h, kc, core, 2).wait_send()
        each_k(h, functools.partial(sends_kv, h), drain_kv)
        each_k(h, functools.partial(takes_kv, h), drain_forward)

        def drain_q(to, h=h):
            for index in range(len(col_parts)):
                q_copy(h, to, index).wait_send()

        each_q(h, functools.partial(sends_q, h), drain_q)
        each_q(h, functools.partial(takes_q, h), drain_p)


def shards(n, kz, hidden, w_query, w_key, w_value, cached_key, cached_value, doc_lengths, selected):
    tok, width = hidden.shape
    cols = w_key.shape[1]
    qcols = w_query.shape[1]
    sel_rows = selected.shape[0] // n
    docs = doc_lengths.shape[0]
    pad = round_up(sel_rows, LANES)
    heads = cols // HEAD_DIM
    qrows = GROUP * pad
    cut = (tok - sel_rows) // LANES * LANES
    cut_q = q_cols(qrows)
    side = max(split_chips(n // 2))
    others = max(1, side - 1)
    bf, f32 = jnp.bfloat16, jnp.float32
    dma = pltpu.SemaphoreType.DMA
    hbm = pl.BlockSpec(memory_space=pltpu.HBM)
    vmem = pl.BlockSpec(memory_space=pltpu.VMEM)
    attended, score = pl.pallas_call(
        functools.partial(kernel, n, kz, docs, sel_rows),
        out_shape=(
            pltpu.VMEM((sel_rows, qcols), bf),
            pltpu.VMEM((1, tok), f32),
        ),
        in_specs=[hbm] * 8,
        out_specs=(vmem, vmem),
        scratch_shapes=[
            pltpu.VMEM((tok, width), bf),
            pltpu.VMEM((width, qcols), bf),
            pltpu.VMEM((width, cols), bf),
            pltpu.VMEM((width, cols), bf),
            pltpu.VMEM((tok, cols), bf),
            pltpu.VMEM((tok, cols), bf),
            pltpu.VMEM((pad, width), bf),
            pltpu.VMEM((heads, side, 2, tok, HEAD_DIM), bf),
            pltpu.VMEM((heads, side, 2, HEAD_DIM + EXTRA, tok), bf),
            pltpu.VMEM((heads, tok, HEAD_DIM), bf),
            pltpu.VMEM((heads, HEAD_DIM, tok), bf),
            pltpu.VMEM((heads, side, qrows, HEAD_DIM), bf),
            pltpu.VMEM((heads, side, qrows // cut_q, HEAD_DIM, cut_q), bf),
            pltpu.VMEM((heads, side, qrows // cut_q, 2, cut_q), f32),
            pltpu.VMEM((heads, side, qrows // cut_q, HEAD_DIM, cut_q), bf),
            pltpu.VMEM((heads, side, qrows // cut_q, 2, cut_q), f32),
            pltpu.VMEM((tok, cols), f32),
            pltpu.VMEM((tok, cols), f32),
            pltpu.VMEM((heads, side, 8, qrows), f32),
            pltpu.VMEM((heads, side, HEAD_DIM + EXTRA, qrows), f32),
            pltpu.VMEM((tok, pad), f32),
            pltpu.VMEM((tok, LANES), f32),
            pltpu.VMEM((tok - cut, tok), bf),
            pltpu.VMEM((1, tok), f32),
            pltpu.VMEM((kz, 1, tok), f32),
            pltpu.VMEM((n, round_up(docs, 8), 128), f32),
            pltpu.SMEM(doc_lengths.shape, jnp.int32),
            pltpu.SMEM(selected.shape, jnp.int32),
            dma((3 * HID_CHUNKS + 4 + heads,)),
            dma((heads, others, qrows // cut_q)),
            dma((heads, others, qrows // cut_q)),
            dma((heads, others, qrows // cut_q, 2)),
            dma((heads, others, qrows // cut_q, 2)),
            dma((heads, others, 2, 2)),
            dma((heads, others, 2, 2)),
            dma((heads, others, 2, 2)),
            dma((heads, others, 2, 2)),
            dma((heads, 2)),
            dma((heads, 2)),
            dma((max(1, kz - 1),)),
            dma((max(1, kz - 1),)),
            dma((n - 1,)),
            dma((n - 1,)),
            pltpu.SemaphoreType.REGULAR,
        ],
        compiler_params=pltpu.CompilerParams(
            collective_id=0, has_side_effects=True, vmem_limit_bytes=56 * 1024 * 1024
        ),
        name="blend",
    )(hidden, w_query, w_key, w_value, cached_key, cached_value, doc_lengths, selected)
    return attended, score.reshape(tok)


def solution(mesh):
    return jax.shard_map(
        functools.partial(shards, mesh.shape["seq"], mesh.shape["kvh"]),
        mesh=mesh,
        in_specs=(
            P("seq", None),
            P(None, "kvh"),
            P(None, "kvh"),
            P(None, "kvh"),
            P("seq", "kvh"),
            P("seq", "kvh"),
            P(),
            P(),
        ),
        out_specs=(P("seq", "kvh"), P("seq")),
        check_vma=False,
    )
```
